32 devices in a mesh: dp: 4 (over y, z), stage: 8 (over x, core).
Axes of the slice: x: 4, y: 2, z: 2, core: 2. Of those that a mesh axis runs over, the one named last changes fastest.
The devices are a block of a 4x4x8 slice.
Arguments:
- token_ids: int32 [32, 256], P('dp'), parts along dimension 0
- label_ids: int32 [32, 256], P('dp'), parts along dimension 0
- embedding: bfloat16 [50304, 768], P('stage')
- w_in: bfloat16 [8, 768, 3072], P('stage')
- w_out: bfloat16 [8, 3072, 768], P('stage')
Outputs:
- output 1: float32 [4], P('dp'), parts along dimension 0
- output 2: float32 [32, 768, 3072], P(('dp', 'stage')), parts along dimension 0
- output 3: float32 [32, 3072, 768], P(('dp', 'stage')), parts along dimension 0
- output 4: float32 [201216, 768], P(('dp', 'stage')), parts along dimension 0
There are 4 independent parts. The reference program is written for one: setup_inputs(seed, part) draws one part's arguments, and reference() takes and returns one part's arrays. A program takes and returns all parts, laid end to end along the dimension named above; an argument that names none is the same for every part.
All inputs are finite; a program needn't handle non-finite values.
Results may differ from the reference program's by a relative error of at most 0.0165463.
Values are sent between devices in bfloat16 or wider.
A program may use at most 768 MiB of HBM per device.

```python
import functools
import jax
import jax.numpy as jnp
from jax import lax

VOCAB_SIZE = 50304
MODEL_DIM = 768
FFN_DIM = 3072
STAGES = 8
MICROBATCHES = 8
MICRO_TOKENS = 256
HOT_IDS = 64
NORM_EPS = 1e-6


def draw_ids(hot_ids, id_key):
    key_pick, key_unif, key_mix = jax.random.split(id_key, 3)
    shape_ids = (MICROBATCHES, MICRO_TOKENS)
    picked = hot_ids[jax.random.randint(key_pick, shape_ids, 0, HOT_IDS)]
    uniform_ids = jax.random.randint(key_unif, shape_ids, 0, VOCAB_SIZE)
    use_hot = jax.random.randint(key_mix, shape_ids, 0, 2) == 1
    return jnp.where(use_hot, picked, uniform_ids).astype(jnp.int32)


def setup_inputs(seed: int = 0, part: int = 0) -> dict:
    root_key = jax.random.key(seed)
    key_ids, key_emb, key_in, key_out = jax.random.split(root_key, 4)
    part_key = jax.random.fold_in(key_ids, part)
    key_hot, key_tok, key_lab = jax.random.split(part_key, 3)
    hot_ids = jax.random.randint(key_hot, (HOT_IDS,), 0, VOCAB_SIZE)
    token_ids = draw_ids(hot_ids, key_tok)
    label_ids = draw_ids(hot_ids, key_lab)
    embedding = jax.random.normal(key_emb, (VOCAB_SIZE, MODEL_DIM), jnp.float32).astype(jnp.bfloat16)
    w_in = (jax.random.normal(key_in, (STAGES, MODEL_DIM, FFN_DIM), jnp.float32) * MODEL_DIM ** -0.5).astype(jnp.bfloat16)
    w_out = (jax.random.normal(key_out, (STAGES, FFN_DIM, MODEL_DIM), jnp.float32) * 2.0 * (FFN_DIM * STAGES) ** -0.5).astype(jnp.bfloat16)
    return {"token_ids": token_ids, "label_ids": label_ids, "embedding": embedding, "w_in": w_in, "w_out": w_out}


def rms_normed(act_rows):
    acts_f = act_rows.astype(jnp.float32)
    return (acts_f * lax.rsqrt(jnp.mean(acts_f * acts_f, axis=-1, keepdims=True) + NORM_EPS)).astype(jnp.bfloat16)


def summed_loss(emb_f32, w_in_f32, w_out_f32, token_ids, label_ids):
    logit_scale = MODEL_DIM ** -0.5
    vocab_iota = jnp.arange(VOCAB_SIZE, dtype=jnp.int32)

    def layer_step(act_rows, weights):
        w_first, w_second = weights
        acts_f = act_rows.astype(jnp.float32)
        pre_act = jnp.dot(acts_f, w_first, preferred_element_type=jnp.float32)
        hidden = jax.nn.gelu(pre_act).astype(jnp.bfloat16)
        out_f = acts_f + jnp.dot(hidden.astype(jnp.float32), w_second, preferred_element_type=jnp.float32)
        return out_f.astype(jnp.bfloat16), None

    def micro_step(loss_total, ids_pair):
        tok_row, lab_row = ids_pair
        act_rows = emb_f32[tok_row].astype(jnp.bfloat16)
        act_rows, _ = lax.scan(layer_step, act_rows, (w_in_f32, w_out_f32))
        normed = rms_normed(act_rows).astype(jnp.float32)
        logits = jnp.dot(normed, emb_f32.T, preferred_element_type=jnp.float32) * logit_scale
        picked = jnp.sum(jnp.where(lab_row[:, None] == vocab_iota[None, :], logits, 0.0), axis=1)
        return loss_total + jnp.sum(jax.nn.logsumexp(logits, axis=1) - picked), None

    loss_total, _ = lax.scan(jax.checkpoint(micro_step), jnp.zeros((), jnp.float32), (token_ids, label_ids))
    return loss_total


def reference(token_ids, label_ids, embedding, w_in, w_out):
    loss_fn = functools.partial(summed_loss, token_ids=token_ids, label_ids=label_ids)
    loss_total, pull_back = jax.vjp(loss_fn, embedding.astype(jnp.float32), w_in.astype(jnp.float32), w_out.astype(jnp.float32))
    grad_emb, grad_in, grad_out = pull_back(jnp.ones((), jnp.float32))
    mean_loss = (loss_total / (MICROBATCHES * MICRO_TOKENS)).reshape(1)
    return (mean_loss, grad_in, grad_out, grad_emb)
```

```python
import functools
import math

import jax
import jax.numpy as jnp
from jax import lax
from jax.experimental import pallas as pl
from jax.experimental.pallas import tpu as pltpu
from jax.sharding import PartitionSpec as P

NORM_EPS = 1e-6
MESH = pl.DeviceIdType.MESH
F32 = jnp.float32
BF16 = jnp.bfloat16
GELU_A = math.sqrt(2.0 / math.pi)
GELU_B = 0.044715
LOG2E = math.log2(math.e)
CHUNK = 128
HEAD_MBS = 2
VMEM_LIMIT = 67_000_000


def dot_nn(a, b):
    return lax.dot_general(a, b, (((1,), (0,)), ((), ())), preferred_element_type=F32)


def dot_nt(a, b):
    return lax.dot_general(a, b, (((1,), (1,)), ((), ())), preferred_element_type=F32)


def dot_tn(a, b):
    return lax.dot_general(a, b, (((0,), (0,)), ((), ())), preferred_element_type=F32)


def gelu_f32(pre):
    inner = GELU_A * (pre + GELU_B * (pre * pre * pre))
    return (0.5 * pre) * (1.0 + jnp.tanh(inner))


def norm_scale(x_f32):
    return lax.rsqrt(jnp.mean(x_f32 * x_f32, axis=-1, keepdims=True) + NORM_EPS)


def remote(src, dst, send_sem, recv_sem, stage):
    return pltpu.make_async_remote_copy(
        src_ref=src, dst_ref=dst, send_sem=send_sem, recv_sem=recv_sem, device_id={"stage": stage}, device_id_type=MESH
    )


def group_barrier(stage, n_stage):
    barrier = pltpu.get_barrier_semaphore()
    for off in range(1, n_stage):
        pl.semaphore_signal(barrier, inc=1, device_id={"stage": lax.rem(stage + off, n_stage)}, device_id_type=MESH)
    pl.semaphore_wait(barrier, n_stage - 1)


def vocab_tile(rows):
    for parts in range(2, rows + 1):
        if rows % parts == 0 and (rows // parts) % 16 == 0 and rows // parts <= 2400:
            return rows // parts
    return rows


def sub_blocks(rows, size):
    return [(start, min(size, rows - start)) for start in range(0, rows, size)]


def forward_chunk(x, w1, w2, pre_slot, hid):
    ffn = w1.shape[1]
    width = ffn // 4
    for part in range(4):
        cols = pl.ds(part * width, width)
        pre = dot_nn(x, w1[:, cols])
        pre_slot[:, cols] = pre
        hid[:, cols] = gelu_f32(pre).astype(BF16)
    return x.astype(F32) + dot_nn(hid[...], w2[...])


def head_logits(n_t, emb, logits, lab_row, tokens):
    rows = emb.shape[0]
    tile = vocab_tile(rows)
    c2 = LOG2E * emb.shape[1] ** -0.5

    def tile_step(idx, carry):
        mx, sm, lb = carry
        base = pl.multiple_of(idx * tile, 16)
        for start, size in sub_blocks(tile, 256):
            at = pl.ds(base + start, size)
            block = dot_nn(emb[at, :], n_t[...])
            logits[at, :] = block
            b3 = block.reshape(size // 8, 8, tokens)
            row_ids = lax.broadcasted_iota(jnp.int32, (size, tokens), 0) + (base + start)
            hit = jnp.where(row_ids == lab_row, block, 0.0).reshape(size // 8, 8, tokens)
            mx_new = jnp.maximum(mx, jnp.max(b3, axis=0))
            sm = sm * jnp.exp2((mx - mx_new) * c2) + jnp.sum(jnp.exp2((b3 - mx_new[None]) * c2), axis=0)
            lb = lb + jnp.sum(hit, axis=0)
            mx = mx_new
        return mx, sm, lb

    init = (jnp.full((8, tokens), -3.0e38, F32), jnp.zeros((8, tokens), F32), jnp.zeros((8, tokens), F32))
    mx, sm, lb = lax.fori_loop(0, rows // tile, tile_step, init)
    top = jnp.max(mx, axis=0, keepdims=True)
    tot = jnp.sum(sm * jnp.exp2((mx - top) * c2), axis=0, keepdims=True)
    lab = jnp.sum(lb, axis=0, keepdims=True)
    return top, tot, lab


def head_grad_tile(idx, tile, emb, logits, d_slot, lab_row, top, shift, tokens):
    scale = emb.shape[1] ** -0.5
    c2 = LOG2E * scale
    base = pl.multiple_of(idx * tile, 16)
    for start, size in sub_blocks(tile, 256):
        at = pl.ds(base + start, size)
        row_ids = lax.broadcasted_iota(jnp.int32, (size, tokens), 0) + (base + start)
        prob = jnp.exp2((logits[at, :] - top) * c2 - shift)
        d_slot[pl.ds(start, size), :] = (prob - jnp.where(row_ids == lab_row, scale, 0.0)).astype(BF16)
    return dot_tn(d_slot[...], emb[pl.ds(base, tile), :])


def forward_head_kernel(
    n_stage, lab_ref, part_hbm, emb_hbm, w1_hbm, w2_hbm,
    pre_out, xin_out, n_out, dt_out, dxl_out, loss_out,
    emb, w1, w2, x_in, x_out, n_all, comb, buf_a, buf_b, logits, n_t, pre_stg, hid, d_stg, gn_acc, stats, loss_acc,
    load_sem, part_sem, lk_send, lk_a, lk_b, x_send, x_recv, n_send, n_recv, st_send, st_recv,
    g_send, g_a, g_b, pre_sem, d_sem, out_sem,
):
    s = lax.axis_index("stage")
    last = n_stage - 1
    mbs, mtok, dim = x_in.shape
    n_half = mtok // CHUNK
    rows = emb.shape[0]
    tile = vocab_tile(rows)
    tokens = HEAD_MBS * mtok
    rounds = mbs // HEAD_MBS
    scale = dim ** -0.5
    c2 = LOG2E * scale
    row_start = s * rows

    loads = [pltpu.make_async_copy(src, dst, load_sem.at[i])
             for i, (src, dst) in enumerate([(w1_hbm, w1), (w2_hbm, w2), (emb_hbm, emb)])]
    for mb in range(mbs):
        pltpu.make_async_copy(part_hbm.at[mb], comb.at[mb], part_sem.at[mb]).start()
    for ld in loads:
        ld.start()
    group_barrier(s, n_stage)

    def half(mb, hf):
        return (mb, pl.ds(pl.multiple_of(hf * CHUNK, CHUNK), CHUNK))

    def at_half(ref, mb, hf):
        return ref.at[mb, pl.ds(pl.multiple_of(hf * CHUNK, CHUNK), CHUNK)]

    def lk_copy(mb, hf, child):
        parent, slot, sem = {1: (0, buf_a, lk_a), 2: (3, buf_a, lk_a), 3: (1, buf_a, lk_a), 4: (5, buf_a, lk_a),
                             6: (7, buf_a, lk_a), 5: (3, buf_b, lk_b), 7: (0, buf_b, lk_b)}[child]
        c = mb * n_half + hf
        return remote(at_half(comb, mb, hf), at_half(slot, mb, hf), lk_send.at[c], sem.at[c], parent)

    def lk_wait(mb, hf, slot, sem):
        c = mb * n_half + hf
        remote(at_half(comb, mb, hf), at_half(slot, mb, hf), lk_send.at[c], sem.at[c], 0).wait_recv()

    def chunks(fn):
        def step(c, _):
            fn(c // n_half, lax.rem(c, n_half))
            return 0
        lax.fori_loop(0, mbs * n_half, step, 0)

    def halves(mb, fn):
        def step(hf, _):
            fn(mb, hf)
            return 0
        lax.fori_loop(0, n_half, step, 0)

    def part_wait(mb, _):
        pltpu.make_async_copy(part_hbm.at[mb], comb.at[mb], part_sem.at[mb]).wait()
        return 0

    lax.fori_loop(0, mbs, part_wait, 0)

    for child in (2, 4, 6):
        @pl.when(s == child)
        def _(child=child):
            chunks(lambda mb, hf: lk_copy(mb, hf, child).start())

    def add_in(mb, hf, slots):
        idx = half(mb, hf)
        total = comb[idx].astype(F32)
        for slot, sem in slots:
            lk_wait(mb, hf, slot, sem)
            total = total + slot[idx].astype(F32)
        comb[idx] = total.astype(BF16)

    for child in (5, 7):
        @pl.when(s == child)
        def _(child=child):
            def fwd(mb, hf):
                add_in(mb, hf, [(buf_a, lk_a)])
                lk_copy(mb, hf, child).start()
            chunks(fwd)

    loads[0].wait()
    loads[1].wait()
    loads[2].wait()

    def x_copy(mb, hf, dst_stage):
        c = mb * n_half + hf
        return remote(at_half(x_out, mb, hf), at_half(x_in, mb, hf), x_send.at[c], x_recv.at[c], dst_stage)

    def n_copy(mb, hf, lane, dst_stage):
        c = mb * n_half + hf
        return remote(at_half(n_all, mb, hf), at_half(n_all, mb, hf), n_send.at[lane, c], n_recv.at[c], dst_stage)

    def pre_copy(c):
        slot = lax.rem(c, 2)
        return pltpu.make_async_copy(pre_stg.at[slot], pre_out.at[c], pre_sem.at[slot])

    def fwd_chunk(mb, hf):
        c = mb * n_half + hf
        idx = half(mb, hf)

        @pl.when(s == 0)
        def _():
            total = comb[idx].astype(F32)
            for slot, sem in ((buf_a, lk_a), (buf_b, lk_b)):
                lk_wait(mb, hf, slot, sem)
                total = total + slot[idx].astype(F32)
            x_in[idx] = total.astype(BF16)

        @pl.when(s > 0)
        def _():
            x_copy(mb, hf, 0).wait_recv()

        @pl.when(c >= 2)
        def _():
            pre_copy(c - 2).wait()

        out = forward_chunk(x_in[idx], w1, w2, pre_stg.at[lax.rem(c, 2)], hid).astype(BF16)
        x_out[idx] = out
        pre_copy(c).start()

        @pl.when(s < last)
        def _():
            x_copy(mb, hf, s + 1).start()

        @pl.when(s == last)
        def _():
            out_f = out.astype(F32)
            n_all[idx] = (out_f * norm_scale(out_f)).astype(BF16)
            for lane, dst in enumerate((5, 1, 6)):
                n_copy(mb, hf, lane, dst).start()

    def n_forward(mb, hf):
        @pl.when(s < last)
        def _():
            n_copy(mb, hf, 0, last).wait_recv()
        for src, dsts in ((5, (3, 4)), (3, (2,)), (1, (0,))):
            @pl.when(s == src)
            def _(dsts=dsts):
                for lane, dst in enumerate(dsts):
                    n_copy(mb, hf, lane, dst).start()

    def lab_row_of(r):
        parts = [lab_ref[pl.ds(r * HEAD_MBS + i, 1), :] for i in range(HEAD_MBS)]
        return jnp.concatenate(parts, axis=1) - row_start

    def st_copy(r, off):
        dst = lax.rem(s + off, n_stage)
        return remote(stats.at[r, s], stats.at[r, s], st_send.at[r, off], st_recv.at[r, off], dst)

    def head_a(r):
        n_t[...] = n_all[pl.ds(r * HEAD_MBS, HEAD_MBS)].reshape(tokens, dim).T
        lab_row = lab_row_of(r)
        top, tot, lab = head_logits(n_t, emb, logits, lab_row, tokens)
        stats[r, s] = jnp.concatenate([top, tot, lab, jnp.zeros((5, tokens), F32)], axis=0)
        for off in range(1, n_stage):
            st_copy(r, off).start()

    def d_copy(r, idx):
        slot = lax.rem(idx, 2)
        dst = dt_out.at[pl.ds(pl.multiple_of(idx * tile, 16), tile), pl.ds(pl.multiple_of(r * tokens, tokens), tokens)]
        return pltpu.make_async_copy(d_stg.at[slot], dst, d_sem.at[slot])

    def head_b(r):
        for off in range(1, n_stage):
            src = lax.rem(s + n_stage - off, n_stage)
            remote(stats.at[r, s], stats.at[r, src], st_send.at[r, off], st_recv.at[r, off], src).wait_recv()
        blocks = [stats[r, i] for i in range(n_stage)]
        top = blocks[0][0:1]
        for blk in blocks[1:]:
            top = jnp.maximum(top, blk[0:1])
        tot = jnp.zeros_like(top)
        lab = jnp.zeros_like(top)
        for blk in blocks:
            tot = tot + blk[1:2] * jnp.exp2((blk[0:1] - top) * c2)
            lab = lab + blk[2:3]
        loss_acc[...] = loss_acc[...] + (jnp.log(tot) + (top - lab) * scale)
        shift = jnp.log(tot) * LOG2E - math.log2(scale)
        lab_row = lab_row_of(r)

        def tile_step(idx, _):
            @pl.when(idx >= 2)
            def _():
                d_copy(r, idx - 2).wait()
            part = head_grad_tile(idx, tile, emb, logits, d_stg.at[lax.rem(idx, 2)], lab_row, top, shift, tokens)
            gn_acc[...] = gn_acc[...] + part
            d_copy(r, idx).start()
            return 0

        gn_acc[...] = jnp.zeros_like(gn_acc)
        lax.fori_loop(0, rows // tile, tile_step, 0)
        comb[pl.ds(r * HEAD_MBS, HEAD_MBS)] = gn_acc[...].reshape(HEAD_MBS, mtok, dim).astype(BF16)
        for idx in range(rows // tile - 2, rows // tile):
            d_copy(r, idx).wait()
        for child in (0, 2, 4):
            @pl.when(s == child)
            def _(child=child):
                g_copy(r, child).start()
        for child in (1, 3):
            @pl.when(s == child)
            def _(child=child):
                g_add(r, [(buf_a, g_a)])
                g_copy(r, child).start()

    def g_copy(r, child):
        parent, slot, sem = {0: (1, buf_a, g_a), 2: (3, buf_a, g_a), 4: (5, buf_a, g_a), 1: (6, buf_a, g_a),
                             6: (7, buf_a, g_a), 3: (5, buf_b, g_b), 5: (7, buf_b, g_b)}[child]
        at = pl.ds(r * HEAD_MBS, HEAD_MBS)
        return remote(comb.at[at], slot.at[at], g_send.at[r], sem.at[r], parent)

    def g_total(r, slots):
        at = pl.ds(r * HEAD_MBS, HEAD_MBS)
        total = comb[at].astype(F32)
        for slot, sem in slots:
            remote(comb.at[at], slot.at[at], g_send.at[r], sem.at[r], 0).wait_recv()
            total = total + slot[at].astype(F32)
        return total

    def g_add(r, slots):
        comb[pl.ds(r * HEAD_MBS, HEAD_MBS)] = g_total(r, slots).astype(BF16)

    def g_mid(r):
        @pl.when(s == 6)
        def _():
            g_add(r, [(buf_a, g_a)])
            g_copy(r, 6).start()

        @pl.when(s == 5)
        def _():
            g_add(r, [(buf_a, g_a), (buf_b, g_b)])
            g_copy(r, 5).start()

    def g_final(r):
        @pl.when(s == last)
        def _():
            at = pl.ds(r * HEAD_MBS, HEAD_MBS)
            grad_n = g_total(r, [(buf_a, g_a), (buf_b, g_b)])
            x_f = x_out[at].astype(F32)
            inv = norm_scale(x_f)
            n_f = x_f * inv
            dx = inv * (grad_n - n_f * jnp.mean(grad_n * n_f, axis=-1, keepdims=True))
            comb[at] = dx.astype(BF16)
            pltpu.make_async_copy(comb.at[at], dxl_out.at[at], out_sem.at[2]).start()
            pltpu.make_async_copy(comb.at[at], dxl_out.at[at], out_sem.at[2]).wait()

    loss_acc[...] = jnp.zeros_like(loss_acc)
    first_a = HEAD_MBS + 1 + last
    n_steps = HEAD_MBS * (rounds - 1) + first_a + 4

    def step(k, _):
        for node, lead in ((3, 1), (1, 0)):
            c_mb = k + lead
            @pl.when((s == node) & (c_mb < mbs))
            def _(node=node, c_mb=c_mb):
                def comb_fwd(mb, hf):
                    add_in(mb, hf, [(buf_a, lk_a), (buf_b, lk_b)] if node == 3 else [(buf_a, lk_a)])
                    lk_copy(mb, hf, node).start()
                if node == 3:
                    @pl.when(k == 0)
                    def _():
                        halves(0, comb_fwd)
                halves(c_mb, comb_fwd)

        n_mb = k - n_stage
        @pl.when((n_mb >= 0) & (n_mb < mbs))
        def _():
            halves(n_mb, n_forward)

        f_mb = k - s
        @pl.when((f_mb >= 0) & (f_mb < mbs))
        def _():
            halves(f_mb, fwd_chunk)

        @pl.when(k == first_a)
        def _():
            @pl.when(s > 0)
            def _():
                chunks(lambda mb, hf: lk_copy(mb, hf, 1).wait_send())

        rel = k - first_a
        r = rel // HEAD_MBS
        even = lax.rem(rel + HEAD_MBS * n_stage, HEAD_MBS) == 0

        @pl.when(even & (rel >= 0) & (r < rounds))
        def _():
            head_a(r)

        @pl.when(even & (rel >= HEAD_MBS) & (r - 1 < rounds))
        def _():
            g_mid(r - 1)

        @pl.when(jnp.logical_not(even) & (rel >= 0) & (r < rounds))
        def _():
            head_b(r)

        @pl.when(jnp.logical_not(even) & (rel >= HEAD_MBS) & (r - 1 < rounds))
        def _():
            g_final(r - 1)
        return 0

    lax.fori_loop(0, n_steps, step, 0)

    out_copies = [pltpu.make_async_copy(x_in, xin_out, out_sem.at[0]), pltpu.make_async_copy(n_all, n_out, out_sem.at[1])]
    for cp in out_copies:
        cp.start()
    loss_out[...] = jnp.broadcast_to(jnp.sum(loss_acc[...], axis=1, keepdims=True), loss_out.shape)
    for c in (mbs * n_half - 2, mbs * n_half - 1):
        pre_copy(c).wait()
    for cp in out_copies:
        cp.wait()

    @pl.when(s < last)
    def _():
        chunks(lambda mb, hf: x_copy(mb, hf, 0).wait_send())
        def g_drain(r, _):
            g_copy(r, 1).wait_send()
            return 0
        lax.fori_loop(0, rounds, g_drain, 0)

    for src, count in ((last, 3), (5, 2), (3, 1), (1, 1)):
        @pl.when(s == src)
        def _(count=count):
            def drain(mb, hf):
                for lane in range(count):
                    n_copy(mb, hf, lane, 0).wait_send()
            chunks(drain)

    def st_drain(r, _):
        for off in range(1, n_stage):
            st_copy(r, off).wait_send()
        return 0
    lax.fori_loop(0, rounds, st_drain, 0)


def forward_head(n_stage, labels, part, emb, w1, w2):
    mbs, mtok, dim = part.shape
    rows = emb.shape[0]
    ffn = w1.shape[1]
    n_half = mtok // CHUNK
    chunks = mbs * n_half
    rounds = mbs // HEAD_MBS
    tokens = HEAD_MBS * mtok
    tile = vocab_tile(rows)
    any_spec = pl.BlockSpec(memory_space=pl.ANY)
    vmem_spec = pl.BlockSpec(memory_space=pltpu.VMEM)
    act = pltpu.VMEM((mbs, mtok, dim), BF16)
    dma = pltpu.SemaphoreType.DMA
    return pl.pallas_call(
        functools.partial(forward_head_kernel, n_stage),
        out_shape=(
            jax.ShapeDtypeStruct((chunks, CHUNK, ffn), F32),
            jax.ShapeDtypeStruct((mbs, mtok, dim), BF16),
            jax.ShapeDtypeStruct((mbs, mtok, dim), BF16),
            jax.ShapeDtypeStruct((rows, mbs * mtok), BF16),
            jax.ShapeDtypeStruct((mbs, mtok, dim), BF16),
            jax.ShapeDtypeStruct((8, 128), F32),
        ),
        in_specs=[vmem_spec] + [any_spec] * 4,
        out_specs=(any_spec,) * 5 + (vmem_spec,),
        scratch_shapes=[
            pltpu.VMEM((rows, dim), BF16), pltpu.VMEM((dim, ffn), BF16), pltpu.VMEM((ffn, dim), BF16),
            act, act, act, act, act, act,
            pltpu.VMEM((rows, tokens), F32), pltpu.VMEM((dim, tokens), BF16),
            pltpu.VMEM((2, CHUNK, ffn), F32), pltpu.VMEM((CHUNK, ffn), BF16),
            pltpu.VMEM((2, tile, tokens), BF16), pltpu.VMEM((tokens, dim), F32),
            pltpu.VMEM((rounds, n_stage, 8, tokens), F32), pltpu.VMEM((1, tokens), F32),
            dma((3,)), dma((mbs,)), dma((chunks,)), dma((chunks,)), dma((chunks,)),
            dma((chunks,)), dma((chunks,)), dma((3, chunks)), dma((chunks,)),
            dma((rounds, n_stage)), dma((rounds, n_stage)), dma((rounds,)), dma((rounds,)), dma((rounds,)),
            dma((2,)), dma((2,)), dma((3,)),
        ],
        compiler_params=pltpu.CompilerParams(collective_id=0, has_side_effects=True, vmem_limit_bytes=VMEM_LIMIT),
        name="forward_head",
    )(labels, part, emb, w1, w2)


def backward_kernel(
    n_stage, w1_hbm, w2_hbm, pre_hbm, dxl_hbm,
    h_out, dp_out, g_out, gx_out,
    w1, w2, g_in, g_send_buf, gx, pre_stg, h_stg, dp_stg,
    load_sem, dxl_sem, pre_sem, h_sem, dp_sem, out_sem, b_send, b_recv, x_send, x_recv,
):
    s = lax.axis_index("stage")
    last = n_stage - 1
    mbs, mtok, dim = g_in.shape
    ffn = w1.shape[1]
    width = ffn // 4

    loads = [pltpu.make_async_copy(src, dst, load_sem.at[i]) for i, (src, dst) in enumerate([(w2_hbm, w2), (w1_hbm, w1)])]
    for ld in loads:
        ld.start()

    def pre_copy(mb):
        slot = lax.rem(mb, 2)
        return pltpu.make_async_copy(pre_hbm.at[mb], pre_stg.at[slot], pre_sem.at[slot])

    pre_copy(0).start()
    pre_copy(1).start()

    @pl.when(s == last)
    def _():
        pltpu.make_async_copy(dxl_hbm, g_in, dxl_sem.at[0]).start()

    group_barrier(s, n_stage)

    @pl.when(s == last)
    def _():
        pltpu.make_async_copy(dxl_hbm, g_in, dxl_sem.at[0]).wait()
    for ld in loads:
        ld.wait()

    def b_copy(mb, dst):
        return remote(g_send_buf.at[mb], g_in.at[mb], b_send.at[mb], b_recv.at[mb], dst)

    def gx_copy(mb, lane, dst):
        return remote(gx.at[mb], gx.at[mb], x_send.at[lane, mb], x_recv.at[mb], dst)

    def hid_copies(mb):
        slot = lax.rem(mb, 2)
        return (pltpu.make_async_copy(h_stg.at[slot], h_out.at[mb], h_sem.at[slot]),
                pltpu.make_async_copy(dp_stg.at[slot], dp_out.at[mb], dp_sem.at[slot]))

    def backward_mb(mb):
        slot = lax.rem(mb, 2)

        @pl.when(s < last)
        def _():
            b_copy(mb, 0).wait_recv()

        @pl.when(mb >= 2)
        def _():
            for cp in hid_copies(mb - 2):
                cp.wait()
        pre_copy(mb).wait()
        grad = g_in[mb]
        for part in range(4):
            cols = pl.ds(part * width, width)
            dh = dot_nt(grad, w2[cols, :])
            pre = pre_stg[slot, :, cols]
            sq = pre * pre
            th = jnp.tanh(GELU_A * (pre + GELU_B * (sq * pre)))
            half_sum = 0.5 * (1.0 + th)
            h_stg[slot, :, cols] = (pre * half_sum).astype(BF16)
            slope = half_sum + (0.5 * pre) * (1.0 - th * th) * (GELU_A + (3.0 * GELU_A * GELU_B) * sq)
            dp_stg[slot, :, cols] = (dh * slope).astype(BF16)
        dx = (grad.astype(F32) + dot_nt(dp_stg[slot], w1[...])).astype(BF16)

        @pl.when(s > 0)
        def _():
            g_send_buf[mb] = dx
            b_copy(mb, s - 1).start()

        @pl.when(s == 0)
        def _():
            gx[mb] = dx
            for lane, dst in enumerate((3, last, 1)):
                gx_copy(mb, lane, dst).start()
        for cp in hid_copies(mb):
            cp.start()

        @pl.when(mb + 2 < mbs)
        def _():
            pre_copy(mb + 2).start()

    def gx_forward(mb):
        @pl.when(s > 0)
        def _():
            gx_copy(mb, 0, 0).wait_recv()
        for src, dsts in ((3, (5, 2)), (last, (6,)), (5, (4,))):
            @pl.when(s == src)
            def _(dsts=dsts):
                for lane, dst in enumerate(dsts):
                    gx_copy(mb, lane, dst).start()

    def step(k, _):
        b_mb = k - (last - s)
        @pl.when((b_mb >= 0) & (b_mb < mbs))
        def _():
            backward_mb(b_mb)

        x_mb = k - n_stage
        @pl.when((x_mb >= 0) & (x_mb < mbs))
        def _():
            gx_forward(x_mb)
        return 0

    lax.fori_loop(0, mbs + n_stage, step, 0)

    outs = [pltpu.make_async_copy(g_in, g_out, out_sem.at[0]), pltpu.make_async_copy(gx, gx_out, out_sem.at[1])]
    for cp in outs:
        cp.start()
    for mb in (mbs - 2, mbs - 1):
        for cp in hid_copies(mb):
            cp.wait()
    for cp in outs:
        cp.wait()

    @pl.when(s > 0)
    def _():
        def drain(mb, _):
            b_copy(mb, 0).wait_send()
            return 0
        lax.fori_loop(0, mbs, drain, 0)

    for src, count in ((0, 3), (3, 2), (last, 1), (5, 1)):
        @pl.when(s == src)
        def _(count=count):
            def drain(mb, _):
                for lane in range(count):
                    gx_copy(mb, lane, 0 if src != 0 else 1).wait_send()
                return 0
            lax.fori_loop(0, mbs, drain, 0)


def backward(n_stage, w1, w2, pre, dxl):
    mbs, mtok, dim = dxl.shape
    ffn = w1.shape[1]
    any_spec = pl.BlockSpec(memory_space=pl.ANY)
    act = pltpu.VMEM((mbs, mtok, dim), BF16)
    dma = pltpu.SemaphoreType.DMA
    return pl.pallas_call(
        functools.partial(backward_kernel, n_stage),
        out_shape=(
            jax.ShapeDtypeStruct((mbs, mtok, ffn), BF16),
            jax.ShapeDtypeStruct((mbs, mtok, ffn), BF16),
            jax.ShapeDtypeStruct((mbs, mtok, dim), BF16),
            jax.ShapeDtypeStruct((mbs, mtok, dim), BF16),
        ),
        in_specs=[any_spec] * 4,
        out_specs=(any_spec,) * 4,
        scratch_shapes=[
            pltpu.VMEM((dim, ffn), BF16), pltpu.VMEM((ffn, dim), BF16),
            act, act, act,
            pltpu.VMEM((2, mtok, ffn), F32), pltpu.VMEM((2, mtok, ffn), BF16), pltpu.VMEM((2, mtok, ffn), BF16),
            dma((2,)), dma((1,)), dma((2,)), dma((2,)), dma((2,)), dma((2,)),
            dma((mbs,)), dma((mbs,)), dma((3, mbs)), dma((mbs,)),
        ],
        compiler_params=pltpu.CompilerParams(collective_id=1, has_side_effects=True, vmem_limit_bytes=VMEM_LIMIT),
        name="backward",
    )(w1, w2, pre, dxl)


ROWS_E = 512
PACK = 256


def emb_grad_kernel(rows, n_stage, tok_ref, dt_ref, n_ref, gx_ref, out_ref, packed, packed_id, count_ref):
    i = pl.program_id(0)
    mbs, mtok = tok_ref.shape
    n_pack = mbs * mtok // PACK

    @pl.when(i == 0)
    def _():
        s = lax.axis_index("stage")
        loc = tok_ref[...] - s * rows
        here = (loc >= 0) & (loc < rows)
        flag = here.astype(F32)
        upper = (lax.broadcasted_iota(jnp.int32, (mtok, mtok), 0) <= lax.broadcasted_iota(jnp.int32, (mtok, mtok), 1))
        within = dot_nn(flag.astype(BF16), upper.astype(BF16))
        total = jnp.sum(flag, axis=1, keepdims=True)
        lower = (lax.broadcasted_iota(jnp.int32, (mbs, mbs), 1) < lax.broadcasted_iota(jnp.int32, (mbs, mbs), 0))
        before = jnp.sum(jnp.where(lower, jnp.transpose(jnp.broadcast_to(total, (mbs, mbs))), 0.0), axis=1, keepdims=True)
        pos = jnp.where(here, within - 1.0 + before, -1.0).astype(jnp.int32)
        count = jnp.sum(flag).astype(jnp.int32)
        count_ref[0] = count

        for b in range(n_pack):
            @pl.when(b * PACK < count)
            def _(b=b):
                slot = lax.broadcasted_iota(jnp.int32, (PACK, mtok), 0) + b * PACK
                acc = jnp.zeros((PACK, gx_ref.shape[2]), F32)
                ids = jnp.zeros((PACK, 1), F32)
                for mb in range(mbs):
                    pick = slot == pos[mb:mb + 1, :]
                    acc = acc + dot_nn(pick.astype(BF16), gx_ref[mb])
                    ids = ids + jnp.sum(jnp.where(pick, loc[mb:mb + 1, :].astype(F32), 0.0), axis=1, keepdims=True)
                filled = lax.broadcasted_iota(jnp.int32, (PACK, 1), 0) + b * PACK < count
                packed[b] = acc.astype(BF16)
                packed_id[b] = jnp.broadcast_to(jnp.where(filled, ids.astype(jnp.int32), -1), (PACK, 128))

    out_ref[...] = dot_nn(dt_ref[...], n_ref[...].reshape(mbs * mtok, n_ref.shape[2]))
    lane = lax.broadcasted_iota(jnp.int32, (PACK, ROWS_E), 1) + i * ROWS_E

    def add_pack(b, _):
        match = lane == packed_id[b][:, 0:1]
        out_ref[...] = out_ref[...] + dot_tn(match.astype(BF16), packed[b])
        return 0

    lax.fori_loop(0, (count_ref[0] + PACK - 1) // PACK, add_pack, 0)


def emb_grad(n_stage, tok, dt, n_all, gx):
    rows, total = dt.shape
    mbs, mtok, dim = gx.shape
    whole = lambda shape: pl.BlockSpec(shape, lambda i: (0,) * len(shape))
    return pl.pallas_call(
        functools.partial(emb_grad_kernel, rows, n_stage),
        grid=(pl.cdiv(rows, ROWS_E),),
        out_shape=jax.ShapeDtypeStruct((rows, dim), F32),
        in_specs=[whole((mbs, mtok)), pl.BlockSpec((ROWS_E, total), lambda i: (i, 0)), whole((mbs, mtok, dim)), whole((mbs, mtok, dim))],
        out_specs=pl.BlockSpec((ROWS_E, dim), lambda i: (i, 0)),
        scratch_shapes=[
            pltpu.VMEM((total // PACK, PACK, dim), BF16),
            pltpu.VMEM((total // PACK, PACK, 128), jnp.int32),
            pltpu.SMEM((1,), jnp.int32),
        ],
        compiler_params=pltpu.CompilerParams(vmem_limit_bytes=50_000_000),
        name="emb_grad",
    )(tok, dt, n_all, gx)


def solution(mesh):
    n_stage = mesh.shape["stage"]

    def stage_body(token_ids, label_ids, emb_rows, w_in, w_out):
        stage_idx = lax.axis_index("stage")
        mbs, mtok = token_ids.shape
        rows, dim = emb_rows.shape
        ffn = w_in.shape[2]
        w1 = w_in[0]
        w2 = w_out[0]
        local_tok = token_ids - stage_idx * rows
        tok_here = (local_tok >= 0) & (local_tok < rows)
        looked_up = jnp.take(emb_rows, jnp.clip(local_tok, 0, rows - 1), axis=0)
        part = jnp.where(tok_here[..., None], looked_up, 0)

        pre, x_in, n_all, dt, dxl, loss = forward_head(n_stage, label_ids, part, emb_rows, w1, w2)
        hid, dpre, g_all, gx = backward(n_stage, w1, w2, pre.reshape(mbs, mtok, ffn), dxl)
        tokens = mbs * mtok
        grad_in = dot_tn(x_in.reshape(tokens, dim), dpre.reshape(tokens, ffn))
        grad_out = dot_tn(hid.reshape(tokens, ffn), g_all.reshape(tokens, dim))
        grad_emb = emb_grad(n_stage, token_ids, dt, n_all, gx)
        mean_loss = (loss[0, 0] / tokens).reshape(1)
        return mean_loss, grad_in[None], grad_out[None], grad_emb

    return jax.shard_map(
        stage_body,
        mesh=mesh,
        in_specs=(P("dp", None), P("dp", None), P("stage", None), P("stage", None, None), P("stage", None, None)),
        out_specs=(P("dp"), P(("dp", "stage"), None, None), P(("dp", "stage"), None, None), P(("dp", "stage"), None)),
        check_vma=False,
    )
```

```python
import functools
import math

import jax
import jax.numpy as jnp
from jax import lax
from jax.experimental import pallas as pl
from jax.experimental.pallas import tpu as pltpu
from jax.sharding import PartitionSpec as P

NORM_EPS = 1e-6
MESH = pl.DeviceIdType.MESH
F32 = jnp.float32
BF16 = jnp.bfloat16
GELU_A = math.sqrt(2.0 / math.pi)
GELU_B = 0.044715
LOG2E = math.log2(math.e)
CHUNK = 128
HEAD_MBS = 2
VMEM_LIMIT = 67_000_000


def dot_nn(a, b):
    return lax.dot_general(a, b, (((1,), (0,)), ((), ())), preferred_element_type=F32)


def dot_nt(a, b):
    return lax.dot_general(a, b, (((1,), (1,)), ((), ())), preferred_element_type=F32)


def dot_tn(a, b):
    return lax.dot_general(a, b, (((0,), (0,)), ((), ())), preferred_element_type=F32)


def gelu_and_slope(pre):
    sq = pre * pre
    th = jnp.tanh(pre * (GELU_A + (GELU_A * GELU_B) * sq))
    half_sum = 0.5 + 0.5 * th
    hid = pre * half_sum
    slope = half_sum + (hid - hid * th) * (GELU_A + (3.0 * GELU_A * GELU_B) * sq)
    return hid, slope


def norm_scale(x_f32):
    return lax.rsqrt(jnp.mean(x_f32 * x_f32, axis=-1, keepdims=True) + NORM_EPS)


def remote(src, dst, send_sem, recv_sem, stage):
    return pltpu.make_async_remote_copy(
        src_ref=src, dst_ref=dst, send_sem=send_sem, recv_sem=recv_sem, device_id={"stage": stage}, device_id_type=MESH
    )


def group_barrier(stage, n_stage):
    barrier = pltpu.get_barrier_semaphore()
    for off in range(1, n_stage):
        pl.semaphore_signal(barrier, inc=1, device_id={"stage": lax.rem(stage + off, n_stage)}, device_id_type=MESH)
    pl.semaphore_wait(barrier, n_stage - 1)


def vocab_tile(rows):
    for parts in range(2, rows + 1):
        if rows % parts == 0 and (rows // parts) % 16 == 0 and rows // parts <= 2400:
            return rows // parts
    return rows


def sub_blocks(rows, size):
    return [(start, min(size, rows - start)) for start in range(0, rows, size)]


def forward_chunk(x, w1, w2, slope_slot, hid_slot):
    ffn = w1.shape[1]
    width = ffn // 4
    for part in range(4):
        cols = pl.ds(part * width, width)
        hid, slope = gelu_and_slope(dot_nn(x, w1[:, cols]))
        slope_slot[:, cols] = slope
        hid_slot[:, cols] = hid.astype(BF16)
    return x.astype(F32) + dot_nn(hid_slot[...], w2[...])


def backward_chunk(grad, wt, slope_slot, dpre_slot):
    ffn = slope_slot.shape[1]
    dim = grad.shape[1]
    for part in range(ffn // dim):
        cols = pl.ds(part * dim, dim)
        d_hid = dot_nn(grad, wt[pl.ds(ffn + part * dim, dim), :])
        dpre_slot[:, cols] = (d_hid * slope_slot[:, cols]).astype(BF16)
    return grad.astype(F32) + dot_nn(dpre_slot[...], wt[pl.ds(0, ffn), :])


def transpose_weights(w1, w2, wt):
    dim, ffn = w1.shape
    for part in range(ffn // dim):
        at = pl.ds(part * dim, dim)
        wt[at, :] = w1[:, at].T
        wt[pl.ds(ffn + part * dim, dim), :] = w2[at, :].T


def head_logits(n_t, emb, logits, lab_row, tokens):
    rows = emb.shape[0]
    tile = vocab_tile(rows)
    c2 = LOG2E * emb.shape[1] ** -0.5

    def tile_step(idx, carry):
        mx, sm, lb = carry
        base = pl.multiple_of(idx * tile, 16)
        for start, size in sub_blocks(tile, 256):
            at = pl.ds(base + start, size)
            block = dot_nn(emb[at, :], n_t[...])
            logits[at, :] = block
            b3 = block.reshape(size // 8, 8, tokens)
            row_ids = lax.broadcasted_iota(jnp.int32, (size, tokens), 0) + (base + start)
            hit = jnp.where(row_ids == lab_row, block, 0.0).reshape(size // 8, 8, tokens)
            mx_new = jnp.maximum(mx, jnp.max(b3, axis=0))
            sm = sm * jnp.exp2((mx - mx_new) * c2) + jnp.sum(jnp.exp2((b3 - mx_new[None]) * c2), axis=0)
            lb = lb + jnp.sum(hit, axis=0)
            mx = mx_new
        return mx, sm, lb

    init = (jnp.full((8, tokens), -3.0e38, F32), jnp.zeros((8, tokens), F32), jnp.zeros((8, tokens), F32))
    mx, sm, lb = lax.fori_loop(0, rows // tile, tile_step, init)
    top = jnp.max(mx, axis=0, keepdims=True)
    tot = jnp.sum(sm * jnp.exp2((mx - top) * c2), axis=0, keepdims=True)
    lab = jnp.sum(lb, axis=0, keepdims=True)
    return top, tot, lab


def head_grad_tile(base, size_all, emb, logits, d_slot, lab_row, top, shift, tokens):
    scale = emb.shape[1] ** -0.5
    c2 = LOG2E * scale
    total = None
    for start, size in sub_blocks(size_all, 256):
        at = pl.ds(base + start, size)
        row_ids = lax.broadcasted_iota(jnp.int32, (size, tokens), 0) + (base + start)
        prob = jnp.exp2((logits[at, :] - top) * c2 - shift)
        d_log = (prob - jnp.where(row_ids == lab_row, scale, 0.0)).astype(BF16)
        d_slot[pl.ds(start, size), :] = d_log
        part = dot_tn(d_log, emb[at, :])
        total = part if total is None else total + part
    return total


E_ROWS = 512
LOOKUP_LEAD = 1
LOOKUP_PARENT = {2: (3, 0), 1: (0, 0), 4: (5, 0), 6: (7, 0), 5: (3, 1), 7: (0, 1), 3: (0, 2)}
GRAD_PARENT = {0: (1, 0), 2: (3, 0), 4: (5, 0), 1: (6, 0), 6: (7, 0), 3: (5, 1), 5: (7, 1)}


def step_kernel(
    n_stage, lab_ref, part_hbm, emb_hbm, w1_hbm, w2_hbm,
    slope_out, hid_out, dpre_out, xin_out, n_out, g_out, gx_out, dt_out, ge_out, loss_out,
    emb, w1, w2, x_in, x_out, n_all, comb, buf_a, buf_b, slope_stg, act_stg, stats, loss_acc,
    load_sem, part_sem, lk_send, lk_a, lk_b, lk_c, x_send, x_recv, n_send, n_recv, st_send, st_recv,
    g_send, g_a, g_b, b_send, b_recv, gx_send, gx_recv, slope_sem, act_sem, d_sem, e_sem, out_sem, gx_sem,
):
    s = lax.axis_index("stage")
    last = n_stage - 1
    mbs, mtok, dim = x_in.shape
    n_half = mtok // CHUNK
    n_chunks = mbs * n_half
    rows = emb.shape[0]
    ffn = w1.shape[1]
    tile = vocab_tile(rows)
    tokens = HEAD_MBS * mtok
    rounds = mbs // HEAD_MBS
    scale = dim ** -0.5
    c2 = LOG2E * scale
    row_start = s * rows
    bufs = (buf_a, buf_b, x_in)
    lk_sems = (lk_a, lk_b, lk_c)

    loads = [pltpu.make_async_copy(src, dst, load_sem.at[i])
             for i, (src, dst) in enumerate([(w1_hbm, w1), (w2_hbm, w2), (emb_hbm, emb)])]
    for mb in range(mbs):
        pltpu.make_async_copy(part_hbm.at[mb], comb.at[mb], part_sem.at[mb]).start()
    for ld in loads:
        ld.start()
    group_barrier(s, n_stage)

    def pos(c):
        return (c // n_half, pl.ds(pl.multiple_of(lax.rem(c, n_half) * CHUNK, CHUNK), CHUNK))

    def at_chunk(ref, c):
        return ref.at[c // n_half, pl.ds(pl.multiple_of(lax.rem(c, n_half) * CHUNK, CHUNK), CHUNK)]

    def loop(lo, hi, fn):
        def body(i, _):
            fn(i)
            return 0
        lax.fori_loop(lo, hi, body, 0)

    def chunks_of(mb, fn):
        loop(mb * n_half, (mb + 1) * n_half, fn)

    def each_role(roles, fn):
        for node in roles:
            @pl.when(s == node)
            def _(node=node):
                fn(node)

    def lk_copy(c, child):
        parent, slot = LOOKUP_PARENT[child]
        return remote(at_chunk(comb, c), at_chunk(bufs[slot], c), lk_send.at[c], lk_sems[slot].at[c], parent)

    def lk_total(c, slots):
        total = comb[pos(c)].astype(F32)
        for slot in range(slots):
            remote(at_chunk(comb, c), at_chunk(bufs[slot], c), lk_send.at[c], lk_sems[slot].at[c], 0).wait_recv()
            total = total + bufs[slot][pos(c)].astype(F32)
        return total.astype(BF16)

    def lk_forward(c, node, slots):
        comb[pos(c)] = lk_total(c, slots)
        lk_copy(c, node).start()

    loop(0, mbs, lambda mb: pltpu.make_async_copy(part_hbm.at[mb], comb.at[mb], part_sem.at[mb]).wait())
    each_role((1, 2, 4, 6), lambda node: loop(0, n_chunks, lambda c: lk_copy(c, node).start()))
    each_role((5, 7), lambda node: loop(0, n_chunks, lambda c: lk_forward(c, node, 1)))
    loads[0].wait()
    loads[1].wait()

    n_routes = {last: (5, 1, 6), 5: (4,), 1: (3, 0), 3: (2,)}

    def x_copy(c, dst_stage):
        return remote(at_chunk(x_out, c), at_chunk(x_in, c), x_send.at[c], x_recv.at[c], dst_stage)

    def n_copy(c, lane, dst_stage):
        return remote(at_chunk(n_all, c), at_chunk(n_all, c), n_send.at[lane, c], n_recv.at[c], dst_stage)

    def fwd_copies(c):
        slot = lax.rem(c, 2)
        return (pltpu.make_async_copy(slope_stg.at[slot], slope_out.at[c], slope_sem.at[slot]),
                pltpu.make_async_copy(act_stg.at[slot], hid_out.at[c], act_sem.at[slot]))

    def fwd_chunk(c):
        idx = pos(c)

        @pl.when(s == 0)
        def _():
            x_in[idx] = lk_total(c, 3)

        @pl.when(s > 0)
        def _():
            x_copy(c, 0).wait_recv()

        @pl.when(c >= 2)
        def _():
            for cp in fwd_copies(c - 2):
                cp.wait()

        slot = lax.rem(c, 2)
        out = forward_chunk(x_in[idx], w1, w2, slope_stg.at[slot], act_stg.at[slot]).astype(BF16)
        x_out[idx] = out
        for cp in fwd_copies(c):
            cp.start()

        @pl.when(s < last)
        def _():
            x_copy(c, s + 1).start()

        @pl.when(s == last)
        def _():
            out_f = out.astype(F32)
            n_all[idx] = (out_f * norm_scale(out_f)).astype(BF16)
            for lane, dst in enumerate(n_routes[last]):
                n_copy(c, lane, dst).start()

    def n_round(r, fn):
        loop(r * HEAD_MBS * n_half, (r + 1) * HEAD_MBS * n_half, fn)

    def n_early(r):
        def take(c, node):
            n_copy(c, 0, 0 if node == last else last).wait_recv()
            for lane, dst in enumerate(n_routes[node]):
                n_copy(c, lane, dst).start()
        each_role((1, 5), lambda node: n_round(r, lambda c: take(c, node)))

    def n_mid(r):
        def take(c, node):
            n_copy(c, 0, last).wait_recv()
            n_copy(c, 0, n_routes[node][0]).start()
        each_role((3,), lambda node: n_round(r, lambda c: take(c, node)))

    def n_late(r):
        @pl.when((lax.rem(s, 2) == 0))
        def _():
            n_round(r, lambda c: n_copy(c, 0, last).wait_recv())

    def g_copy(mb, child):
        parent, slot = GRAD_PARENT[child]
        return remote(comb.at[mb], bufs[slot].at[mb], g_send.at[mb], (g_a, g_b)[slot].at[mb], parent)

    def g_total(mb, slots):
        total = comb[mb].astype(F32)
        for slot in range(slots):
            remote(comb.at[mb], bufs[slot].at[mb], g_send.at[mb], (g_a, g_b)[slot].at[mb], 0).wait_recv()
            total = total + bufs[slot][mb].astype(F32)
        return total

    def g_forward(mb, node, slots):
        comb[mb] = g_total(mb, slots).astype(BF16)
        g_copy(mb, node).start()

    def g_low(r):
        each_role((1, 3), lambda node: loop(r * HEAD_MBS, (r + 1) * HEAD_MBS, lambda mb: g_forward(mb, node, 1)))

    def g_mid(r):
        each_role((6,), lambda node: loop(r * HEAD_MBS, (r + 1) * HEAD_MBS, lambda mb: g_forward(mb, node, 1)))
        each_role((5,), lambda node: loop(r * HEAD_MBS, (r + 1) * HEAD_MBS, lambda mb: g_forward(mb, node, 2)))

    def g_final(mb):
        @pl.when(s == last)
        def _():
            grad_n = g_total(mb, 2)
            x_f = x_out[mb].astype(F32)
            inv = norm_scale(x_f)
            n_f = x_f * inv
            dx = inv * (grad_n - n_f * jnp.mean(grad_n * n_f, axis=-1, keepdims=True))
            comb[mb] = dx.astype(BF16)

    def lab_row_of(r):
        parts = [lab_ref[pl.ds(r * HEAD_MBS + i, 1), :] for i in range(HEAD_MBS)]
        return jnp.concatenate(parts, axis=1) - row_start

    def st_copy(r, off):
        dst = lax.rem(s + off, n_stage)
        return remote(stats.at[r, s], stats.at[r, s], st_send.at[r, off], st_recv.at[r, off], dst)

    saves = [pltpu.make_async_copy(x_in, xin_out, out_sem.at[0]), pltpu.make_async_copy(n_all, n_out, out_sem.at[1])]

    def forward_and_head(logits, n_t, d_stg, gn_acc):
        n_tiles = rows // tile

        def head_a(r):
            n_late(r)

            @pl.when(r == rounds - 1)
            def _():
                for cp in saves:
                    cp.start()

            n_t[...] = n_all[pl.ds(r * HEAD_MBS, HEAD_MBS)].reshape(tokens, dim).T
            top, tot, lab = head_logits(n_t, emb, logits, lab_row_of(r), tokens)

            @pl.when(r == rounds - 1)
            def _():
                for cp in saves:
                    cp.wait()

                @pl.when(s < last)
                def _():
                    loop(0, n_chunks, lambda c: x_copy(c, 0).wait_send())
                for src, dsts in n_routes.items():
                    @pl.when(s == src)
                    def _(dsts=dsts):
                        loop(0, n_chunks, lambda c: [n_copy(c, lane, dst).wait_send() for lane, dst in enumerate(dsts)])
            stats[r, s] = jnp.concatenate([top, tot, lab, jnp.zeros((5, tokens), F32)], axis=0)
            for off in range(1, n_stage):
                st_copy(r, off).start()

        def d_copy(seq):
            slot = lax.rem(seq, 2)
            r = seq // n_tiles
            idx = lax.rem(seq, n_tiles)
            dst = dt_out.at[pl.ds(pl.multiple_of(idx * tile, 16), tile), pl.ds(pl.multiple_of(r * tokens, tokens), tokens)]
            return pltpu.make_async_copy(d_stg.at[slot], dst, d_sem.at[slot])

        def head_b(r):
            @pl.when(r + 1 < rounds)
            def _():
                n_early(r + 1)
            for off in range(1, n_stage):
                src = lax.rem(s + n_stage - off, n_stage)
                remote(stats.at[r, s], stats.at[r, src], st_send.at[r, off], st_recv.at[r, off], src).wait_recv()
            blocks = [stats[r, i] for i in range(n_stage)]
            top = blocks[0][0:1]
            for blk in blocks[1:]:
                top = jnp.maximum(top, blk[0:1])
            tot = jnp.zeros_like(top)
            lab = jnp.zeros_like(top)
            for blk in blocks:
                tot = tot + blk[1:2] * jnp.exp2((blk[0:1] - top) * c2)
                lab = lab + blk[2:3]
            loss_acc[...] = loss_acc[...] + (jnp.log(tot) + (top - lab) * scale)
            shift = jnp.log(tot) * LOG2E - math.log2(scale)
            lab_row = lab_row_of(r)

            def tile_step(idx):
                seq = r * n_tiles + idx

                @pl.when(seq >= 2)
                def _():
                    d_copy(seq - 2).wait()
                @pl.when((idx == n_tiles - 1) & (r + 1 < rounds))
                def _():
                    n_mid(r + 1)
                base = pl.multiple_of(idx * tile, 16)
                part = head_grad_tile(base, tile, emb, logits, d_stg.at[lax.rem(seq, 2)], lab_row, top, shift, tokens)
                gn_acc[...] = gn_acc[...] + part
                d_copy(seq).start()

            gn_acc[...] = jnp.zeros_like(gn_acc)
            loop(0, n_tiles, tile_step)
            comb[pl.ds(r * HEAD_MBS, HEAD_MBS)] = gn_acc[...].reshape(HEAD_MBS, mtok, dim).astype(BF16)
            each_role((0, 2, 4), lambda node: loop(r * HEAD_MBS, (r + 1) * HEAD_MBS, lambda mb: g_copy(mb, node).start()))
        loss_acc[...] = jnp.zeros_like(loss_acc)
        first_a = HEAD_MBS + 1 + last

        def step(k):
            @pl.when((s == 3) & (k == 0))
            def _():
                loop(0, LOOKUP_LEAD * n_half, lambda c: lk_forward(c, 3, 2))

            @pl.when((s == 3) & (k + LOOKUP_LEAD < mbs))
            def _():
                chunks_of(k + LOOKUP_LEAD, lambda c: lk_forward(c, 3, 2))

            f_mb = k - s

            @pl.when((f_mb >= 0) & (f_mb < mbs))
            def _():
                chunks_of(f_mb, fwd_chunk)

            @pl.when(k == first_a)
            def _():
                loads[2].wait()

                @pl.when(s > 0)
                def _():
                    loop(0, n_chunks, lambda c: lk_copy(c, 1).wait_send())

            rel = k - first_a
            r = rel // HEAD_MBS
            even = lax.rem(rel + HEAD_MBS * n_stage, HEAD_MBS) == 0

            @pl.when(k == first_a)
            def _():
                n_early(0)
                n_mid(0)

            @pl.when(even & (rel >= 0))
            def _():
                head_a(r)

            @pl.when(even & (rel >= HEAD_MBS))
            def _():
                g_low(r - 1)

                @pl.when(r >= 2)
                def _():
                    loop((r - 2) * HEAD_MBS, (r - 1) * HEAD_MBS, g_final)

            @pl.when(jnp.logical_not(even) & (rel >= 0))
            def _():
                head_b(r)

            @pl.when(jnp.logical_not(even) & (rel >= HEAD_MBS))
            def _():
                g_mid(r - 1)

        loop(0, first_a + HEAD_MBS * rounds, step)
        for c in (n_chunks - 2, n_chunks - 1):
            for cp in fwd_copies(c):
                cp.wait()
        for seq in (rounds * n_tiles - 2, rounds * n_tiles - 1):
            d_copy(seq).wait()

    pl.run_scoped(
        forward_and_head,
        pltpu.VMEM((rows, tokens), F32), pltpu.VMEM((dim, tokens), BF16),
        pltpu.VMEM((2, tile, tokens), BF16), pltpu.VMEM((tokens, dim), F32),
    )
    loss_out[...] = jnp.broadcast_to(jnp.sum(loss_acc[...], axis=1, keepdims=True), loss_out.shape)

    g_in, g_buf, gx, wt = x_in, x_out, n_all, emb

    def b_copy(c, dst):
        return remote(at_chunk(g_buf, c), at_chunk(g_in, c), b_send.at[c], b_recv.at[c], dst)

    def gx_copy(c, lane, dst):
        return remote(at_chunk(gx, c), at_chunk(gx, c), gx_send.at[lane, c], gx_recv.at[c], dst)

    def slope_copy(c):
        slot = lax.rem(c, 2)
        return pltpu.make_async_copy(slope_out.at[c], slope_stg.at[slot], slope_sem.at[slot])

    def dpre_copy(c):
        slot = lax.rem(c, 2)
        return pltpu.make_async_copy(act_stg.at[slot], dpre_out.at[c], act_sem.at[slot])

    gx_split = n_chunks // 2
    gx_routes = {0: ((3, 0, n_chunks), (last, 0, n_chunks), (1, 0, n_chunks)), 3: ((2, 0, n_chunks), (5, 0, gx_split)),
                 last: ((6, 0, n_chunks), (5, gx_split, n_chunks)), 5: ((4, 0, n_chunks),)}

    def gx_send_all(c, node):
        for lane, (dst, lo, hi) in enumerate(gx_routes[node]):
            @pl.when((c >= lo) & (c < hi))
            def _(lane=lane, dst=dst):
                gx_copy(c, lane, dst).start()


    def bwd_chunk(c):
        slot = lax.rem(c, 2)
        idx = pos(c)

        @pl.when(s < last)
        def _():
            b_copy(c, 0).wait_recv()

        @pl.when(s == last)
        def _():
            g_in[idx] = comb[idx]

        @pl.when(c >= 2)
        def _():
            dpre_copy(c - 2).wait()
        slope_copy(c).wait()
        dx = backward_chunk(g_in[idx], wt, slope_stg.at[slot], act_stg.at[slot]).astype(BF16)

        @pl.when(s > 0)
        def _():
            g_buf[idx] = dx
            b_copy(c, s - 1).start()

        @pl.when(s == 0)
        def _():
            gx[idx] = dx
            gx_send_all(c, 0)
        dpre_copy(c).start()

        @pl.when(c + 2 < n_chunks)
        def _():
            slope_copy(c + 2).start()

    full = rows // E_ROWS
    rest = rows - full * E_ROWS

    def backward(n_rows, d_in, e_stg):
        def d_load(i, size=E_ROWS):
            slot = lax.rem(i, 2)
            src = dt_out.at[pl.ds(pl.multiple_of(i * E_ROWS, E_ROWS), size)]
            return pltpu.make_async_copy(src, d_in.at[slot, pl.ds(0, size)], d_sem.at[slot])

        def e_save(i, size=E_ROWS):
            slot = lax.rem(i, 2)
            dst = ge_out.at[pl.ds(pl.multiple_of(i * E_ROWS, E_ROWS), size)]
            return pltpu.make_async_copy(e_stg.at[slot, pl.ds(0, size)], dst, e_sem.at[slot])

        def e_tile(i):
            slot = lax.rem(i, 2)

            @pl.when(i + 1 < full)
            def _():
                d_load(i + 1).start()
            if rest:
                @pl.when(i + 1 == full)
                def _():
                    d_load(full, rest).start()
            d_load(i).wait()

            @pl.when(i >= 2)
            def _():
                e_save(i - 2).wait()
            e_stg[slot] = dot_nn(d_in[slot], n_rows[...].reshape(mbs * mtok, dim))
            e_save(i).start()

        n_load = pltpu.make_async_copy(n_out, n_rows, out_sem.at[1])
        n_load.start()
        slope_copy(0).start()
        slope_copy(1).start()
        d_load(0).start()
        g_low(rounds - 1)
        transpose_weights(w1, w2, wt)
        n_load.wait()
        early = jnp.minimum((last - s) * 2, full)
        loop(0, early, e_tile)

        def gx_save(c):
            return pltpu.make_async_copy(at_chunk(gx, c), at_chunk(gx_out, c), gx_sem.at[c])

        def gx_forward(c):
            @pl.when(s > 0)
            def _():
                gx_copy(c, 0, 0).wait_recv()
            each_role((3, last, 5), lambda node: gx_send_all(c, node))
            gx_save(c).start()

        def step(k):
            @pl.when(k >= mbs - 2 * HEAD_MBS)
            def _():
                @pl.when(k < mbs)
                def _():
                    g_final(k)
            b_mb = k - (last - s)

            @pl.when((b_mb >= 0) & (b_mb < mbs))
            def _():
                chunks_of(b_mb, bwd_chunk)

            @pl.when(k == 2)
            def _():
                g_mid(rounds - 1)

            x_mb = k - n_stage

            @pl.when((s == 3) & (x_mb >= 0) & (x_mb < gx_split // n_half))
            def _():
                chunks_of(x_mb, gx_forward)

        loop(0, mbs + last, step)
        g_save = pltpu.make_async_copy(g_in, g_out, out_sem.at[0])
        g_save.start()
        loop(early, full, e_tile)
        loop(jnp.where(s == 3, gx_split, 0), n_chunks, gx_forward)
        if rest:
            d_load(full, rest).wait()
            e_save(full - 2).wait()
            slot = full % 2
            e_stg[slot, pl.ds(0, rest)] = dot_nn(d_in[slot, pl.ds(0, rest)], n_rows[...].reshape(mbs * mtok, dim))
            e_save(full, rest).start()

        g_save.wait()
        if rest:
            e_save(full - 1).wait()
            e_save(full, rest).wait()
        else:
            e_save(full - 2).wait()
            e_save(full - 1).wait()
        for c in (n_chunks - 2, n_chunks - 1):
            dpre_copy(c).wait()
        loop(0, n_chunks, lambda c: gx_save(c).wait())

    pl.run_scoped(
        backward,
        pltpu.VMEM((mbs, mtok, dim), BF16), pltpu.VMEM((2, E_ROWS, mbs * mtok), BF16), pltpu.VMEM((2, E_ROWS, dim), F32),
    )

    @pl.when(s < last)
    def _():
        loop(0, mbs, lambda mb: g_copy(mb, 1).wait_send())

    @pl.when(s > 0)
    def _():
        loop(0, n_chunks, lambda c: b_copy(c, 0).wait_send())
    for src, routes in gx_routes.items():
        @pl.when(s == src)
        def _(routes=routes):
            for lane, (dst, lo, hi) in enumerate(routes):
                loop(lo, hi, lambda c: gx_copy(c, lane, dst).wait_send())
    loop(0, rounds, lambda r: [st_copy(r, off).wait_send() for off in range(1, n_stage)])


def pipeline_step(n_stage, labels, part, emb, w1, w2):
    mbs, mtok, dim = part.shape
    rows = emb.shape[0]
    ffn = w1.shape[1]
    chunks = mbs * mtok // CHUNK
    rounds = mbs // HEAD_MBS
    tokens = HEAD_MBS * mtok
    any_spec = pl.BlockSpec(memory_space=pl.ANY)
    vmem_spec = pl.BlockSpec(memory_space=pltpu.VMEM)
    act = pltpu.VMEM((mbs, mtok, dim), BF16)
    dma = pltpu.SemaphoreType.DMA
    act_shape = jax.ShapeDtypeStruct((mbs, mtok, dim), BF16)
    hid_shape = jax.ShapeDtypeStruct((chunks, CHUNK, ffn), BF16)
    return pl.pallas_call(
        functools.partial(step_kernel, n_stage),
        out_shape=(
            jax.ShapeDtypeStruct((chunks, CHUNK, ffn), F32), hid_shape, hid_shape,
            act_shape, act_shape, act_shape, act_shape,
            jax.ShapeDtypeStruct((rows, mbs * mtok), BF16),
            jax.ShapeDtypeStruct((rows, dim), F32),
            jax.ShapeDtypeStruct((8, 128), F32),
        ),
        in_specs=[vmem_spec] + [any_spec] * 4,
        out_specs=(any_spec,) * 9 + (vmem_spec,),
        scratch_shapes=[
            pltpu.VMEM((rows, dim), BF16), pltpu.VMEM((dim, ffn), BF16), pltpu.VMEM((ffn, dim), BF16),
            act, act, act, act, act, act,
            pltpu.VMEM((2, CHUNK, ffn), F32), pltpu.VMEM((2, CHUNK, ffn), BF16),
            pltpu.VMEM((rounds, n_stage, 8, tokens), F32), pltpu.VMEM((1, tokens), F32),
            dma((3,)), dma((mbs,)), dma((chunks,)), dma((chunks,)), dma((chunks,)), dma((chunks,)),
            dma((chunks,)), dma((chunks,)), dma((3, chunks)), dma((chunks,)),
            dma((rounds, n_stage)), dma((rounds, n_stage)), dma((mbs,)), dma((mbs,)), dma((mbs,)),
            dma((chunks,)), dma((chunks,)), dma((3, chunks)), dma((chunks,)),
            dma((2,)), dma((2,)), dma((2,)), dma((2,)), dma((2,)), dma((chunks,)),
        ],
        compiler_params=pltpu.CompilerParams(collective_id=0, has_side_effects=True, vmem_limit_bytes=VMEM_LIMIT),
        name="pipeline_step",
    )(labels, part, emb, w1, w2)


PACK = 256
TAIL_STEPS = 12


def tail_kernel(
    rows, tok_ref, x_hbm, g_hbm, gx_hbm, dpre_ref, hid_ref, ge_ref,
    g1_ref, g2_ref, out_ref,
    x_buf, g_buf, x_t, packed, packed_id, count_ref, sem,
):
    i = pl.program_id(0)
    mbs, mtok = tok_ref.shape
    total, dim = g_buf.shape
    n_pack = total // PACK
    e_rows = out_ref.shape[0]
    x_load = pltpu.make_async_copy(x_hbm, x_buf, sem.at[0])
    g_load = pltpu.make_async_copy(g_hbm, g_buf, sem.at[1])
    gx_load = pltpu.make_async_copy(gx_hbm, x_buf, sem.at[2])

    @pl.when(i == 0)
    def _():
        x_load.start()
        g_load.start()
        x_load.wait()
        x_t[...] = x_buf[...].T
        gx_load.start()
        g_load.wait()

        s = lax.axis_index("stage")
        loc = tok_ref[...] - s * rows
        here = (loc >= 0) & (loc < rows)
        flag = here.astype(F32)
        upper = (lax.broadcasted_iota(jnp.int32, (mtok, mtok), 0) <= lax.broadcasted_iota(jnp.int32, (mtok, mtok), 1))
        within = dot_nn(flag.astype(BF16), upper.astype(BF16))
        total_row = jnp.sum(flag, axis=1, keepdims=True)
        lower = (lax.broadcasted_iota(jnp.int32, (mbs, mbs), 1) < lax.broadcasted_iota(jnp.int32, (mbs, mbs), 0))
        before = jnp.sum(jnp.where(lower, jnp.transpose(jnp.broadcast_to(total_row, (mbs, mbs))), 0.0), axis=1, keepdims=True)
        slot_of = jnp.where(here, within - 1.0 + before, -1.0).astype(jnp.int32)
        count = jnp.sum(flag).astype(jnp.int32)
        count_ref[0] = count
        gx_load.wait()

        for b in range(n_pack):
            @pl.when(b * PACK < jnp.maximum(count, 1))
            def _(b=b):
                slot = lax.broadcasted_iota(jnp.int32, (PACK, mtok), 0) + b * PACK
                acc = jnp.zeros((PACK, dim), F32)
                ids = jnp.zeros((PACK, 1), F32)
                for mb in range(mbs):
                    pick = slot == slot_of[mb:mb + 1, :]
                    acc = acc + dot_nn(pick.astype(BF16), x_buf[pl.ds(mb * mtok, mtok), :])
                    ids = ids + jnp.sum(jnp.where(pick, loc[mb:mb + 1, :].astype(F32), 0.0), axis=1, keepdims=True)
                filled = lax.broadcasted_iota(jnp.int32, (PACK, 1), 0) + b * PACK < count
                packed[b] = acc.astype(BF16)
                packed_id[b] = jnp.broadcast_to(jnp.where(filled, ids.astype(jnp.int32), -1), (PACK, 128))

    g1_ref[0] = dot_nn(x_t[...], dpre_ref[...])
    g2_ref[0] = dot_tn(hid_ref[...], g_buf[...])
    lane = lax.broadcasted_iota(jnp.int32, (PACK, e_rows), 1) + i * e_rows

    def match_of(b):
        return (lane == packed_id[b][:, 0:1]).astype(BF16)

    out_ref[...] = ge_ref[...] + dot_tn(match_of(0), packed[0])

    def add_pack(b, _):
        out_ref[...] = out_ref[...] + dot_tn(match_of(b), packed[b])
        return 0

    lax.fori_loop(1, (count_ref[0] + PACK - 1) // PACK, add_pack, 0)


def tail(tok, x, g, gx, dpre, hid, ge):
    rows, dim = ge.shape
    total, ffn = dpre.shape
    mbs, mtok = tok.shape
    width = ffn // TAIL_STEPS
    e_rows = -(-rows // (TAIL_STEPS * 16)) * 16
    any_spec = pl.BlockSpec(memory_space=pl.ANY)
    dma = pltpu.SemaphoreType.DMA
    return pl.pallas_call(
        functools.partial(tail_kernel, rows),
        grid=(TAIL_STEPS,),
        out_shape=(
            jax.ShapeDtypeStruct((1, dim, ffn), F32),
            jax.ShapeDtypeStruct((1, ffn, dim), F32),
            jax.ShapeDtypeStruct((rows, dim), F32),
        ),
        in_specs=[
            pl.BlockSpec((mbs, mtok), lambda i: (0, 0)), any_spec, any_spec, any_spec,
            pl.BlockSpec((total, width), lambda i: (0, i)),
            pl.BlockSpec((total, width), lambda i: (0, i)),
            pl.BlockSpec((e_rows, dim), lambda i: (i, 0)),
        ],
        out_specs=(
            pl.BlockSpec((1, dim, width), lambda i: (0, 0, i)),
            pl.BlockSpec((1, width, dim), lambda i: (0, i, 0)),
            pl.BlockSpec((e_rows, dim), lambda i: (i, 0)),
        ),
        scratch_shapes=[
            pltpu.VMEM((total, dim), BF16), pltpu.VMEM((total, dim), BF16), pltpu.VMEM((dim, total), BF16),
            pltpu.VMEM((total // PACK, PACK, dim), BF16), pltpu.VMEM((total // PACK, PACK, 128), jnp.int32),
            pltpu.SMEM((1,), jnp.int32), dma((3,)),
        ],
        compiler_params=pltpu.CompilerParams(vmem_limit_bytes=60_000_000),
        name="tail",
    )(tok, x, g, gx, dpre, hid, ge)


def solution(mesh):
    n_stage = mesh.shape["stage"]

    def stage_body(token_ids, label_ids, emb_rows, w_in, w_out):
        stage_idx = lax.axis_index("stage")
        mbs, mtok = token_ids.shape
        rows, dim = emb_rows.shape
        ffn = w_in.shape[2]
        tokens = mbs * mtok
        local_tok = token_ids - stage_idx * rows
        tok_here = (local_tok >= 0) & (local_tok < rows)
        looked_up = jnp.take(emb_rows, jnp.clip(local_tok, 0, rows - 1), axis=0)
        part = jnp.where(tok_here[..., None], looked_up, 0)

        _, hid, dpre, x_in, _, g_all, gx, _, ge, loss = pipeline_step(n_stage, label_ids, part, emb_rows, w_in[0], w_out[0])
        flat = lambda a: a.reshape(tokens, a.shape[-1])
        grad_in, grad_out, grad_emb = tail(token_ids, flat(x_in), flat(g_all), flat(gx), flat(dpre), flat(hid), ge)
        mean_loss = (loss[0, 0] / tokens).reshape(1)
        return mean_loss, grad_in, grad_out, grad_emb

    return jax.shard_map(
        stage_body,
        mesh=mesh,
        in_specs=(P("dp", None), P("dp", None), P("stage", None), P("stage", None, None), P("stage", None, None)),
        out_specs=(P("dp"), P(("dp", "stage"), None, None), P(("dp", "stage"), None, None), P(("dp", "stage"), None)),
        check_vma=False,
    )
```

```python
import functools
import math

import jax
import jax.numpy as jnp
from jax import lax
from jax.experimental import pallas as pl
from jax.experimental.pallas import tpu as pltpu
from jax.sharding import PartitionSpec as P

NORM_EPS = 1e-6
MESH = pl.DeviceIdType.MESH
F32 = jnp.float32
BF16 = jnp.bfloat16
GELU_A = math.sqrt(2.0 / math.pi)
GELU_B = 0.044715
LOG2E = math.log2(math.e)
CHUNK = 128
HEAD_MBS = 2
VMEM_LIMIT = 67_000_000


def dot_nn(a, b):
    return lax.dot_general(a, b, (((1,), (0,)), ((), ())), preferred_element_type=F32)


def dot_nt(a, b):
    return lax.dot_general(a, b, (((1,), (1,)), ((), ())), preferred_element_type=F32)


def dot_tn(a, b):
    return lax.dot_general(a, b, (((0,), (0,)), ((), ())), preferred_element_type=F32)


def gelu_and_slope(pre):
    sq = pre * pre
    th = jnp.tanh(pre * (GELU_A + (GELU_A * GELU_B) * sq))
    half_sum = 0.5 + 0.5 * th
    hid = pre * half_sum
    slope = half_sum + (hid - hid * th) * (GELU_A + (3.0 * GELU_A * GELU_B) * sq)
    return hid, slope


def norm_scale(x_f32):
    return lax.rsqrt(jnp.mean(x_f32 * x_f32, axis=-1, keepdims=True) + NORM_EPS)


def remote(src, dst, send_sem, recv_sem, stage):
    return pltpu.make_async_remote_copy(
        src_ref=src, dst_ref=dst, send_sem=send_sem, recv_sem=recv_sem, device_id={"stage": stage}, device_id_type=MESH
    )


def group_barrier(stage, n_stage):
    barrier = pltpu.get_barrier_semaphore()
    for off in range(1, n_stage):
        pl.semaphore_signal(barrier, inc=1, device_id={"stage": lax.rem(stage + off, n_stage)}, device_id_type=MESH)
    pl.semaphore_wait(barrier, n_stage - 1)


def vocab_tile(rows):
    for parts in range(2, rows + 1):
        if rows % parts == 0 and (rows // parts) % 16 == 0 and rows // parts <= 2400:
            return rows // parts
    return rows


def sub_blocks(rows, size):
    return [(start, min(size, rows - start)) for start in range(0, rows, size)]


def forward_chunk(x, w1, w2, slope_slot, hid_slot):
    ffn = w1.shape[1]
    width = ffn // 4
    for part in range(4):
        cols = pl.ds(part * width, width)
        hid, slope = gelu_and_slope(dot_nn(x, w1[:, cols]))
        slope_slot[:, cols] = slope
        hid_slot[:, cols] = hid.astype(BF16)
    return x.astype(F32) + dot_nn(hid_slot[...], w2[...])


def backward_chunk(grad, wt, slope_slot, dpre_slot):
    ffn = slope_slot.shape[1]
    dim = grad.shape[1]
    for part in range(ffn // dim):
        cols = pl.ds(part * dim, dim)
        d_hid = dot_nn(grad, wt[pl.ds(ffn + part * dim, dim), :])
        dpre_slot[:, cols] = (d_hid * slope_slot[:, cols]).astype(BF16)
    return grad.astype(F32) + dot_nn(dpre_slot[...], wt[pl.ds(0, ffn), :])


def transpose_weights(w1, w2, wt):
    dim, ffn = w1.shape
    for part in range(ffn // dim):
        at = pl.ds(part * dim, dim)
        wt[at, :] = w1[:, at].T
        wt[pl.ds(ffn + part * dim, dim), :] = w2[at, :].T


def head_logits(n_t, emb, logits, lab_row, tokens):
    rows = emb.shape[0]
    tile = vocab_tile(rows)
    c2 = LOG2E * emb.shape[1] ** -0.5

    def tile_step(idx, carry):
        mx, sm, lb = carry
        base = pl.multiple_of(idx * tile, 16)
        for start, size in sub_blocks(tile, 256):
            at = pl.ds(base + start, size)
            block = dot_nn(emb[at, :], n_t[...])
            logits[at, :] = block
            b3 = block.reshape(size // 8, 8, tokens)
            row_ids = lax.broadcasted_iota(jnp.int32, (size, tokens), 0) + (base + start)
            hit = jnp.where(row_ids == lab_row, block, 0.0).reshape(size // 8, 8, tokens)
            mx_new = jnp.maximum(mx, jnp.max(b3, axis=0))
            sm = sm * jnp.exp2((mx - mx_new) * c2) + jnp.sum(jnp.exp2((b3 - mx_new[None]) * c2), axis=0)
            lb = lb + jnp.sum(hit, axis=0)
            mx = mx_new
        return mx, sm, lb

    init = (jnp.full((8, tokens), -3.0e38, F32), jnp.zeros((8, tokens), F32), jnp.zeros((8, tokens), F32))
    mx, sm, lb = lax.fori_loop(0, rows // tile, tile_step, init)
    top = jnp.max(mx, axis=0, keepdims=True)
    tot = jnp.sum(sm * jnp.exp2((mx - top) * c2), axis=0, keepdims=True)
    lab = jnp.sum(lb, axis=0, keepdims=True)
    return top, tot, lab


def head_grad_tile(base, size_all, emb, logits, d_slot, lab_row, top, shift, tokens):
    scale = emb.shape[1] ** -0.5
    c2 = LOG2E * scale
    total = None
    for start, size in sub_blocks(size_all, 256):
        at = pl.ds(base + start, size)
        row_ids = lax.broadcasted_iota(jnp.int32, (size, tokens), 0) + (base + start)
        prob = jnp.exp2((logits[at, :] - top) * c2 - shift)
        d_log = (prob - jnp.where(row_ids == lab_row, scale, 0.0)).astype(BF16)
        d_slot[pl.ds(start, size), :] = d_log
        part = dot_tn(d_log, emb[at, :])
        total = part if total is None else total + part
    return total


LOOK = 160


def look_at(w):
    return pl.ds(w * LOOK if isinstance(w, int) else pl.multiple_of(w * LOOK, 16), LOOK)


def ranks(flag, upper, lower):
    within = dot_nn(flag.astype(BF16), upper)
    total = jnp.sum(flag, axis=1, keepdims=True)
    rows = flag.shape[0]
    before = jnp.sum(jnp.where(lower, jnp.transpose(jnp.broadcast_to(total, (rows, rows))), 0.0), axis=1, keepdims=True)
    return within - flag + before, jnp.sum(flag).astype(jnp.int32)


def triangles(mbs, mtok):
    upper = (lax.broadcasted_iota(jnp.int32, (mtok, mtok), 0)
             <= lax.broadcasted_iota(jnp.int32, (mtok, mtok), 1)).astype(BF16)
    lower = lax.broadcasted_iota(jnp.int32, (mbs, mbs), 1) < lax.broadcasted_iota(jnp.int32, (mbs, mbs), 0)
    return upper, lower


def lookup_kernel(tok_ref, emb_hbm, part_hbm, emb, part, rank_ref, picks, found, emb_sem, part_sem):
    mbs, mtok = tok_ref.shape
    rows, dim = emb.shape
    tile = vocab_tile(rows)
    n_tiles = rows // tile
    loads = [pltpu.make_async_copy(emb_hbm.at[pl.ds(i * tile, tile)], emb.at[pl.ds(i * tile, tile)], emb_sem.at[i])
             for i in range(n_tiles)]
    for ld in loads:
        ld.start()

    loc = tok_ref[...] - lax.axis_index("stage") * rows
    upper, lower = triangles(mbs, mtok)
    counts = []
    for i in range(n_tiles):
        inside = (loc >= i * tile) & (loc < (i + 1) * tile)
        rank, number = ranks(inside.astype(F32), upper, lower)
        rank_ref[i] = jnp.where(inside, rank, -1.0).astype(jnp.int32)
        counts.append(number)

    def window(i, k, w):
        slot = lax.broadcasted_iota(jnp.int32, (LOOK, mtok), 0) + k * LOOK
        ids = jnp.zeros((LOOK, 1), F32)
        for mb in range(mbs):
            pick = slot == rank_ref[i, mb:mb + 1, :]
            picks[mb, look_at(w), :] = pick.astype(BF16)
            ids = ids + jnp.sum(jnp.where(pick, loc[mb:mb + 1, :].astype(F32), 0.0), axis=1, keepdims=True)
        filled = lax.broadcasted_iota(jnp.int32, (LOOK, 1), 0) + k * LOOK < counts[i]
        return jnp.where(filled, ids.astype(jnp.int32), -1)

    def find(i, w, ids):
        lane = lax.broadcasted_iota(jnp.int32, (LOOK, tile), 1) + i * tile
        rows_found = dot_nn((lane == ids).astype(BF16), emb[pl.ds(i * tile, tile), :])
        found[look_at(w), :] = rows_found.astype(BF16)

    first_ids = [window(i, 0, i) for i in range(n_tiles)]
    for i in range(n_tiles):
        loads[i].wait()
        find(i, i, first_ids[i])

    n_windows = jnp.int32(n_tiles)
    for i in range(n_tiles):
        def extra(k, w, i=i):
            find(i, w, window(i, k, w))
            return w + 1
        n_windows = lax.fori_loop(1, (counts[i] + LOOK - 1) // LOOK, extra, n_windows)

    def save(mb):
        return pltpu.make_async_copy(part.at[mb], part_hbm.at[mb], part_sem.at[mb])

    base = n_tiles * LOOK
    for mb in range(mbs):
        part[mb] = dot_tn(picks[mb, 0:base, :], found[0:base, :]).astype(BF16)

        @pl.when(n_windows == n_tiles)
        def _(mb=mb):
            save(mb).start()

    @pl.when(n_windows > n_tiles)
    def _():
        for mb in range(mbs):
            def add(w, _, mb=mb):
                at = look_at(w)
                part[mb] = part[mb] + dot_tn(picks[mb, at, :], found[at, :]).astype(BF16)
                return 0
            lax.fori_loop(n_tiles, n_windows, add, 0)
            save(mb).start()

    for mb in range(mbs):
        save(mb).wait()


def lookup(tok, emb):
    mbs, mtok = tok.shape
    rows, dim = emb.shape
    n_tiles = rows // vocab_tile(rows)
    slots = (n_tiles + mbs * mtok // LOOK) * LOOK
    any_spec = pl.BlockSpec(memory_space=pl.ANY)
    dma = pltpu.SemaphoreType.DMA
    return pl.pallas_call(
        lookup_kernel,
        out_shape=jax.ShapeDtypeStruct((mbs, mtok, dim), BF16),
        in_specs=[pl.BlockSpec(memory_space=pltpu.VMEM), any_spec],
        out_specs=any_spec,
        scratch_shapes=[
            pltpu.VMEM((rows, dim), BF16), pltpu.VMEM((mbs, mtok, dim), BF16), pltpu.VMEM((n_tiles, mbs, mtok), jnp.int32),
            pltpu.VMEM((mbs, slots, mtok), BF16), pltpu.VMEM((slots, dim), BF16),
            dma((n_tiles,)), dma((mbs,)),
        ],
        compiler_params=pltpu.CompilerParams(vmem_limit_bytes=VMEM_LIMIT),
        name="lookup",
    )(tok, emb)


E_ROWS = 512
LOOKUP_LEAD = 1
LOOKUP_PARENT = {2: (3, 0), 1: (0, 0), 4: (5, 0), 6: (7, 0), 5: (3, 1), 7: (0, 1), 3: (0, 2)}
GRAD_PARENT = {0: (1, 0), 2: (3, 0), 4: (5, 0), 1: (6, 0), 6: (7, 0), 3: (5, 1), 5: (7, 1)}


def step_kernel(
    n_stage, lab_ref, part_hbm, emb_hbm, w1_hbm, w2_hbm,
    slope_out, hid_out, dpre_out, xin_out, n_out, g_out, gx_out, dt_out, ge_out, loss_out,
    emb, w1, w2, x_in, x_out, n_all, comb, buf_a, buf_b, slope_stg, act_stg, stats, loss_acc,
    load_sem, part_sem, lk_send, lk_a, lk_b, lk_c, x_send, x_recv, n_send, n_recv, st_send, st_recv,
    g_send, g_a, g_b, b_send, b_recv, gx_send, gx_recv, slope_sem, act_sem, d_sem, e_sem, out_sem, gx_sem,
):
    s = lax.axis_index("stage")
    last = n_stage - 1
    mbs, mtok, dim = x_in.shape
    n_half = mtok // CHUNK
    n_chunks = mbs * n_half
    rows = emb.shape[0]
    ffn = w1.shape[1]
    tile = vocab_tile(rows)
    tokens = HEAD_MBS * mtok
    rounds = mbs // HEAD_MBS
    scale = dim ** -0.5
    c2 = LOG2E * scale
    row_start = s * rows
    bufs = (buf_a, buf_b, x_in)
    lk_sems = (lk_a, lk_b, lk_c)

    loads = [pltpu.make_async_copy(src, dst, load_sem.at[i])
             for i, (src, dst) in enumerate([(w1_hbm, w1), (w2_hbm, w2), (emb_hbm, emb)])]
    for mb in range(mbs):
        pltpu.make_async_copy(part_hbm.at[mb], comb.at[mb], part_sem.at[mb]).start()
    for ld in loads:
        ld.start()
    group_barrier(s, n_stage)

    def pos(c):
        return (c // n_half, pl.ds(pl.multiple_of(lax.rem(c, n_half) * CHUNK, CHUNK), CHUNK))

    def at_chunk(ref, c):
        return ref.at[c // n_half, pl.ds(pl.multiple_of(lax.rem(c, n_half) * CHUNK, CHUNK), CHUNK)]

    def loop(lo, hi, fn):
        def body(i, _):
            fn(i)
            return 0
        lax.fori_loop(lo, hi, body, 0)

    def chunks_of(mb, fn):
        loop(mb * n_half, (mb + 1) * n_half, fn)

    def each_role(roles, fn):
        for node in roles:
            @pl.when(s == node)
            def _(node=node):
                fn(node)

    def lk_copy(c, child):
        parent, slot = LOOKUP_PARENT[child]
        return remote(at_chunk(comb, c), at_chunk(bufs[slot], c), lk_send.at[c], lk_sems[slot].at[c], parent)

    def lk_total(c, slots):
        total = comb[pos(c)].astype(F32)
        for slot in range(slots):
            remote(at_chunk(comb, c), at_chunk(bufs[slot], c), lk_send.at[c], lk_sems[slot].at[c], 0).wait_recv()
            total = total + bufs[slot][pos(c)].astype(F32)
        return total.astype(BF16)

    def lk_forward(c, node, slots):
        comb[pos(c)] = lk_total(c, slots)
        lk_copy(c, node).start()

    loop(0, mbs, lambda mb: pltpu.make_async_copy(part_hbm.at[mb], comb.at[mb], part_sem.at[mb]).wait())
    each_role((1, 2, 4, 6), lambda node: loop(0, n_chunks, lambda c: lk_copy(c, node).start()))
    each_role((5, 7), lambda node: loop(0, n_chunks, lambda c: lk_forward(c, node, 1)))
    loads[0].wait()
    loads[1].wait()

    n_routes = {last: (5, 1, 6), 5: (4,), 1: (3, 0), 3: (2,)}

    def x_copy(c, dst_stage):
        return remote(at_chunk(x_out, c), at_chunk(x_in, c), x_send.at[c], x_recv.at[c], dst_stage)

    def n_copy(c, lane, dst_stage):
        return remote(at_chunk(n_all, c), at_chunk(n_all, c), n_send.at[lane, c], n_recv.at[c], dst_stage)

    def fwd_copies(c):
        slot = lax.rem(c, 2)
        return (pltpu.make_async_copy(slope_stg.at[slot], slope_out.at[c], slope_sem.at[slot]),
                pltpu.make_async_copy(act_stg.at[slot], hid_out.at[c], act_sem.at[slot]))

    def fwd_chunk(c):
        idx = pos(c)

        @pl.when(s == 0)
        def _():
            x_in[idx] = lk_total(c, 3)

        @pl.when(s > 0)
        def _():
            x_copy(c, 0).wait_recv()

        @pl.when(c >= 2)
        def _():
            for cp in fwd_copies(c - 2):
                cp.wait()

        slot = lax.rem(c, 2)
        out = forward_chunk(x_in[idx], w1, w2, slope_stg.at[slot], act_stg.at[slot]).astype(BF16)
        x_out[idx] = out
        for cp in fwd_copies(c):
            cp.start()

        @pl.when(s < last)
        def _():
            x_copy(c, s + 1).start()

        @pl.when(s == last)
        def _():
            out_f = out.astype(F32)
            n_all[idx] = (out_f * norm_scale(out_f)).astype(BF16)
            for lane, dst in enumerate(n_routes[last]):
                n_copy(c, lane, dst).start()

    def n_round(r, fn):
        loop(r * HEAD_MBS * n_half, (r + 1) * HEAD_MBS * n_half, fn)

    def n_early(r):
        def take(c, node):
            n_copy(c, 0, 0 if node == last else last).wait_recv()
            for lane, dst in enumerate(n_routes[node]):
                n_copy(c, lane, dst).start()
        each_role((1, 5), lambda node: n_round(r, lambda c: take(c, node)))

    def n_mid(r):
        def take(c, node):
            n_copy(c, 0, last).wait_recv()
            n_copy(c, 0, n_routes[node][0]).start()
        each_role((3,), lambda node: n_round(r, lambda c: take(c, node)))

    def n_late(r):
        @pl.when((lax.rem(s, 2) == 0))
        def _():
            n_round(r, lambda c: n_copy(c, 0, last).wait_recv())

    def g_copy(mb, child):
        parent, slot = GRAD_PARENT[child]
        return remote(comb.at[mb], bufs[slot].at[mb], g_send.at[mb], (g_a, g_b)[slot].at[mb], parent)

    def g_total(mb, slots):
        total = comb[mb].astype(F32)
        for slot in range(slots):
            remote(comb.at[mb], bufs[slot].at[mb], g_send.at[mb], (g_a, g_b)[slot].at[mb], 0).wait_recv()
            total = total + bufs[slot][mb].astype(F32)
        return total

    def g_forward(mb, node, slots):
        comb[mb] = g_total(mb, slots).astype(BF16)
        g_copy(mb, node).start()

    def g_low(r):
        each_role((1, 3), lambda node: loop(r * HEAD_MBS, (r + 1) * HEAD_MBS, lambda mb: g_forward(mb, node, 1)))

    def g_mid(r):
        each_role((6,), lambda node: loop(r * HEAD_MBS, (r + 1) * HEAD_MBS, lambda mb: g_forward(mb, node, 1)))
        each_role((5,), lambda node: loop(r * HEAD_MBS, (r + 1) * HEAD_MBS, lambda mb: g_forward(mb, node, 2)))

    def g_final(mb):
        @pl.when(s == last)
        def _():
            grad_n = g_total(mb, 2)
            x_f = x_out[mb].astype(F32)
            inv = norm_scale(x_f)
            n_f = x_f * inv
            dx = inv * (grad_n - n_f * jnp.mean(grad_n * n_f, axis=-1, keepdims=True))
            comb[mb] = dx.astype(BF16)

    def lab_row_of(r):
        parts = [lab_ref[pl.ds(r * HEAD_MBS + i, 1), :] for i in range(HEAD_MBS)]
        return jnp.concatenate(parts, axis=1) - row_start

    def st_copy(r, off):
        dst = lax.rem(s + off, n_stage)
        return remote(stats.at[r, s], stats.at[r, s], st_send.at[r, off], st_recv.at[r, off], dst)

    saves = [pltpu.make_async_copy(x_in, xin_out, out_sem.at[0]), pltpu.make_async_copy(n_all, n_out, out_sem.at[1])]

    def forward_and_head(logits, n_t, d_stg, gn_acc):
        n_tiles = rows // tile

        def head_a(r):
            n_late(r)

            @pl.when(r == rounds - 1)
            def _():
                for cp in saves:
                    cp.start()

            n_t[...] = n_all[pl.ds(r * HEAD_MBS, HEAD_MBS)].reshape(tokens, dim).T
            top, tot, lab = head_logits(n_t, emb, logits, lab_row_of(r), tokens)

            @pl.when(r == rounds - 1)
            def _():
                for cp in saves:
                    cp.wait()

                @pl.when(s < last)
                def _():
                    loop(0, n_chunks, lambda c: x_copy(c, 0).wait_send())
                for src, dsts in n_routes.items():
                    @pl.when(s == src)
                    def _(dsts=dsts):
                        loop(0, n_chunks, lambda c: [n_copy(c, lane, dst).wait_send() for lane, dst in enumerate(dsts)])
            stats[r, s] = jnp.concatenate([top, tot, lab, jnp.zeros((5, tokens), F32)], axis=0)
            for off in range(1, n_stage):
                st_copy(r, off).start()

        def d_copy(seq):
            slot = lax.rem(seq, 2)
            r = seq // n_tiles
            idx = lax.rem(seq, n_tiles)
            dst = dt_out.at[pl.ds(pl.multiple_of(idx * tile, 16), tile), pl.ds(pl.multiple_of(r * tokens, tokens), tokens)]
            return pltpu.make_async_copy(d_stg.at[slot], dst, d_sem.at[slot])

        def head_b(r):
            @pl.when(r + 1 < rounds)
            def _():
                n_early(r + 1)
            for off in range(1, n_stage):
                src = lax.rem(s + n_stage - off, n_stage)
                remote(stats.at[r, s], stats.at[r, src], st_send.at[r, off], st_recv.at[r, off], src).wait_recv()
            blocks = [stats[r, i] for i in range(n_stage)]
            top = blocks[0][0:1]
            for blk in blocks[1:]:
                top = jnp.maximum(top, blk[0:1])
            tot = jnp.zeros_like(top)
            lab = jnp.zeros_like(top)
            for blk in blocks:
                tot = tot + blk[1:2] * jnp.exp2((blk[0:1] - top) * c2)
                lab = lab + blk[2:3]
            loss_acc[...] = loss_acc[...] + (jnp.log(tot) + (top - lab) * scale)
            shift = jnp.log(tot) * LOG2E - math.log2(scale)
            lab_row = lab_row_of(r)

            def tile_step(idx):
                seq = r * n_tiles + idx

                @pl.when(seq >= 2)
                def _():
                    d_copy(seq - 2).wait()
                @pl.when((idx == n_tiles - 1) & (r + 1 < rounds))
                def _():
                    n_mid(r + 1)
                base = pl.multiple_of(idx * tile, 16)
                part = head_grad_tile(base, tile, emb, logits, d_stg.at[lax.rem(seq, 2)], lab_row, top, shift, tokens)
                gn_acc[...] = gn_acc[...] + part
                d_copy(seq).start()

            gn_acc[...] = jnp.zeros_like(gn_acc)
            loop(0, n_tiles, tile_step)
            comb[pl.ds(r * HEAD_MBS, HEAD_MBS)] = gn_acc[...].reshape(HEAD_MBS, mtok, dim).astype(BF16)
            each_role((0, 2, 4), lambda node: loop(r * HEAD_MBS, (r + 1) * HEAD_MBS, lambda mb: g_copy(mb, node).start()))
        loss_acc[...] = jnp.zeros_like(loss_acc)
        first_a = HEAD_MBS + 1 + last

        def step(k):
            @pl.when((s == 3) & (k == 0))
            def _():
                loop(0, LOOKUP_LEAD * n_half, lambda c: lk_forward(c, 3, 2))

            @pl.when((s == 3) & (k + LOOKUP_LEAD < mbs))
            def _():
                chunks_of(k + LOOKUP_LEAD, lambda c: lk_forward(c, 3, 2))

            f_mb = k - s

            @pl.when((f_mb >= 0) & (f_mb < mbs))
            def _():
                chunks_of(f_mb, fwd_chunk)

            @pl.when(k == first_a)
            def _():
                loads[2].wait()

                @pl.when(s > 0)
                def _():
                    loop(0, n_chunks, lambda c: lk_copy(c, 1).wait_send())

            rel = k - first_a
            r = rel // HEAD_MBS
            even = lax.rem(rel + HEAD_MBS * n_stage, HEAD_MBS) == 0

            @pl.when(k == first_a)
            def _():
                n_early(0)
                n_mid(0)

            @pl.when(even & (rel >= 0))
            def _():
                head_a(r)

            @pl.when(even & (rel >= HEAD_MBS))
            def _():
                g_low(r - 1)

                @pl.when(r >= 2)
                def _():
                    loop((r - 2) * HEAD_MBS, (r - 1) * HEAD_MBS, g_final)

            @pl.when(jnp.logical_not(even) & (rel >= 0))
            def _():
                head_b(r)

            @pl.when(jnp.logical_not(even) & (rel >= HEAD_MBS))
            def _():
                g_mid(r - 1)

        loop(0, first_a + HEAD_MBS * rounds, step)
        for c in (n_chunks - 2, n_chunks - 1):
            for cp in fwd_copies(c):
                cp.wait()
        for seq in (rounds * n_tiles - 2, rounds * n_tiles - 1):
            d_copy(seq).wait()

    pl.run_scoped(
        forward_and_head,
        pltpu.VMEM((rows, tokens), F32), pltpu.VMEM((dim, tokens), BF16),
        pltpu.VMEM((2, tile, tokens), BF16), pltpu.VMEM((tokens, dim), F32),
    )
    loss_out[...] = jnp.broadcast_to(jnp.sum(loss_acc[...], axis=1, keepdims=True), loss_out.shape)

    g_in, g_buf, gx, wt = x_in, x_out, n_all, emb

    def b_copy(c, dst):
        return remote(at_chunk(g_buf, c), at_chunk(g_in, c), b_send.at[c], b_recv.at[c], dst)

    def gx_copy(c, lane, dst):
        return remote(at_chunk(gx, c), at_chunk(gx, c), gx_send.at[lane, c], gx_recv.at[c], dst)

    def slope_copy(c):
        slot = lax.rem(c, 2)
        return pltpu.make_async_copy(slope_out.at[c], slope_stg.at[slot], slope_sem.at[slot])

    def dpre_copy(c):
        slot = lax.rem(c, 2)
        return pltpu.make_async_copy(act_stg.at[slot], dpre_out.at[c], act_sem.at[slot])

    gx_split = n_chunks // 2
    gx_routes = {0: ((3, 0, n_chunks), (last, 0, n_chunks), (1, 0, n_chunks)), 3: ((2, 0, n_chunks), (5, 0, gx_split)),
                 last: ((6, 0, n_chunks), (5, gx_split, n_chunks)), 5: ((4, 0, n_chunks),)}

    def gx_send_all(c, node):
        for lane, (dst, lo, hi) in enumerate(gx_routes[node]):
            @pl.when((c >= lo) & (c < hi))
            def _(lane=lane, dst=dst):
                gx_copy(c, lane, dst).start()


    def bwd_chunk(c):
        slot = lax.rem(c, 2)
        idx = pos(c)

        @pl.when(s < last)
        def _():
            b_copy(c, 0).wait_recv()

        @pl.when(s == last)
        def _():
            g_in[idx] = comb[idx]

        @pl.when(c >= 2)
        def _():
            dpre_copy(c - 2).wait()
        slope_copy(c).wait()
        dx = backward_chunk(g_in[idx], wt, slope_stg.at[slot], act_stg.at[slot]).astype(BF16)

        @pl.when(s > 0)
        def _():
            g_buf[idx] = dx
            b_copy(c, s - 1).start()

        @pl.when(s == 0)
        def _():
            gx[idx] = dx
            gx_send_all(c, 0)
        dpre_copy(c).start()

        @pl.when(c + 2 < n_chunks)
        def _():
            slope_copy(c + 2).start()

    full = rows // E_ROWS
    rest = rows - full * E_ROWS

    def backward(n_rows, d_in, e_stg):
        def d_load(i, size=E_ROWS):
            slot = lax.rem(i, 2)
            src = dt_out.at[pl.ds(pl.multiple_of(i * E_ROWS, E_ROWS), size)]
            return pltpu.make_async_copy(src, d_in.at[slot, pl.ds(0, size)], d_sem.at[slot])

        def e_save(i, size=E_ROWS):
            slot = lax.rem(i, 2)
            dst = ge_out.at[pl.ds(pl.multiple_of(i * E_ROWS, E_ROWS), size)]
            return pltpu.make_async_copy(e_stg.at[slot, pl.ds(0, size)], dst, e_sem.at[slot])

        def e_tile(i):
            slot = lax.rem(i, 2)

            @pl.when(i + 1 < full)
            def _():
                d_load(i + 1).start()
            if rest:
                @pl.when(i + 1 == full)
                def _():
                    d_load(full, rest).start()
            d_load(i).wait()

            @pl.when(i >= 2)
            def _():
                e_save(i - 2).wait()
            e_stg[slot] = dot_nn(d_in[slot], n_rows[...].reshape(mbs * mtok, dim))
            e_save(i).start()

        n_load = pltpu.make_async_copy(n_out, n_rows, out_sem.at[1])
        n_load.start()
        slope_copy(0).start()
        slope_copy(1).start()
        d_load(0).start()
        g_low(rounds - 1)
        transpose_weights(w1, w2, wt)
        n_load.wait()
        early = jnp.minimum((last - s) * 2, full)
        loop(0, early, e_tile)

        def gx_save(c):
            return pltpu.make_async_copy(at_chunk(gx, c), at_chunk(gx_out, c), gx_sem.at[c])

        def gx_forward(c):
            @pl.when(s > 0)
            def _():
                gx_copy(c, 0, 0).wait_recv()
            each_role((3, last, 5), lambda node: gx_send_all(c, node))
            gx_save(c).start()

        def step(k):
            @pl.when(k >= mbs - 2 * HEAD_MBS)
            def _():
                @pl.when(k < mbs)
                def _():
                    g_final(k)
            b_mb = k - (last - s)

            @pl.when((b_mb >= 0) & (b_mb < mbs))
            def _():
                chunks_of(b_mb, bwd_chunk)

            @pl.when(k == 2)
            def _():
                g_mid(rounds - 1)

            x_mb = k - n_stage

            @pl.when((s == 3) & (x_mb >= 0) & (x_mb < gx_split // n_half))
            def _():
                chunks_of(x_mb, gx_forward)

        loop(0, mbs + last, step)
        g_save = pltpu.make_async_copy(g_in, g_out, out_sem.at[0])
        g_save.start()
        loop(early, full, e_tile)
        loop(jnp.where(s == 3, gx_split, 0), n_chunks, gx_forward)
        if rest:
            d_load(full, rest).wait()
            e_save(full - 2).wait()
            slot = full % 2
            e_stg[slot, pl.ds(0, rest)] = dot_nn(d_in[slot, pl.ds(0, rest)], n_rows[...].reshape(mbs * mtok, dim))
            e_save(full, rest).start()

        g_save.wait()
        if rest:
            e_save(full - 1).wait()
            e_save(full, rest).wait()
        else:
            e_save(full - 2).wait()
            e_save(full - 1).wait()
        for c in (n_chunks - 2, n_chunks - 1):
            dpre_copy(c).wait()
        loop(0, n_chunks, lambda c: gx_save(c).wait())

    pl.run_scoped(
        backward,
        pltpu.VMEM((mbs, mtok, dim), BF16), pltpu.VMEM((2, E_ROWS, mbs * mtok), BF16), pltpu.VMEM((2, E_ROWS, dim), F32),
    )

    @pl.when(s < last)
    def _():
        loop(0, mbs, lambda mb: g_copy(mb, 1).wait_send())

    @pl.when(s > 0)
    def _():
        loop(0, n_chunks, lambda c: b_copy(c, 0).wait_send())
    for src, routes in gx_routes.items():
        @pl.when(s == src)
        def _(routes=routes):
            for lane, (dst, lo, hi) in enumerate(routes):
                loop(lo, hi, lambda c: gx_copy(c, lane, dst).wait_send())
    loop(0, rounds, lambda r: [st_copy(r, off).wait_send() for off in range(1, n_stage)])


def pipeline_step(n_stage, labels, part, emb, w1, w2):
    mbs, mtok, dim = part.shape
    rows = emb.shape[0]
    ffn = w1.shape[1]
    chunks = mbs * mtok // CHUNK
    rounds = mbs // HEAD_MBS
    tokens = HEAD_MBS * mtok
    any_spec = pl.BlockSpec(memory_space=pl.ANY)
    vmem_spec = pl.BlockSpec(memory_space=pltpu.VMEM)
    act = pltpu.VMEM((mbs, mtok, dim), BF16)
    dma = pltpu.SemaphoreType.DMA
    act_shape = jax.ShapeDtypeStruct((mbs, mtok, dim), BF16)
    hid_shape = jax.ShapeDtypeStruct((chunks, CHUNK, ffn), BF16)
    return pl.pallas_call(
        functools.partial(step_kernel, n_stage),
        out_shape=(
            jax.ShapeDtypeStruct((chunks, CHUNK, ffn), F32), hid_shape, hid_shape,
            act_shape, act_shape, act_shape, act_shape,
            jax.ShapeDtypeStruct((rows, mbs * mtok), BF16),
            jax.ShapeDtypeStruct((rows, dim), F32),
            jax.ShapeDtypeStruct((8, 128), F32),
        ),
        in_specs=[vmem_spec] + [any_spec] * 4,
        out_specs=(any_spec,) * 9 + (vmem_spec,),
        scratch_shapes=[
            pltpu.VMEM((rows, dim), BF16), pltpu.VMEM((dim, ffn), BF16), pltpu.VMEM((ffn, dim), BF16),
            act, act, act, act, act, act,
            pltpu.VMEM((2, CHUNK, ffn), F32), pltpu.VMEM((2, CHUNK, ffn), BF16),
            pltpu.VMEM((rounds, n_stage, 8, tokens), F32), pltpu.VMEM((1, tokens), F32),
            dma((3,)), dma((mbs,)), dma((chunks,)), dma((chunks,)), dma((chunks,)), dma((chunks,)),
            dma((chunks,)), dma((chunks,)), dma((3, chunks)), dma((chunks,)),
            dma((rounds, n_stage)), dma((rounds, n_stage)), dma((mbs,)), dma((mbs,)), dma((mbs,)),
            dma((chunks,)), dma((chunks,)), dma((3, chunks)), dma((chunks,)),
            dma((2,)), dma((2,)), dma((2,)), dma((2,)), dma((2,)), dma((chunks,)),
        ],
        compiler_params=pltpu.CompilerParams(collective_id=0, has_side_effects=True, vmem_limit_bytes=VMEM_LIMIT),
        name="pipeline_step",
    )(labels, part, emb, w1, w2)


WINDOW = 256
W_COLS = 1024
E_SLOTS = 4


def tail_kernel(
    rows, tok_ref, loss_ref, x_hbm, g_hbm, gx_hbm, dpre_hbm, hid_hbm, ge_hbm,
    loss_out, g1_out, g2_out, out_hbm,
    x_buf, g_buf, gx_buf, dp_buf, hid_buf, g1_stg, g2_stg, e_buf, packed, packed_id, bounds,
    act_sem, dp_sem, hid_sem, g1_sem, g2_sem, e_in_sem, e_out_sem,
):
    mbs, mtok = tok_ref.shape
    total, dim = g_buf.shape
    ffn = dpre_hbm.shape[1]
    n_blocks = ffn // W_COLS
    e_rows = e_buf.shape[1]
    n_e = rows // e_rows
    per_block = n_e // n_blocks

    def cols(j):
        return pl.ds(pl.multiple_of(j * W_COLS, W_COLS), W_COLS)

    def e_at(i):
        return pl.ds(pl.multiple_of(i * e_rows, 8), e_rows)

    def dp_load(j):
        slot = lax.rem(j, 2)
        return pltpu.make_async_copy(dpre_hbm.at[:, cols(j)], dp_buf.at[slot], dp_sem.at[slot])

    def hid_load(j):
        slot = lax.rem(j, 2)
        return pltpu.make_async_copy(hid_hbm.at[:, cols(j)], hid_buf.at[slot], hid_sem.at[slot])

    def e_load(i):
        slot = lax.rem(i, E_SLOTS)
        return pltpu.make_async_copy(ge_hbm.at[e_at(i)], e_buf.at[slot], e_in_sem.at[slot])

    def e_save(i):
        slot = lax.rem(i, E_SLOTS)
        return pltpu.make_async_copy(e_buf.at[slot], out_hbm.at[e_at(i)], e_out_sem.at[slot])

    def g1_save(j):
        return pltpu.make_async_copy(g1_stg, g1_out.at[0, :, cols(j)], g1_sem.at[0])

    def g2_save(j):
        return pltpu.make_async_copy(g2_stg, g2_out.at[0, cols(j)], g2_sem.at[0])

    x_load = pltpu.make_async_copy(x_hbm, x_buf, act_sem.at[0])
    g_load = pltpu.make_async_copy(g_hbm, g_buf, act_sem.at[1])
    gx_load = pltpu.make_async_copy(gx_hbm, gx_buf, act_sem.at[2])
    gx_load.start()
    loss_out[0] = loss_ref[0, 0] * (1.0 / total)

    s = lax.axis_index("stage")
    loc = tok_ref[...] - s * rows
    upper, lower = triangles(mbs, mtok)
    slot_of = jnp.full((mbs, mtok), -1.0, F32)
    count = jnp.int32(0)
    bounds[0] = count
    for i in range(n_e):
        inside = (loc >= i * e_rows) & (loc < (i + 1) * e_rows)
        rank, number = ranks(inside.astype(F32), upper, lower)
        slot_of = jnp.where(inside, rank + count.astype(F32), slot_of)
        count = count + number
        bounds[i + 1] = count
    slot_of = slot_of.astype(jnp.int32)
    n_packs = jnp.maximum((count + WINDOW - 1) // WINDOW, 1)

    def pack(b):
        slot = lax.broadcasted_iota(jnp.int32, (WINDOW, mtok), 0) + b * WINDOW
        ids = jnp.zeros((WINDOW, 1), F32)
        picks = []
        for mb in range(mbs):
            pick = slot == slot_of[mb:mb + 1, :]
            picks.append(pick.astype(BF16))
            ids = ids + jnp.sum(jnp.where(pick, loc[mb:mb + 1, :].astype(F32), 0.0), axis=1, keepdims=True)
        at = pl.ds(pl.multiple_of(b * WINDOW, WINDOW), WINDOW)
        packed[at, :] = dot_nn(jnp.concatenate(picks, axis=1), gx_buf[...]).astype(BF16)
        filled = lax.broadcasted_iota(jnp.int32, (WINDOW, 1), 0) + b * WINDOW < count
        packed_id[at, :] = jnp.broadcast_to(jnp.where(filled, ids.astype(jnp.int32), -1), (WINDOW, 128))

    def loop(lo, hi, fn):
        def body(i, _):
            fn(i)
            return 0
        lax.fori_loop(lo, hi, body, 0)

    def e_tile(i):
        slot = lax.rem(i, E_SLOTS)
        first = jnp.minimum((bounds[i] // 16) * 16, (n_packs - 1) * WINDOW)
        lane = lax.broadcasted_iota(jnp.int32, (WINDOW, e_rows), 1) + i * e_rows

        def window(k):
            start = pl.multiple_of(jnp.minimum(first + k * WINDOW, (n_packs - 1) * WINDOW), 16)
            at = pl.ds(start, WINDOW)
            fresh = lax.broadcasted_iota(jnp.int32, (WINDOW, 1), 0) + start >= first + k * WINDOW
            ids = jnp.where(fresh, packed_id[at, :][:, 0:1], -1)
            return dot_tn((lane == ids).astype(BF16), packed[at, :])

        e_load(i).wait()
        e_buf[slot] = e_buf[slot] + window(0)

        def more(k):
            e_buf[slot] = e_buf[slot] + window(k)

        loop(1, (bounds[i + 1] - first + WINDOW - 1) // WINDOW, more)
        e_save(i).start()

    def block(j):
        slot = lax.rem(j, 2)

        @pl.when(j == 0)
        def _():
            x_load.wait()

        @pl.when(j > 0)
        def _():
            g1_save(j - 1).wait()
        dp_load(j).wait()

        @pl.when(j == 0)
        def _():
            for cp in (e_load(0), e_load(1), g_load, hid_load(0)):
                cp.start()
        g1_stg[...] = dot_tn(x_buf[...], dp_buf[slot])
        g1_save(j).start()

        @pl.when(j + 1 < n_blocks)
        def _():
            dp_load(j + 1).start()

        def tile(i):
            @pl.when(i + 2 < n_e)
            def _():
                @pl.when(i + 2 >= E_SLOTS)
                def _():
                    e_save(i + 2 - E_SLOTS).wait()
                e_load(i + 2).start()
            e_tile(i)

        loop(j * per_block, (j + 1) * per_block, tile)

        @pl.when(j == 0)
        def _():
            g_load.wait()

        @pl.when(j > 0)
        def _():
            g2_save(j - 1).wait()
        hid_load(j).wait()

        @pl.when(j + 1 < n_blocks)
        def _():
            hid_load(j + 1).start()
        g2_stg[...] = dot_tn(hid_buf[slot], g_buf[...])
        g2_save(j).start()

    x_load.start()
    dp_load(0).start()
    gx_load.wait()
    loop(0, n_packs, pack)
    loop(0, n_blocks, block)
    g1_save(n_blocks - 1).wait()
    g2_save(n_blocks - 1).wait()
    for i in range(max(n_e - E_SLOTS, 0), n_e):
        e_save(i).wait()


def tail(tok, loss, x, g, gx, dpre, hid, ge):
    rows, dim = ge.shape
    total, ffn = dpre.shape
    n_blocks = ffn // W_COLS
    e_rows = rows // (2 * n_blocks)
    n_e = rows // e_rows
    any_spec = pl.BlockSpec(memory_space=pl.ANY)
    vmem_spec = pl.BlockSpec(memory_space=pltpu.VMEM)
    dma = pltpu.SemaphoreType.DMA
    act = pltpu.VMEM((total, dim), BF16)
    return pl.pallas_call(
        functools.partial(tail_kernel, rows),
        out_shape=(
            jax.ShapeDtypeStruct((1,), F32),
            jax.ShapeDtypeStruct((1, dim, ffn), F32),
            jax.ShapeDtypeStruct((1, ffn, dim), F32),
            jax.ShapeDtypeStruct((rows, dim), F32),
        ),
        in_specs=[vmem_spec, vmem_spec] + [any_spec] * 6,
        out_specs=(pl.BlockSpec(memory_space=pltpu.SMEM), any_spec, any_spec, any_spec),
        scratch_shapes=[
            act, act, act, pltpu.VMEM((2, total, W_COLS), BF16), pltpu.VMEM((2, total, W_COLS), BF16),
            pltpu.VMEM((dim, W_COLS), F32), pltpu.VMEM((W_COLS, dim), F32), pltpu.VMEM((E_SLOTS, e_rows, dim), F32),
            pltpu.VMEM((total, dim), BF16), pltpu.VMEM((total, 128), jnp.int32), pltpu.SMEM((n_e + 1,), jnp.int32),
            dma((3,)), dma((2,)), dma((2,)), dma((1,)), dma((1,)), dma((E_SLOTS,)), dma((E_SLOTS,)),
        ],
        compiler_params=pltpu.CompilerParams(vmem_limit_bytes=VMEM_LIMIT),
        name="tail",
    )(tok, loss, x, g, gx, dpre, hid, ge)


def solution(mesh):
    n_stage = mesh.shape["stage"]

    def stage_body(token_ids, label_ids, emb_rows, w_in, w_out):
        tokens = token_ids.shape[0] * token_ids.shape[1]
        part = lookup(token_ids, emb_rows)
        _, hid, dpre, x_in, _, g_all, gx, _, ge, loss = pipeline_step(n_stage, label_ids, part, emb_rows, w_in[0], w_out[0])
        flat = lambda a: a.reshape(tokens, a.shape[-1])
        mean_loss, grad_in, grad_out, grad_emb = tail(token_ids, loss, flat(x_in), flat(g_all), flat(gx), flat(dpre), flat(hid), ge)
        return mean_loss, grad_in, grad_out, grad_emb

    return jax.shard_map(
        stage_body,
        mesh=mesh,
        in_specs=(P("dp", None), P("dp", None), P("stage", None), P("stage", None, None), P("stage", None, None)),
        out_specs=(P("dp"), P(("dp", "stage"), None, None), P(("dp", "stage"), None, None), P(("dp", "stage"), None)),
        check_vma=False,
    )
```

```python
import functools
import math

import jax
import jax.numpy as jnp
from jax import lax
from jax.experimental import pallas as pl
from jax.experimental.pallas import tpu as pltpu
from jax.sharding import PartitionSpec as P

NORM_EPS = 1e-6
MESH = pl.DeviceIdType.MESH
F32 = jnp.float32
BF16 = jnp.bfloat16
GELU_A = math.sqrt(2.0 / math.pi)
GELU_B = 0.044715
LOG2E = math.log2(math.e)
CHUNK = 128
HEAD_MBS = 2
VMEM_LIMIT = 67_000_000


def dot_nn(a, b):
    return lax.dot_general(a, b, (((1,), (0,)), ((), ())), preferred_element_type=F32)


def dot_nt(a, b):
    return lax.dot_general(a, b, (((1,), (1,)), ((), ())), preferred_element_type=F32)


def dot_tn(a, b):
    return lax.dot_general(a, b, (((0,), (0,)), ((), ())), preferred_element_type=F32)


def gelu_and_slope(pre):
    sq = pre * pre
    th = jnp.tanh(pre * (GELU_A + (GELU_A * GELU_B) * sq))
    half_sum = 0.5 + 0.5 * th
    hid = pre * half_sum
    slope = half_sum + (hid - hid * th) * (GELU_A + (3.0 * GELU_A * GELU_B) * sq)
    return hid, slope


def norm_scale(x_f32):
    return lax.rsqrt(jnp.mean(x_f32 * x_f32, axis=-1, keepdims=True) + NORM_EPS)


def remote(src, dst, send_sem, recv_sem, stage):
    return pltpu.make_async_remote_copy(
        src_ref=src, dst_ref=dst, send_sem=send_sem, recv_sem=recv_sem, device_id={"stage": stage}, device_id_type=MESH
    )


def group_barrier(stage, n_stage):
    barrier = pltpu.get_barrier_semaphore()
    for off in range(1, n_stage):
        pl.semaphore_signal(barrier, inc=1, device_id={"stage": lax.rem(stage + off, n_stage)}, device_id_type=MESH)
    pl.semaphore_wait(barrier, n_stage - 1)


def vocab_tile(rows):
    for parts in range(2, rows + 1):
        if rows % parts == 0 and (rows // parts) % 16 == 0 and rows // parts <= 2400:
            return rows // parts
    return rows


def sub_blocks(rows, size):
    return [(start, min(size, rows - start)) for start in range(0, rows, size)]


def forward_chunk(x, w1, w2, slope_slot, hid_slot):
    ffn = w1.shape[1]
    width = ffn // 4
    for part in range(4):
        cols = pl.ds(part * width, width)
        hid, slope = gelu_and_slope(dot_nn(x, w1[:, cols]))
        slope_slot[:, cols] = slope
        hid_slot[:, cols] = hid.astype(BF16)
    return x.astype(F32) + dot_nn(hid_slot[...], w2[...])


def forward_pair(x, w1, w2, slope_slots, hid_slots):
    ffn = w1.shape[1]
    width = ffn // 4
    for part in range(4):
        cols = pl.ds(part * width, width)
        hid, slope = gelu_and_slope(dot_nn(x, w1[:, cols]))
        for slot in range(2):
            slope_slots[slot, :, cols] = slope[slot * CHUNK:(slot + 1) * CHUNK]
            hid_slots[slot, :, cols] = hid[slot * CHUNK:(slot + 1) * CHUNK].astype(BF16)
    return x.astype(F32) + dot_nn(hid_slots[...].reshape(2 * CHUNK, ffn), w2[...])


def backward_chunk(grad, w2_t, w1_t, slope_slot, dpre_slot):
    ffn = slope_slot.shape[1]
    dim = grad.shape[1]
    for part in range(ffn // dim):
        cols = pl.ds(part * dim, dim)
        dpre_slot[:, cols] = (dot_nn(grad, w2_t[:, cols]) * slope_slot[:, cols]).astype(BF16)
    return grad.astype(F32) + dot_nn(dpre_slot[...], w1_t[...])


def swap_transposed(w1, w2):
    dim, ffn = w1.shape
    side = 256

    def strip(part, _):
        at = pl.ds(pl.multiple_of(part * side, side), side)
        for i in range(dim // side):
            rows = pl.ds(i * side, side)
            from_w1 = w1[rows, at].T
            from_w2 = w2[at, rows].T
            w2[at, rows] = from_w1
            w1[rows, at] = from_w2
        return 0

    lax.fori_loop(0, ffn // side, strip, 0)


def head_logits(n_t, emb, logits, lab_row, tokens):
    rows = emb.shape[0]
    tile = vocab_tile(rows)
    c2 = LOG2E * emb.shape[1] ** -0.5

    def tile_step(idx, carry):
        mx, sm, lb = carry
        base = pl.multiple_of(idx * tile, 16)
        for start, size in sub_blocks(tile, 256):
            at = pl.ds(base + start, size)
            block = dot_nn(emb[at, :], n_t[...])
            logits[at, :] = block
            b3 = block.reshape(size // 8, 8, tokens)
            row_ids = lax.broadcasted_iota(jnp.int32, (size, tokens), 0) + (base + start)
            hit = jnp.where(row_ids == lab_row, block, 0.0).reshape(size // 8, 8, tokens)
            mx_new = jnp.maximum(mx, jnp.max(b3, axis=0))
            sm = sm * jnp.exp2((mx - mx_new) * c2) + jnp.sum(jnp.exp2((b3 - mx_new[None]) * c2), axis=0)
            lb = lb + jnp.sum(hit, axis=0)
            mx = mx_new
        return mx, sm, lb

    init = (jnp.full((8, tokens), -3.0e38, F32), jnp.zeros((8, tokens), F32), jnp.zeros((8, tokens), F32))
    mx, sm, lb = lax.fori_loop(0, rows // tile, tile_step, init)
    top = jnp.max(mx, axis=0, keepdims=True)
    tot = jnp.sum(sm * jnp.exp2((mx - top) * c2), axis=0, keepdims=True)
    lab = jnp.sum(lb, axis=0, keepdims=True)
    return top, tot, lab


def head_grad_tile(base, size_all, emb, logits, d_slot, lab_row, top, shift, tokens):
    scale = emb.shape[1] ** -0.5
    c2 = LOG2E * scale
    total = None
    for start, size in sub_blocks(size_all, 256):
        at = pl.ds(base + start, size)
        row_ids = lax.broadcasted_iota(jnp.int32, (size, tokens), 0) + (base + start)
        prob = jnp.exp2((logits[at, :] - top) * c2 - shift)
        d_log = (prob - jnp.where(row_ids == lab_row, scale, 0.0)).astype(BF16)
        d_slot[pl.ds(start, size), :] = d_log
        part = dot_tn(d_log, emb[at, :])
        total = part if total is None else total + part
    return total


LOOK = 160


def look_at(w):
    return pl.ds(w * LOOK if isinstance(w, int) else pl.multiple_of(w * LOOK, 16), LOOK)


def ranks(flag, upper, lower):
    within = dot_nn(flag.astype(BF16), upper)
    total = jnp.sum(flag, axis=1, keepdims=True)
    rows = flag.shape[0]
    before = jnp.sum(jnp.where(lower, jnp.transpose(jnp.broadcast_to(total, (rows, rows))), 0.0), axis=1, keepdims=True)
    return within - flag + before, jnp.sum(flag).astype(jnp.int32)


def triangles(mbs, mtok):
    upper = (lax.broadcasted_iota(jnp.int32, (mtok, mtok), 0)
             <= lax.broadcasted_iota(jnp.int32, (mtok, mtok), 1)).astype(BF16)
    lower = lax.broadcasted_iota(jnp.int32, (mbs, mbs), 1) < lax.broadcasted_iota(jnp.int32, (mbs, mbs), 0)
    return upper, lower


def lookup_kernel(tok_ref, emb_hbm, part_hbm, emb, part, rank_ref, picks, found, emb_sem, part_sem):
    mbs, mtok = tok_ref.shape
    rows, dim = emb.shape
    tile = vocab_tile(rows)
    n_tiles = rows // tile
    loads = [pltpu.make_async_copy(emb_hbm.at[pl.ds(i * tile, tile)], emb.at[pl.ds(i * tile, tile)], emb_sem.at[i])
             for i in range(n_tiles)]
    for ld in loads:
        ld.start()

    loc = tok_ref[...] - lax.axis_index("stage") * rows
    upper, lower = triangles(mbs, mtok)
    counts = []
    for i in range(n_tiles):
        inside = (loc >= i * tile) & (loc < (i + 1) * tile)
        rank, number = ranks(inside.astype(F32), upper, lower)
        rank_ref[i] = jnp.where(inside, rank, -1.0).astype(jnp.int32)
        counts.append(number)

    def window(i, k, w):
        slot = lax.broadcasted_iota(jnp.int32, (LOOK, mtok), 0) + k * LOOK
        ids = jnp.zeros((LOOK, 1), F32)
        for mb in range(mbs):
            pick = slot == rank_ref[i, mb:mb + 1, :]
            picks[mb, look_at(w), :] = pick.astype(BF16)
            ids = ids + jnp.sum(jnp.where(pick, loc[mb:mb + 1, :].astype(F32), 0.0), axis=1, keepdims=True)
        filled = lax.broadcasted_iota(jnp.int32, (LOOK, 1), 0) + k * LOOK < counts[i]
        return jnp.where(filled, ids.astype(jnp.int32), -1)

    def find(i, w, ids):
        lane = lax.broadcasted_iota(jnp.int32, (LOOK, tile), 1) + i * tile
        rows_found = dot_nn((lane == ids).astype(BF16), emb[pl.ds(i * tile, tile), :])
        found[look_at(w), :] = rows_found.astype(BF16)

    first_ids = [window(i, 0, i) for i in range(n_tiles)]
    for i in range(n_tiles):
        loads[i].wait()
        find(i, i, first_ids[i])

    n_windows = jnp.int32(n_tiles)
    for i in range(n_tiles):
        def extra(k, w, i=i):
            find(i, w, window(i, k, w))
            return w + 1
        n_windows = lax.fori_loop(1, (counts[i] + LOOK - 1) // LOOK, extra, n_windows)

    def save(mb):
        return pltpu.make_async_copy(part.at[mb], part_hbm.at[mb], part_sem.at[mb])

    base = n_tiles * LOOK
    for mb in range(mbs):
        part[mb] = dot_tn(picks[mb, 0:base, :], found[0:base, :]).astype(BF16)

        @pl.when(n_windows == n_tiles)
        def _(mb=mb):
            save(mb).start()

    @pl.when(n_windows > n_tiles)
    def _():
        for mb in range(mbs):
            def add(w, _, mb=mb):
                at = look_at(w)
                part[mb] = part[mb] + dot_tn(picks[mb, at, :], found[at, :]).astype(BF16)
                return 0
            lax.fori_loop(n_tiles, n_windows, add, 0)
            save(mb).start()

    for mb in range(mbs):
        save(mb).wait()


def lookup(tok, emb):
    mbs, mtok = tok.shape
    rows, dim = emb.shape
    n_tiles = rows // vocab_tile(rows)
    slots = (n_tiles + mbs * mtok // LOOK) * LOOK
    any_spec = pl.BlockSpec(memory_space=pl.ANY)
    dma = pltpu.SemaphoreType.DMA
    return pl.pallas_call(
        lookup_kernel,
        out_shape=jax.ShapeDtypeStruct((mbs, mtok, dim), BF16),
        in_specs=[pl.BlockSpec(memory_space=pltpu.VMEM), any_spec],
        out_specs=any_spec,
        scratch_shapes=[
            pltpu.VMEM((rows, dim), BF16), pltpu.VMEM((mbs, mtok, dim), BF16), pltpu.VMEM((n_tiles, mbs, mtok), jnp.int32),
            pltpu.VMEM((mbs, slots, mtok), BF16), pltpu.VMEM((slots, dim), BF16),
            dma((n_tiles,)), dma((mbs,)),
        ],
        compiler_params=pltpu.CompilerParams(vmem_limit_bytes=VMEM_LIMIT),
        name="lookup",
    )(tok, emb)


E_ROWS = 512
LOOKUP_LEAD = 8
LOOKUP_PARENT = {2: (3, 0), 1: (0, 0), 4: (5, 0), 6: (7, 0), 5: (3, 1), 7: (0, 1), 3: (0, 2)}
GRAD_PARENT = {0: (1, 0), 2: (3, 0), 4: (5, 0), 1: (6, 0), 6: (7, 0), 3: (5, 1), 5: (7, 1)}


def step_kernel(
    n_stage, lab_ref, part_hbm, emb_hbm, w1_hbm, w2_hbm,
    slope_out, hid_out, dpre_out, xin_out, n_out, g_out, gx_out, dt_out, ge_out, loss_out,
    emb, w1, w2, x_in, x_out, n_all, comb, buf_a, buf_b, slope_stg, act_stg, stats, loss_acc,
    load_sem, part_sem, lk_send, lk_a, lk_b, lk_c, x_send, x_recv, n_send, n_recv, st_send, st_recv,
    g_send, g_a, g_b, b_send, b_recv, gx_send, gx_recv, slope_sem, act_sem, d_sem, e_sem, out_sem, gx_sem,
):
    s = lax.axis_index("stage")
    last = n_stage - 1
    mbs, mtok, dim = x_in.shape
    n_half = mtok // CHUNK
    n_chunks = mbs * n_half
    rows = emb.shape[0]
    ffn = w1.shape[1]
    tile = vocab_tile(rows)
    tokens = HEAD_MBS * mtok
    rounds = mbs // HEAD_MBS
    scale = dim ** -0.5
    c2 = LOG2E * scale
    row_start = s * rows
    bufs = (buf_a, buf_b, x_in)
    lk_sems = (lk_a, lk_b, lk_c)

    loads = [pltpu.make_async_copy(src, dst, load_sem.at[i])
             for i, (src, dst) in enumerate([(w1_hbm, w1), (w2_hbm, w2), (emb_hbm, emb)])]
    part_load = pltpu.make_async_copy(part_hbm, comb, part_sem.at[0])
    part_load.start()
    group_barrier(s, n_stage)

    def pos(c):
        return (c // n_half, pl.ds(pl.multiple_of(lax.rem(c, n_half) * CHUNK, CHUNK), CHUNK))

    def at_chunk(ref, c):
        return ref.at[c // n_half, pl.ds(pl.multiple_of(lax.rem(c, n_half) * CHUNK, CHUNK), CHUNK)]

    def loop(lo, hi, fn):
        def body(i, _):
            fn(i)
            return 0
        lax.fori_loop(lo, hi, body, 0)

    def chunks_of(mb, fn):
        loop(mb * n_half, (mb + 1) * n_half, fn)

    def each_role(roles, fn):
        for node in roles:
            @pl.when(s == node)
            def _(node=node):
                fn(node)

    def lk_copy(c, child):
        parent, slot = LOOKUP_PARENT[child]
        return remote(at_chunk(comb, c), at_chunk(bufs[slot], c), lk_send.at[0], lk_sems[slot].at[c], parent)

    def lk_total(c, slots):
        total = comb[pos(c)].astype(F32)
        for slot in range(slots):
            remote(at_chunk(comb, c), at_chunk(bufs[slot], c), lk_send.at[0], lk_sems[slot].at[c], 0).wait_recv()
            total = total + bufs[slot][pos(c)].astype(F32)
        return total.astype(BF16)

    def lk_forward(c, node, slots):
        comb[pos(c)] = lk_total(c, slots)
        lk_copy(c, node).start()

    part_load.wait()
    each_role((1, 2, 4, 6), lambda node: loop(0, n_chunks, lambda c: lk_copy(c, node).start()))
    for ld in loads:
        ld.start()
    each_role((5, 7), lambda node: loop(0, n_chunks, lambda c: lk_forward(c, node, 1)))
    each_role((3,), lambda node: loop(0, LOOKUP_LEAD, lambda c: lk_forward(c, node, 2)))
    loads[0].wait()
    loads[1].wait()

    n_routes = {last: (5, 1, 6), 5: (4,), 1: (3, 0), 3: (2,)}

    def x_copy(c, dst_stage):
        return remote(at_chunk(x_out, c), at_chunk(x_in, c), x_send.at[0], x_recv.at[c], dst_stage)

    def n_copy(c, lane, dst_stage):
        return remote(at_chunk(n_all, c), at_chunk(n_all, c), n_send.at[lane], n_recv.at[c], dst_stage)

    def fwd_copies(c):
        slot = lax.rem(c, 2)
        return (pltpu.make_async_copy(slope_stg.at[slot], slope_out.at[c], slope_sem.at[slot]),
                pltpu.make_async_copy(act_stg.at[slot], hid_out.at[c], act_sem.at[slot]))

    def slope_copy(c):
        slot = lax.rem(c, 2)
        return pltpu.make_async_copy(slope_out.at[c], slope_stg.at[slot], slope_sem.at[slot])

    def fwd_chunk(c):
        idx = pos(c)

        @pl.when((s == 3) & (c + LOOKUP_LEAD < n_chunks))
        def _():
            lk_forward(c + LOOKUP_LEAD, 3, 2)

        @pl.when(s == 0)
        def _():
            x_in[idx] = lk_total(c, 3)

        @pl.when(s > 0)
        def _():
            x_copy(c, 0).wait_recv()

        @pl.when(c >= 2)
        def _():
            for cp in fwd_copies(c - 2):
                cp.wait()

        slot = lax.rem(c, 2)
        out = forward_chunk(x_in[idx], w1, w2, slope_stg.at[slot], act_stg.at[slot]).astype(BF16)
        x_out[idx] = out
        for cp in fwd_copies(c):
            cp.start()

        @pl.when(s < last)
        def _():
            x_copy(c, s + 1).start()

        @pl.when(s == last)
        def _():
            out_f = out.astype(F32)
            n_all[idx] = (out_f * norm_scale(out_f)).astype(BF16)
            for lane, dst in enumerate(n_routes[last]):
                n_copy(c, lane, dst).start()

    def last_fwd_pair(mb):
        first = mb * n_half
        for c in (first, first + 1):
            x_copy(c, 0).wait_recv()
            for cp in fwd_copies(c - 2):
                cp.wait()
        out = forward_pair(x_in[mb], w1, w2, slope_stg, act_stg).astype(BF16)
        x_out[mb] = out
        out_f = out.astype(F32)
        n_all[mb] = (out_f * norm_scale(out_f)).astype(BF16)
        for c in (first, first + 1):
            for cp in fwd_copies(c):
                cp.start()
            for lane, dst in enumerate(n_routes[last]):
                n_copy(c, lane, dst).start()

    def n_round(r, fn):
        loop(r * HEAD_MBS * n_half, (r + 1) * HEAD_MBS * n_half, fn)

    def n_early(r):
        def take(c, node):
            n_copy(c, 0, 0 if node == last else last).wait_recv()
            for lane, dst in enumerate(n_routes[node]):
                n_copy(c, lane, dst).start()
        each_role((1, 5), lambda node: n_round(r, lambda c: take(c, node)))

    def n_mid(r):
        def take(c, node):
            n_copy(c, 0, last).wait_recv()
            n_copy(c, 0, n_routes[node][0]).start()
        each_role((3,), lambda node: n_round(r, lambda c: take(c, node)))

    def n_late(r):
        @pl.when((lax.rem(s, 2) == 0))
        def _():
            n_round(r, lambda c: n_copy(c, 0, last).wait_recv())

    def g_copy(mb, child):
        parent, slot = GRAD_PARENT[child]
        return remote(comb.at[mb], bufs[slot].at[mb], g_send.at[0], (g_a, g_b)[slot].at[mb], parent)

    def g_total(mb, slots):
        total = comb[mb].astype(F32)
        for slot in range(slots):
            remote(comb.at[mb], bufs[slot].at[mb], g_send.at[0], (g_a, g_b)[slot].at[mb], 0).wait_recv()
            total = total + bufs[slot][mb].astype(F32)
        return total

    def g_forward(mb, node, slots):
        comb[mb] = g_total(mb, slots).astype(BF16)
        g_copy(mb, node).start()

    def g_low(r):
        each_role((1, 3), lambda node: loop(r * HEAD_MBS, (r + 1) * HEAD_MBS, lambda mb: g_forward(mb, node, 1)))

    def g_mid(r):
        each_role((6,), lambda node: loop(r * HEAD_MBS, (r + 1) * HEAD_MBS, lambda mb: g_forward(mb, node, 1)))
        each_role((5,), lambda node: loop(r * HEAD_MBS, (r + 1) * HEAD_MBS, lambda mb: g_forward(mb, node, 2)))

    def g_final(mb):
        @pl.when(s == last)
        def _():
            grad_n = g_total(mb, 2)
            x_f = x_out[mb].astype(F32)
            inv = norm_scale(x_f)
            n_f = x_f * inv
            dx = inv * (grad_n - n_f * jnp.mean(grad_n * n_f, axis=-1, keepdims=True))
            comb[mb] = dx.astype(BF16)

    def lab_row_of(r):
        parts = [lab_ref[pl.ds(r * HEAD_MBS + i, 1), :] for i in range(HEAD_MBS)]
        return jnp.concatenate(parts, axis=1) - row_start

    def st_copy(r, off):
        dst = lax.rem(s + off, n_stage)
        return remote(stats.at[r, s], stats.at[r, s], st_send.at[0], st_recv.at[r], dst)

    saves = [pltpu.make_async_copy(x_in, xin_out, out_sem.at[0]), pltpu.make_async_copy(n_all, n_out, out_sem.at[1])]

    def forward_and_head(logits, n_t, d_stg, gn_acc):
        n_tiles = rows // tile

        def head_a(r):
            n_late(r)

            @pl.when(r == rounds - 1)
            def _():
                for cp in saves:
                    cp.start()

            n_t[...] = n_all[pl.ds(r * HEAD_MBS, HEAD_MBS)].reshape(tokens, dim).T
            top, tot, lab = head_logits(n_t, emb, logits, lab_row_of(r), tokens)

            @pl.when(r == rounds - 1)
            def _():
                for cp in saves:
                    cp.wait()

                for src, dsts in n_routes.items():
                    @pl.when(s == src)
                    def _(dsts=dsts):
                        for lane, dst in enumerate(dsts):
                            remote(n_all, n_all, n_send.at[lane], n_recv.at[0], dst).wait_send()
            stats[r, s] = jnp.concatenate([top, tot, lab, jnp.zeros((5, tokens), F32)], axis=0)
            for off in range(1, n_stage):
                st_copy(r, off).start()

        def d_copy(seq):
            slot = lax.rem(seq, 2)
            r = seq // n_tiles
            idx = lax.rem(seq, n_tiles)
            dst = dt_out.at[pl.ds(pl.multiple_of(idx * tile, 16), tile), pl.ds(pl.multiple_of(r * tokens, tokens), tokens)]
            return pltpu.make_async_copy(d_stg.at[slot], dst, d_sem.at[slot])

        def head_b(r):
            @pl.when(r + 1 < rounds)
            def _():
                n_early(r + 1)

            @pl.when((r == rounds - 2) & (s < last))
            def _():
                remote(x_out, x_in, x_send.at[0], x_recv.at[0], 0).wait_send()

            @pl.when(r == jnp.where(s == last, rounds - 1, rounds - 2))
            def _():
                swap_transposed(w1, w2)
            others = stats.at[r, pl.ds(0, last)]
            remote(others, others, st_send.at[0], st_recv.at[r], lax.rem(s + 1, n_stage)).wait_recv()
            blocks = [stats[r, i] for i in range(n_stage)]
            top = blocks[0][0:1]
            for blk in blocks[1:]:
                top = jnp.maximum(top, blk[0:1])
            tot = jnp.zeros_like(top)
            lab = jnp.zeros_like(top)
            for blk in blocks:
                tot = tot + blk[1:2] * jnp.exp2((blk[0:1] - top) * c2)
                lab = lab + blk[2:3]
            loss_acc[...] = loss_acc[...] + (jnp.log(tot) + (top - lab) * scale)
            shift = jnp.log(tot) * LOG2E - math.log2(scale)
            lab_row = lab_row_of(r)

            def tile_step(idx):
                seq = r * n_tiles + idx

                @pl.when(seq >= 2)
                def _():
                    d_copy(seq - 2).wait()
                @pl.when((idx == n_tiles - 1) & (r + 1 < rounds))
                def _():
                    n_mid(r + 1)
                base = pl.multiple_of(idx * tile, 16)
                part = head_grad_tile(base, tile, emb, logits, d_stg.at[lax.rem(seq, 2)], lab_row, top, shift, tokens)
                gn_acc[...] = gn_acc[...] + part
                d_copy(seq).start()

            gn_acc[...] = jnp.zeros_like(gn_acc)
            loop(0, n_tiles, tile_step)
            comb[pl.ds(r * HEAD_MBS, HEAD_MBS)] = gn_acc[...].reshape(HEAD_MBS, mtok, dim).astype(BF16)
            each_role((0, 2, 4), lambda node: loop(r * HEAD_MBS, (r + 1) * HEAD_MBS, lambda mb: g_copy(mb, node).start()))
        loss_acc[...] = jnp.zeros_like(loss_acc)
        first_a = HEAD_MBS + 1 + last

        def step(k):
            f_mb = k - s

            paired = (s == last) & (f_mb >= 2 * HEAD_MBS)

            @pl.when((f_mb >= 0) & (f_mb < mbs) & jnp.logical_not(paired))
            def _():
                chunks_of(f_mb, fwd_chunk)

            @pl.when((f_mb < mbs) & paired)
            def _():
                last_fwd_pair(f_mb)

            @pl.when(k == first_a)
            def _():
                loads[2].wait()

                @pl.when(s > 0)
                def _():
                    remote(comb, buf_a, lk_send.at[0], lk_a.at[0], 0).wait_send()

            rel = k - first_a
            r = rel // HEAD_MBS
            even = lax.rem(rel + HEAD_MBS * n_stage, HEAD_MBS) == 0

            @pl.when(k == first_a)
            def _():
                n_early(0)
                n_mid(0)

            @pl.when(even & (rel >= 0))
            def _():
                head_a(r)

            @pl.when(even & (rel >= HEAD_MBS))
            def _():
                g_low(r - 1)

                @pl.when(r == 2)
                def _():
                    loop(0, HEAD_MBS, g_final)

            @pl.when(jnp.logical_not(even) & (rel >= 0))
            def _():
                head_b(r)

            @pl.when(jnp.logical_not(even) & (rel >= HEAD_MBS))
            def _():
                g_mid(r - 1)

        loop(0, first_a + HEAD_MBS * rounds, step)
        for c in (n_chunks - 2, n_chunks - 1):
            for cp in fwd_copies(c):
                cp.wait()
        slope_copy(0).start()
        slope_copy(1).start()
        g_low(rounds - 1)
        for seq in (rounds * n_tiles - 2, rounds * n_tiles - 1):
            d_copy(seq).wait()

    pl.run_scoped(
        forward_and_head,
        pltpu.VMEM((rows, tokens), F32), pltpu.VMEM((dim, tokens), BF16),
        pltpu.VMEM((2, tile, tokens), BF16), pltpu.VMEM((tokens, dim), F32),
    )
    loss_out[...] = jnp.broadcast_to(jnp.sum(loss_acc[...], axis=1, keepdims=True), loss_out.shape)

    g_in, g_buf, gx = x_in, x_out, n_all

    def b_copy(c, dst):
        return remote(at_chunk(g_buf, c), at_chunk(g_in, c), b_send.at[0], b_recv.at[c], dst)

    def gx_copy(c, lane, dst):
        return remote(at_chunk(gx, c), at_chunk(gx, c), gx_send.at[lane], gx_recv.at[c], dst)

    def dpre_copy(c):
        slot = lax.rem(c, 2)
        return pltpu.make_async_copy(act_stg.at[slot], dpre_out.at[c], act_sem.at[slot])

    gx_split = n_chunks // 2
    gx_routes = {0: ((5, n_chunks - 1, n_chunks), (3, 0, n_chunks), (last, 0, n_chunks), (1, 0, n_chunks)), 3: ((2, 0, n_chunks), (5, 0, gx_split)),
                 last: ((6, 0, n_chunks), (5, gx_split, n_chunks - 1)), 5: ((4, 0, n_chunks),)}

    def gx_send_all(c, node):
        for lane, (dst, lo, hi) in enumerate(gx_routes[node]):
            @pl.when((c >= lo) & (c < hi))
            def _(lane=lane, dst=dst):
                gx_copy(c, lane, dst).start()


    def gx_save(c):
        return pltpu.make_async_copy(at_chunk(gx, c), at_chunk(gx_out, c), gx_sem.at[0])

    def bwd_chunk(c):
        slot = lax.rem(c, 2)
        idx = pos(c)

        @pl.when(s < last)
        def _():
            b_copy(c, 0).wait_recv()

        @pl.when(s == last)
        def _():
            g_in[idx] = comb[idx]

        @pl.when(c >= 2)
        def _():
            dpre_copy(c - 2).wait()
        slope_copy(c).wait()
        dx = backward_chunk(g_in[idx], w1, w2, slope_stg.at[slot], act_stg.at[slot]).astype(BF16)

        @pl.when(s > 0)
        def _():
            g_buf[idx] = dx
            b_copy(c, s - 1).start()

        @pl.when(s == 0)
        def _():
            gx[idx] = dx
            gx_send_all(c, 0)
            gx_save(c).start()
        dpre_copy(c).start()

        @pl.when(c + 2 < n_chunks)
        def _():
            slope_copy(c + 2).start()

    full = rows // E_ROWS
    rest = rows - full * E_ROWS

    def backward(n_rows, d_in, e_stg):
        def d_load(i, size=E_ROWS):
            slot = lax.rem(i, 2)
            src = dt_out.at[pl.ds(pl.multiple_of(i * E_ROWS, E_ROWS), size)]
            return pltpu.make_async_copy(src, d_in.at[slot, pl.ds(0, size)], d_sem.at[slot])

        def e_save(i, size=E_ROWS):
            slot = lax.rem(i, 2)
            dst = ge_out.at[pl.ds(pl.multiple_of(i * E_ROWS, E_ROWS), size)]
            return pltpu.make_async_copy(e_stg.at[slot, pl.ds(0, size)], dst, e_sem.at[slot])

        def e_tile(i):
            slot = lax.rem(i, 2)

            @pl.when(i + 1 < full)
            def _():
                d_load(i + 1).start()
            if rest:
                @pl.when(i + 1 == full)
                def _():
                    d_load(full, rest).start()
            d_load(i).wait()

            @pl.when(i == 0)
            def _():
                n_load.wait()

            @pl.when(i >= 2)
            def _():
                e_save(i - 2).wait()
            e_stg[slot] = dot_nn(d_in[slot], n_rows[...].reshape(mbs * mtok, dim))
            e_save(i).start()

        n_load = pltpu.make_async_copy(n_out, n_rows, out_sem.at[1])
        n_load.start()
        d_load(0).start()
        early = jnp.where(s == last - 1, 0, jnp.minimum((last - s) * 2, full))
        loop(0, early, e_tile)

        def g_save(mb, count):
            at = pl.ds(mb, count)
            return pltpu.make_async_copy(g_in.at[at], g_out.at[at], out_sem.at[0])

        def gx_forward(c):
            gx_copy(c, 0, 0).wait_recv()
            each_role((3, last, 5), lambda node: gx_send_all(c, node))
            gx_save(c).start()

        def step(k):
            @pl.when(k >= HEAD_MBS)
            def _():
                @pl.when(k < mbs)
                def _():
                    g_final(k)
            b_mb = k - (last - s)

            @pl.when(b_mb == mbs - 1)
            def _():
                g_save(0, mbs - 1).start()

            @pl.when((b_mb >= 0) & (b_mb < mbs))
            def _():
                chunks_of(b_mb, bwd_chunk)

            @pl.when(k == 2)
            def _():
                g_mid(rounds - 1)

            x_mb = k - n_stage

            @pl.when((s == 3) & (x_mb >= 0) & (x_mb < gx_split // n_half))
            def _():
                chunks_of(x_mb, gx_forward)

        loop(0, mbs + last, step)
        g_save(mbs - 1, 1).start()
        loop(early, full, e_tile)
        if rest:
            d_load(full, rest).wait()
            e_save(full - 2).wait()
            slot = full % 2
            e_stg[slot, pl.ds(0, rest)] = dot_nn(d_in[slot, pl.ds(0, rest)], n_rows[...].reshape(mbs * mtok, dim))
            e_save(full, rest).start()

        loop(jnp.where(s == 0, n_chunks, jnp.where(s == 3, gx_split, 0)), n_chunks, gx_forward)

        for c in (n_chunks - 2, n_chunks - 1):
            dpre_copy(c).wait()
        pltpu.make_async_copy(g_in, g_out, out_sem.at[0]).wait()
        if rest:
            e_save(full - 1).wait()
            e_save(full, rest).wait()
        else:
            e_save(full - 2).wait()
            e_save(full - 1).wait()
        pltpu.make_async_copy(gx, gx_out, gx_sem.at[0]).wait()
        sent = stats.at[:, pl.ds(0, last)]
        remote(sent, sent, st_send.at[0], st_recv.at[0], lax.rem(s + 1, n_stage)).wait_send()

        @pl.when(s < last)
        def _():
            remote(comb, buf_a, g_send.at[0], g_a.at[0], last).wait_send()

        @pl.when(s > 0)
        def _():
            remote(g_buf, g_in, b_send.at[0], b_recv.at[0], 0).wait_send()
        for src, routes in gx_routes.items():
            @pl.when(s == src)
            def _(routes=routes):
                for lane, (dst, lo, hi) in enumerate(routes):
                    part = gx if hi - lo == n_chunks else gx.at[pl.ds(0, hi - lo), pl.ds(0, CHUNK)]
                    remote(part, part, gx_send.at[lane], gx_recv.at[0], dst).wait_send()

    pl.run_scoped(
        backward,
        pltpu.VMEM((mbs, mtok, dim), BF16), pltpu.VMEM((2, E_ROWS, mbs * mtok), BF16), pltpu.VMEM((2, E_ROWS, dim), F32),
    )


def pipeline_step(n_stage, labels, part, emb, w1, w2):
    mbs, mtok, dim = part.shape
    rows = emb.shape[0]
    ffn = w1.shape[1]
    chunks = mbs * mtok // CHUNK
    rounds = mbs // HEAD_MBS
    tokens = HEAD_MBS * mtok
    any_spec = pl.BlockSpec(memory_space=pl.ANY)
    vmem_spec = pl.BlockSpec(memory_space=pltpu.VMEM)
    act = pltpu.VMEM((mbs, mtok, dim), BF16)
    dma = pltpu.SemaphoreType.DMA
    act_shape = jax.ShapeDtypeStruct((mbs, mtok, dim), BF16)
    hid_shape = jax.ShapeDtypeStruct((chunks, CHUNK, ffn), BF16)
    return pl.pallas_call(
        functools.partial(step_kernel, n_stage),
        out_shape=(
            jax.ShapeDtypeStruct((chunks, CHUNK, ffn), F32), hid_shape, hid_shape,
            act_shape, act_shape, act_shape, act_shape,
            jax.ShapeDtypeStruct((rows, mbs * mtok), BF16),
            jax.ShapeDtypeStruct((rows, dim), F32),
            jax.ShapeDtypeStruct((8, 128), F32),
        ),
        in_specs=[vmem_spec] + [any_spec] * 4,
        out_specs=(any_spec,) * 9 + (vmem_spec,),
        scratch_shapes=[
            pltpu.VMEM((rows, dim), BF16), pltpu.VMEM((dim, ffn), BF16), pltpu.VMEM((ffn, dim), BF16),
            act, act, act, act, act, act,
            pltpu.VMEM((2, CHUNK, ffn), F32), pltpu.VMEM((2, CHUNK, ffn), BF16),
            pltpu.VMEM((rounds, n_stage, 8, tokens), F32), pltpu.VMEM((1, tokens), F32),
            dma((3,)), dma((1,)), dma((1,)), dma((chunks,)), dma((chunks,)), dma((chunks,)),
            dma((1,)), dma((chunks,)), dma((3,)), dma((chunks,)), dma((1,)), dma((rounds,)),
            dma((1,)), dma((mbs,)), dma((mbs,)), dma((1,)), dma((chunks,)), dma((4,)), dma((chunks,)),
            dma((2,)), dma((2,)), dma((2,)), dma((2,)), dma((2,)), dma((1,)),
        ],
        compiler_params=pltpu.CompilerParams(collective_id=0, has_side_effects=True, vmem_limit_bytes=VMEM_LIMIT),
        name="pipeline_step",
    )(labels, part, emb, w1, w2)


WINDOW = 256
W_COLS = 1024
E_SLOTS = 4


def tail_kernel(
    rows, tok_ref, loss_ref, x_hbm, g_hbm, gx_hbm, dpre_hbm, hid_hbm, ge_hbm,
    loss_out, g1_out, g2_out, out_hbm,
    x_buf, g_buf, gx_buf, dp_buf, hid_buf, g1_stg, g2_stg, e_buf, packed, packed_id, bounds,
    act_sem, dp_sem, hid_sem, g1_sem, g2_sem, e_in_sem, e_out_sem,
):
    mbs, mtok = tok_ref.shape
    total, dim = g_buf.shape
    ffn = dpre_hbm.shape[1]
    n_blocks = ffn // W_COLS
    e_rows = e_buf.shape[1]
    n_e = rows // e_rows
    per_block = n_e // n_blocks

    def cols(j):
        return pl.ds(pl.multiple_of(j * W_COLS, W_COLS), W_COLS)

    def e_at(i):
        return pl.ds(pl.multiple_of(i * e_rows, 8), e_rows)

    def dp_load(j):
        slot = lax.rem(j, 2)
        return pltpu.make_async_copy(dpre_hbm.at[:, cols(j)], dp_buf.at[slot], dp_sem.at[slot])

    def hid_load(j):
        slot = lax.rem(j, 2)
        return pltpu.make_async_copy(hid_hbm.at[:, cols(j)], hid_buf.at[slot], hid_sem.at[slot])

    def e_load(i):
        slot = lax.rem(i, E_SLOTS)
        return pltpu.make_async_copy(ge_hbm.at[e_at(i)], e_buf.at[slot], e_in_sem.at[slot])

    def e_save(i):
        slot = lax.rem(i, E_SLOTS)
        return pltpu.make_async_copy(e_buf.at[slot], out_hbm.at[e_at(i)], e_out_sem.at[slot])

    def g1_save(j):
        return pltpu.make_async_copy(g1_stg, g1_out.at[0, :, cols(j)], g1_sem.at[0])

    def g2_save(j):
        return pltpu.make_async_copy(g2_stg, g2_out.at[0, cols(j)], g2_sem.at[0])

    x_load = pltpu.make_async_copy(x_hbm, x_buf, act_sem.at[0])
    g_load = pltpu.make_async_copy(g_hbm, g_buf, act_sem.at[1])
    gx_load = pltpu.make_async_copy(gx_hbm, gx_buf, act_sem.at[2])
    gx_load.start()
    loss_out[0] = loss_ref[0, 0] * (1.0 / total)

    s = lax.axis_index("stage")
    loc = tok_ref[...] - s * rows
    upper, lower = triangles(mbs, mtok)
    slot_of = jnp.full((mbs, mtok), -1.0, F32)
    count = jnp.int32(0)
    bounds[0] = count
    for i in range(n_e):
        inside = (loc >= i * e_rows) & (loc < (i + 1) * e_rows)
        rank, number = ranks(inside.astype(F32), upper, lower)
        slot_of = jnp.where(inside, rank + count.astype(F32), slot_of)
        count = count + number
        bounds[i + 1] = count
    slot_of = slot_of.astype(jnp.int32)
    n_packs = jnp.maximum((count + WINDOW - 1) // WINDOW, 1)

    def pack(b):
        slot = lax.broadcasted_iota(jnp.int32, (WINDOW, mtok), 0) + b * WINDOW
        ids = jnp.zeros((WINDOW, 1), F32)
        picks = []
        for mb in range(mbs):
            pick = slot == slot_of[mb:mb + 1, :]
            picks.append(pick.astype(BF16))
            ids = ids + jnp.sum(jnp.where(pick, loc[mb:mb + 1, :].astype(F32), 0.0), axis=1, keepdims=True)
        at = pl.ds(pl.multiple_of(b * WINDOW, WINDOW), WINDOW)
        packed[at, :] = dot_nn(jnp.concatenate(picks, axis=1), gx_buf[...]).astype(BF16)
        filled = lax.broadcasted_iota(jnp.int32, (WINDOW, 1), 0) + b * WINDOW < count
        packed_id[at, :] = jnp.broadcast_to(jnp.where(filled, ids.astype(jnp.int32), -1), (WINDOW, 128))

    def loop(lo, hi, fn):
        def body(i, _):
            fn(i)
            return 0
        lax.fori_loop(lo, hi, body, 0)

    def e_tile(i):
        slot = lax.rem(i, E_SLOTS)
        first = jnp.minimum((bounds[i] // 16) * 16, (n_packs - 1) * WINDOW)
        lane = lax.broadcasted_iota(jnp.int32, (WINDOW, e_rows), 1) + i * e_rows

        def window(k):
            start = pl.multiple_of(jnp.minimum(first + k * WINDOW, (n_packs - 1) * WINDOW), 16)
            at = pl.ds(start, WINDOW)
            fresh = lax.broadcasted_iota(jnp.int32, (WINDOW, 1), 0) + start >= first + k * WINDOW
            ids = jnp.where(fresh, packed_id[at, :][:, 0:1], -1)
            return dot_tn((lane == ids).astype(BF16), packed[at, :])

        e_load(i).wait()
        e_buf[slot] = e_buf[slot] + window(0)

        def more(k):
            e_buf[slot] = e_buf[slot] + window(k)

        loop(1, (bounds[i + 1] - first + WINDOW - 1) // WINDOW, more)
        e_save(i).start()

    def block(j):
        slot = lax.rem(j, 2)

        @pl.when(j == 0)
        def _():
            x_load.wait()

        @pl.when(j > 0)
        def _():
            g1_save(j - 1).wait()
        dp_load(j).wait()

        @pl.when(j == 0)
        def _():
            for cp in (e_load(0), e_load(1), g_load, hid_load(0)):
                cp.start()
        g1_stg[...] = dot_tn(x_buf[...], dp_buf[slot])
        g1_save(j).start()

        @pl.when(j + 1 < n_blocks)
        def _():
            dp_load(j + 1).start()

        def tile(i):
            @pl.when(i + 2 < n_e)
            def _():
                @pl.when(i + 2 >= E_SLOTS)
                def _():
                    e_save(i + 2 - E_SLOTS).wait()
                e_load(i + 2).start()
            e_tile(i)

        loop(j * per_block, (j + 1) * per_block, tile)

        @pl.when(j == 0)
        def _():
            g_load.wait()

        @pl.when(j > 0)
        def _():
            g2_save(j - 1).wait()
        hid_load(j).wait()

        @pl.when(j + 1 < n_blocks)
        def _():
            hid_load(j + 1).start()
        g2_stg[...] = dot_tn(hid_buf[slot], g_buf[...])
        g2_save(j).start()

    x_load.start()
    dp_load(0).start()
    gx_load.wait()
    loop(0, n_packs, pack)
    loop(0, n_blocks, block)
    g1_save(n_blocks - 1).wait()
    g2_save(n_blocks - 1).wait()
    for i in range(max(n_e - E_SLOTS, 0), n_e):
        e_save(i).wait()


def tail(tok, loss, x, g, gx, dpre, hid, ge):
    rows, dim = ge.shape
    total, ffn = dpre.shape
    n_blocks = ffn // W_COLS
    e_rows = rows // (2 * n_blocks)
    n_e = rows // e_rows
    any_spec = pl.BlockSpec(memory_space=pl.ANY)
    vmem_spec = pl.BlockSpec(memory_space=pltpu.VMEM)
    dma = pltpu.SemaphoreType.DMA
    act = pltpu.VMEM((total, dim), BF16)
    return pl.pallas_call(
        functools.partial(tail_kernel, rows),
        out_shape=(
            jax.ShapeDtypeStruct((1,), F32),
            jax.ShapeDtypeStruct((1, dim, ffn), F32),
            jax.ShapeDtypeStruct((1, ffn, dim), F32),
            jax.ShapeDtypeStruct((rows, dim), F32),
        ),
        in_specs=[vmem_spec, vmem_spec] + [any_spec] * 6,
        out_specs=(pl.BlockSpec(memory_space=pltpu.SMEM), any_spec, any_spec, any_spec),
        scratch_shapes=[
            act, act, act, pltpu.VMEM((2, total, W_COLS), BF16), pltpu.VMEM((2, total, W_COLS), BF16),
            pltpu.VMEM((dim, W_COLS), F32), pltpu.VMEM((W_COLS, dim), F32), pltpu.VMEM((E_SLOTS, e_rows, dim), F32),
            pltpu.VMEM((total, dim), BF16), pltpu.VMEM((total, 128), jnp.int32), pltpu.SMEM((n_e + 1,), jnp.int32),
            dma((3,)), dma((2,)), dma((2,)), dma((1,)), dma((1,)), dma((E_SLOTS,)), dma((E_SLOTS,)),
        ],
        compiler_params=pltpu.CompilerParams(vmem_limit_bytes=VMEM_LIMIT),
        name="tail",
    )(tok, loss, x, g, gx, dpre, hid, ge)


def solution(mesh):
    n_stage = mesh.shape["stage"]

    def stage_body(token_ids, label_ids, emb_rows, w_in, w_out):
        tokens = token_ids.shape[0] * token_ids.shape[1]
        part = lookup(token_ids, emb_rows)
        _, hid, dpre, x_in, _, g_all, gx, _, ge, loss = pipeline_step(n_stage, label_ids, part, emb_rows, w_in[0], w_out[0])
        flat = lambda a: a.reshape(tokens, a.shape[-1])
        mean_loss, grad_in, grad_out, grad_emb = tail(token_ids, loss, flat(x_in), flat(g_all), flat(gx), flat(dpre), flat(hid), ge)
        return mean_loss, grad_in, grad_out, grad_emb

    return jax.shard_map(
        stage_body,
        mesh=mesh,
        in_specs=(P("dp", None), P("dp", None), P("stage", None), P("stage", None, None), P("stage", None, None)),
        out_specs=(P("dp"), P(("dp", "stage"), None, None), P(("dp", "stage"), None, None), P(("dp", "stage"), None)),
        check_vma=False,
    )
```

```python
import functools
import math

import jax
import jax.numpy as jnp
from jax import lax
from jax.experimental import pallas as pl
from jax.experimental.pallas import tpu as pltpu
from jax.sharding import PartitionSpec as P

NORM_EPS = 1e-6
MESH = pl.DeviceIdType.MESH
F32 = jnp.float32
BF16 = jnp.bfloat16
GELU_A = math.sqrt(2.0 / math.pi)
GELU_B = 0.044715
LOG2E = math.log2(math.e)
CHUNK = 128
HEAD_MBS = 2
VMEM_LIMIT = 67_000_000


def dot_nn(a, b):
    return lax.dot_general(a, b, (((1,), (0,)), ((), ())), preferred_element_type=F32)


def dot_nt(a, b):
    return lax.dot_general(a, b, (((1,), (1,)), ((), ())), preferred_element_type=F32)


def dot_tn(a, b):
    return lax.dot_general(a, b, (((0,), (0,)), ((), ())), preferred_element_type=F32)


def gelu_and_slope(pre):
    sq = pre * pre
    th = jnp.tanh(pre * (GELU_A + (GELU_A * GELU_B) * sq))
    half_sum = 0.5 + 0.5 * th
    hid = pre * half_sum
    slope = half_sum + (hid - hid * th) * (GELU_A + (3.0 * GELU_A * GELU_B) * sq)
    return hid, slope


def norm_scale(x_f32):
    return lax.rsqrt(jnp.mean(x_f32 * x_f32, axis=-1, keepdims=True) + NORM_EPS)


def remote(src, dst, send_sem, recv_sem, stage):
    return pltpu.make_async_remote_copy(
        src_ref=src, dst_ref=dst, send_sem=send_sem, recv_sem=recv_sem, device_id={"stage": stage}, device_id_type=MESH
    )


def group_barrier(stage, n_stage):
    barrier = pltpu.get_barrier_semaphore()
    for off in range(1, n_stage):
        pl.semaphore_signal(barrier, inc=1, device_id={"stage": lax.rem(stage + off, n_stage)}, device_id_type=MESH)
    pl.semaphore_wait(barrier, n_stage - 1)


def vocab_tile(rows):
    for parts in range(2, rows + 1):
        if rows % parts == 0 and (rows // parts) % 16 == 0 and rows // parts <= 2400:
            return rows // parts
    return rows


def sub_blocks(rows, size):
    return [(start, min(size, rows - start)) for start in range(0, rows, size)]


def forward_chunk(x, w1, w2, slope_slot, hid_slot):
    ffn = w1.shape[1]
    width = ffn // 4
    for part in range(4):
        cols = pl.ds(part * width, width)
        hid, slope = gelu_and_slope(dot_nn(x, w1[:, cols]))
        slope_slot[:, cols] = slope
        hid_slot[:, cols] = hid.astype(BF16)
    return x.astype(F32) + dot_nn(hid_slot[...], w2[...])


def forward_pair(x, w1, w2, slope_slots, hid_slots):
    ffn = w1.shape[1]
    width = ffn // 4
    for part in range(4):
        cols = pl.ds(part * width, width)
        hid, slope = gelu_and_slope(dot_nn(x, w1[:, cols]))
        for slot in range(2):
            slope_slots[slot, :, cols] = slope[slot * CHUNK:(slot + 1) * CHUNK]
            hid_slots[slot, :, cols] = hid[slot * CHUNK:(slot + 1) * CHUNK].astype(BF16)
    return x.astype(F32) + dot_nn(hid_slots[...].reshape(2 * CHUNK, ffn), w2[...])


def backward_chunk(grad, w2_t, w1_t, slope_slot, dpre_slot):
    ffn = slope_slot.shape[1]
    dim = grad.shape[1]
    for part in range(ffn // dim):
        cols = pl.ds(part * dim, dim)
        dpre_slot[:, cols] = (dot_nn(grad, w2_t[:, cols]) * slope_slot[:, cols]).astype(BF16)
    return grad.astype(F32) + dot_nn(dpre_slot[...], w1_t[...])


def swap_transposed(w1, w2):
    dim, ffn = w1.shape
    side = 256

    def strip(part, _):
        at = pl.ds(pl.multiple_of(part * side, side), side)
        for i in range(dim // side):
            rows = pl.ds(i * side, side)
            from_w1 = w1[rows, at].T
            from_w2 = w2[at, rows].T
            w2[at, rows] = from_w1
            w1[rows, at] = from_w2
        return 0

    lax.fori_loop(0, ffn // side, strip, 0)


def head_logits(n_t, emb, logits, lab_row, tokens):
    rows = emb.shape[0]
    tile = vocab_tile(rows)
    c2 = LOG2E * emb.shape[1] ** -0.5

    def tile_step(idx, carry):
        mx, sm, lb = carry
        base = pl.multiple_of(idx * tile, 16)
        for start, size in sub_blocks(tile, 256):
            at = pl.ds(base + start, size)
            block = dot_nn(emb[at, :], n_t[...])
            logits[at, :] = block
            b3 = block.reshape(size // 8, 8, tokens)
            row_ids = lax.broadcasted_iota(jnp.int32, (size, tokens), 0) + (base + start)
            hit = jnp.where(row_ids == lab_row, block, 0.0).reshape(size // 8, 8, tokens)
            mx_new = jnp.maximum(mx, jnp.max(b3, axis=0))
            sm = sm * jnp.exp2((mx - mx_new) * c2) + jnp.sum(jnp.exp2((b3 - mx_new[None]) * c2), axis=0)
            lb = lb + jnp.sum(hit, axis=0)
            mx = mx_new
        return mx, sm, lb

    init = (jnp.full((8, tokens), -3.0e38, F32), jnp.zeros((8, tokens), F32), jnp.zeros((8, tokens), F32))
    mx, sm, lb = lax.fori_loop(0, rows // tile, tile_step, init)
    top = jnp.max(mx, axis=0, keepdims=True)
    tot = jnp.sum(sm * jnp.exp2((mx - top) * c2), axis=0, keepdims=True)
    lab = jnp.sum(lb, axis=0, keepdims=True)
    return top, tot, lab


def head_grad_tile(base, size_all, emb, logits, d_slot, lab_row, top, shift, tokens):
    scale = emb.shape[1] ** -0.5
    c2 = LOG2E * scale
    total = None
    for start, size in sub_blocks(size_all, 256):
        at = pl.ds(base + start, size)
        row_ids = lax.broadcasted_iota(jnp.int32, (size, tokens), 0) + (base + start)
        prob = jnp.exp2((logits[at, :] - top) * c2 - shift)
        d_log = (prob - jnp.where(row_ids == lab_row, scale, 0.0)).astype(BF16)
        d_slot[pl.ds(start, size), :] = d_log
        part = dot_tn(d_log, emb[at, :])
        total = part if total is None else total + part
    return total


LOOK = 192
LOOK_BASE = 512


def look_at(row):
    return pl.ds(pl.multiple_of(row, 16), LOOK)


def ranks(flag, upper, lower):
    within = dot_nn(flag.astype(BF16), upper)
    total = jnp.sum(flag, axis=1, keepdims=True)
    rows = flag.shape[0]
    before = jnp.sum(jnp.where(lower, jnp.transpose(jnp.broadcast_to(total, (rows, rows))), 0.0), axis=1, keepdims=True)
    return within - flag + before, jnp.sum(flag).astype(jnp.int32)


def triangles(mbs, mtok):
    upper = (lax.broadcasted_iota(jnp.int32, (mtok, mtok), 0)
             <= lax.broadcasted_iota(jnp.int32, (mtok, mtok), 1)).astype(BF16)
    lower = lax.broadcasted_iota(jnp.int32, (mbs, mbs), 1) < lax.broadcasted_iota(jnp.int32, (mbs, mbs), 0)
    return upper, lower


def lookup_kernel(tok_ref, emb_hbm, part_hbm, emb, part, rank_ref, picks, found, emb_sem, part_sem):
    mbs, mtok = tok_ref.shape
    rows, dim = emb.shape
    tile = vocab_tile(rows)
    n_tiles = rows // tile
    loads = [pltpu.make_async_copy(emb_hbm.at[pl.ds(i * tile, tile)], emb.at[pl.ds(i * tile, tile)], emb_sem.at[i])
             for i in range(n_tiles)]
    for ld in loads:
        ld.start()

    picks[:, pl.ds(0, LOOK_BASE + LOOK), :] = jnp.zeros((mbs, LOOK_BASE + LOOK, mtok), BF16)
    found[pl.ds(0, LOOK_BASE + LOOK), :] = jnp.zeros((LOOK_BASE + LOOK, dim), BF16)
    loc = tok_ref[...] - lax.axis_index("stage") * rows
    upper, lower = triangles(mbs, mtok)
    counts = []
    for i in range(n_tiles):
        inside = (loc >= i * tile) & (loc < (i + 1) * tile)
        rank, number = ranks(inside.astype(F32), upper, lower)
        rank_ref[i] = jnp.where(inside, rank, -1.0).astype(jnp.int32)
        counts.append(number)

    def window(i, k, row):
        slot = lax.broadcasted_iota(jnp.int32, (LOOK, mtok), 0) + k * LOOK
        ids = jnp.zeros((LOOK, 1), F32)
        for mb in range(mbs):
            pick = slot == rank_ref[i, mb:mb + 1, :]
            picks[mb, look_at(row), :] = pick.astype(BF16)
            ids = ids + jnp.sum(jnp.where(pick, loc[mb:mb + 1, :].astype(F32), 0.0), axis=1, keepdims=True)
        filled = lax.broadcasted_iota(jnp.int32, (LOOK, 1), 0) + k * LOOK < counts[i]
        return jnp.where(filled, ids.astype(jnp.int32), -1)

    def find(i, row, ids):
        lane = lax.broadcasted_iota(jnp.int32, (LOOK, tile), 1) + i * tile
        rows_found = dot_nn((lane == ids).astype(BF16), emb[pl.ds(i * tile, tile), :])
        found[look_at(row), :] = rows_found.astype(BF16)

    starts = [jnp.int32(0)]
    for number in counts:
        starts.append(starts[-1] + (jnp.minimum(number, LOOK) + 15) // 16 * 16)
    first_ids = [window(i, 0, starts[i]) for i in range(n_tiles)]
    for i in range(n_tiles):
        loads[i].wait()
        find(i, starts[i], first_ids[i])

    extra_end = jnp.int32(1)
    for i in range(n_tiles):
        def extra(k, w, i=i):
            row = LOOK_BASE + w * LOOK
            find(i, row, window(i, k, row))
            return w + 1
        extra_end = lax.fori_loop(1, (counts[i] + LOOK - 1) // LOOK, extra, extra_end)
    crowded = (extra_end > 1) | (starts[n_tiles] > LOOK_BASE)

    def save(mb):
        return pltpu.make_async_copy(part.at[mb], part_hbm.at[mb], part_sem.at[mb])

    for mb in range(mbs):
        part[mb] = dot_tn(picks[mb, 0:LOOK_BASE, :], found[0:LOOK_BASE, :]).astype(BF16)

        @pl.when(jnp.logical_not(crowded))
        def _(mb=mb):
            save(mb).start()

    @pl.when(crowded)
    def _():
        def add_mb(mb, _):
            def add(w, _):
                at = look_at(LOOK_BASE + w * LOOK)
                part[mb] = part[mb] + dot_tn(picks[mb, at, :], found[at, :]).astype(BF16)
                return 0
            lax.fori_loop(0, extra_end, add, 0)
            save(mb).start()
            return 0
        lax.fori_loop(0, mbs, add_mb, 0)

    for mb in range(mbs):
        save(mb).wait()


def lookup(tok, emb):
    mbs, mtok = tok.shape
    rows, dim = emb.shape
    n_tiles = rows // vocab_tile(rows)
    slots = LOOK_BASE + (1 + mbs * mtok // LOOK) * LOOK
    any_spec = pl.BlockSpec(memory_space=pl.ANY)
    dma = pltpu.SemaphoreType.DMA
    return pl.pallas_call(
        lookup_kernel,
        out_shape=jax.ShapeDtypeStruct((mbs, mtok, dim), BF16),
        in_specs=[pl.BlockSpec(memory_space=pltpu.VMEM), any_spec],
        out_specs=any_spec,
        scratch_shapes=[
            pltpu.VMEM((rows, dim), BF16), pltpu.VMEM((mbs, mtok, dim), BF16), pltpu.VMEM((n_tiles, mbs, mtok), jnp.int32),
            pltpu.VMEM((mbs, slots, mtok), BF16), pltpu.VMEM((slots, dim), BF16),
            dma((n_tiles,)), dma((mbs,)),
        ],
        compiler_params=pltpu.CompilerParams(vmem_limit_bytes=VMEM_LIMIT),
        name="lookup",
    )(tok, emb)


E_ROWS = 512
LATE_TILES = 3
EARLY_TILES = (11, 9, 8, 6, 4, 3, 0, 0)
LOOKUP_LEAD = 8
LOOKUP_PARENT = {2: (3, 0), 1: (0, 0), 4: (5, 0), 6: (7, 0), 5: (3, 1), 7: (0, 1), 3: (0, 2)}
GRAD_PARENT = {0: (1, 0), 2: (3, 0), 4: (5, 0), 1: (6, 0), 6: (7, 0), 3: (5, 1), 5: (7, 1)}


def step_kernel(
    n_stage, lab_ref, part_hbm, emb_hbm, w1_hbm, w2_hbm,
    slope_out, hid_out, dpre_out, xin_out, n_out, g_out, gx_out, dt_out, ge_out, loss_out,
    emb, w1, w2, x_in, x_out, n_all, comb, buf_a, buf_b, slope_stg, act_stg, d_stg, stats, loss_acc,
    load_sem, part_sem, lk_send, lk_a, lk_b, lk_c, x_send, x_recv, n_send, n_recv, st_send, st_recv,
    g_send, g_a, g_b, b_send, b_recv, gx_send, gx_recv, slope_sem, act_sem, dt_sem, d_sem, e_sem, out_sem, gx_sem,
):
    s = lax.axis_index("stage")
    last = n_stage - 1
    mbs, mtok, dim = x_in.shape
    n_half = mtok // CHUNK
    n_chunks = mbs * n_half
    rows = emb.shape[0]
    ffn = w1.shape[1]
    tile = vocab_tile(rows)
    tokens = HEAD_MBS * mtok
    rounds = mbs // HEAD_MBS
    scale = dim ** -0.5
    c2 = LOG2E * scale
    row_start = s * rows
    bufs = (buf_a, buf_b, x_in)
    lk_sems = (lk_a, lk_b, lk_c)

    loads = [pltpu.make_async_copy(src, dst, load_sem.at[i])
             for i, (src, dst) in enumerate([(w1_hbm, w1), (w2_hbm, w2), (emb_hbm, emb)])]
    part_load = pltpu.make_async_copy(part_hbm, comb, part_sem.at[0])
    part_load.start()
    group_barrier(s, n_stage)

    def pos(c):
        return (c // n_half, pl.ds(pl.multiple_of(lax.rem(c, n_half) * CHUNK, CHUNK), CHUNK))

    def at_chunk(ref, c):
        return ref.at[c // n_half, pl.ds(pl.multiple_of(lax.rem(c, n_half) * CHUNK, CHUNK), CHUNK)]

    def loop(lo, hi, fn):
        def body(i, _):
            fn(i)
            return 0
        lax.fori_loop(lo, hi, body, 0)

    def chunks_of(mb, fn):
        loop(mb * n_half, (mb + 1) * n_half, fn)

    def each_role(roles, fn):
        for node in roles:
            @pl.when(s == node)
            def _(node=node):
                fn(node)

    def lk_copy(c, child):
        parent, slot = LOOKUP_PARENT[child]
        return remote(at_chunk(comb, c), at_chunk(bufs[slot], c), lk_send.at[0], lk_sems[slot].at[c], parent)

    def lk_total(c, slots):
        total = comb[pos(c)].astype(F32)
        for slot in range(slots):
            remote(at_chunk(comb, c), at_chunk(bufs[slot], c), lk_send.at[0], lk_sems[slot].at[c], 0).wait_recv()
            total = total + bufs[slot][pos(c)].astype(F32)
        return total.astype(BF16)

    def lk_forward(c, node, slots):
        comb[pos(c)] = lk_total(c, slots)
        lk_copy(c, node).start()

    part_load.wait()
    each_role((1, 2, 4, 6), lambda node: loop(0, n_chunks, lambda c: lk_copy(c, node).start()))
    for ld in loads:
        ld.start()
    each_role((5, 7), lambda node: loop(0, n_chunks, lambda c: lk_forward(c, node, 1)))
    each_role((3,), lambda node: loop(0, LOOKUP_LEAD, lambda c: lk_forward(c, node, 2)))
    loads[0].wait()
    loads[1].wait()

    n_routes = {last: (5, 1, 6), 5: (4,), 1: (3, 0), 3: (2,)}

    def x_copy(c, dst_stage):
        return remote(at_chunk(x_out, c), at_chunk(x_in, c), x_send.at[0], x_recv.at[c], dst_stage)

    def n_copy(c, lane, dst_stage):
        return remote(at_chunk(n_all, c), at_chunk(n_all, c), n_send.at[lane], n_recv.at[c], dst_stage)

    def fwd_copies(c):
        slot = lax.rem(c, 2)
        return (pltpu.make_async_copy(slope_stg.at[slot], slope_out.at[c], slope_sem.at[slot]),
                pltpu.make_async_copy(act_stg.at[slot], hid_out.at[c], act_sem.at[slot]))

    def slope_copy(c):
        slot = lax.rem(c, 2)
        return pltpu.make_async_copy(slope_out.at[c], slope_stg.at[slot], slope_sem.at[slot])

    def fwd_chunk(c):
        idx = pos(c)

        @pl.when((s == 3) & (c + LOOKUP_LEAD < n_chunks))
        def _():
            lk_forward(c + LOOKUP_LEAD, 3, 2)

        @pl.when(s == 0)
        def _():
            x_in[idx] = lk_total(c, 3)

        @pl.when(s > 0)
        def _():
            x_copy(c, 0).wait_recv()

        @pl.when(c >= 2)
        def _():
            for cp in fwd_copies(c - 2):
                cp.wait()

        slot = lax.rem(c, 2)
        out = forward_chunk(x_in[idx], w1, w2, slope_stg.at[slot], act_stg.at[slot]).astype(BF16)
        x_out[idx] = out
        for cp in fwd_copies(c):
            cp.start()

        @pl.when(s < last)
        def _():
            x_copy(c, s + 1).start()

        @pl.when(s == last)
        def _():
            out_f = out.astype(F32)
            n_all[idx] = (out_f * norm_scale(out_f)).astype(BF16)
            for lane, dst in enumerate(n_routes[last]):
                n_copy(c, lane, dst).start()

    def last_fwd_pair(mb):
        first = mb * n_half
        for c in (first, first + 1):
            x_copy(c, 0).wait_recv()
            for cp in fwd_copies(c - 2):
                cp.wait()
        out = forward_pair(x_in[mb], w1, w2, slope_stg, act_stg).astype(BF16)
        x_out[mb] = out
        out_f = out.astype(F32)
        n_all[mb] = (out_f * norm_scale(out_f)).astype(BF16)
        for c in (first, first + 1):
            for cp in fwd_copies(c):
                cp.start()
            for lane, dst in enumerate(n_routes[last]):
                n_copy(c, lane, dst).start()

    def n_round(r, fn):
        loop(r * HEAD_MBS * n_half, (r + 1) * HEAD_MBS * n_half, fn)

    def n_early(r):
        def take(c, node):
            n_copy(c, 0, 0 if node == last else last).wait_recv()
            for lane, dst in enumerate(n_routes[node]):
                n_copy(c, lane, dst).start()
        each_role((1, 5), lambda node: n_round(r, lambda c: take(c, node)))

    def n_mid(r):
        def take(c, node):
            n_copy(c, 0, last).wait_recv()
            n_copy(c, 0, n_routes[node][0]).start()
        each_role((3,), lambda node: n_round(r, lambda c: take(c, node)))

    def n_late(r):
        @pl.when((lax.rem(s, 2) == 0))
        def _():
            n_round(r, lambda c: n_copy(c, 0, last).wait_recv())

    def g_copy(mb, child):
        parent, slot = GRAD_PARENT[child]
        return remote(comb.at[mb], bufs[slot].at[mb], g_send.at[0], (g_a, g_b)[slot].at[mb], parent)

    def g_total(mb, slots):
        total = comb[mb].astype(F32)
        for slot in range(slots):
            remote(comb.at[mb], bufs[slot].at[mb], g_send.at[0], (g_a, g_b)[slot].at[mb], 0).wait_recv()
            total = total + bufs[slot][mb].astype(F32)
        return total

    def g_forward(mb, node, slots):
        comb[mb] = g_total(mb, slots).astype(BF16)
        g_copy(mb, node).start()

    def g_low(r):
        each_role((1, 3), lambda node: loop(r * HEAD_MBS, (r + 1) * HEAD_MBS, lambda mb: g_forward(mb, node, 1)))

    def g_mid(r, nodes=(5, 6)):
        each_role(nodes, lambda node: loop(r * HEAD_MBS, (r + 1) * HEAD_MBS, lambda mb: g_forward(mb, node, {5: 2, 6: 1}[node])))

    def g_final(mb):
        @pl.when(s == last)
        def _():
            grad_n = g_total(mb, 2)
            x_f = x_out[mb].astype(F32)
            inv = norm_scale(x_f)
            n_f = x_f * inv
            dx = inv * (grad_n - n_f * jnp.mean(grad_n * n_f, axis=-1, keepdims=True))
            comb[mb] = dx.astype(BF16)

    def lab_row_of(r):
        parts = [lab_ref[pl.ds(r * HEAD_MBS + i, 1), :] for i in range(HEAD_MBS)]
        return jnp.concatenate(parts, axis=1) - row_start

    def st_copy(r, off):
        dst = lax.rem(s + off, n_stage)
        return remote(stats.at[r, s], stats.at[r, s], st_send.at[0], st_recv.at[r], dst)

    saves = [pltpu.make_async_copy(x_in, xin_out, out_sem.at[0]), pltpu.make_async_copy(n_all, n_out, out_sem.at[1])]

    n_tiles = rows // tile

    def d_copy(seq):
        slot = lax.rem(seq, 2)
        r = seq // n_tiles
        idx = lax.rem(seq, n_tiles)
        dst = dt_out.at[pl.ds(pl.multiple_of(idx * tile, 16), tile), pl.ds(pl.multiple_of(r * tokens, tokens), tokens)]
        return pltpu.make_async_copy(d_stg.at[slot], dst, dt_sem.at[slot])

    def forward_and_head(logits, n_t, gn_acc):
        def head_a(r):
            n_late(r)

            @pl.when(r == rounds - 1)
            def _():
                for cp in saves:
                    cp.start()

            n_t[...] = n_all[pl.ds(r * HEAD_MBS, HEAD_MBS)].reshape(tokens, dim).T
            top, tot, lab = head_logits(n_t, emb, logits, lab_row_of(r), tokens)

            @pl.when(r == rounds - 1)
            def _():
                for cp in saves:
                    cp.wait()

                for src, dsts in n_routes.items():
                    @pl.when(s == src)
                    def _(dsts=dsts):
                        for lane, dst in enumerate(dsts):
                            remote(n_all, n_all, n_send.at[lane], n_recv.at[0], dst).wait_send()
            stats[r, s] = jnp.concatenate([top, tot, lab, jnp.zeros((5, tokens), F32)], axis=0)
            for off in range(1, n_stage):
                st_copy(r, off).start()

        def head_b(r):
            @pl.when(r + 1 < rounds)
            def _():
                n_early(r + 1)

            @pl.when((r == rounds - 2) & (s < last))
            def _():
                remote(x_out, x_in, x_send.at[0], x_recv.at[0], 0).wait_send()

            @pl.when(r == rounds - 1)
            def _():
                for c in (n_chunks - 2, n_chunks - 1):
                    for cp in fwd_copies(c):
                        cp.wait()
                slope_copy(0).start()
                slope_copy(1).start()

            @pl.when(r == jnp.where(s == last, rounds - 1, rounds - 2))
            def _():
                swap_transposed(w1, w2)
            others = stats.at[r, pl.ds(0, last)]
            remote(others, others, st_send.at[0], st_recv.at[r], lax.rem(s + 1, n_stage)).wait_recv()
            blocks = [stats[r, i] for i in range(n_stage)]
            top = blocks[0][0:1]
            for blk in blocks[1:]:
                top = jnp.maximum(top, blk[0:1])
            tot = jnp.zeros_like(top)
            lab = jnp.zeros_like(top)
            for blk in blocks:
                tot = tot + blk[1:2] * jnp.exp2((blk[0:1] - top) * c2)
                lab = lab + blk[2:3]
            loss_acc[...] = loss_acc[...] + (jnp.log(tot) + (top - lab) * scale)
            shift = jnp.log(tot) * LOG2E - math.log2(scale)
            lab_row = lab_row_of(r)

            def tile_step(idx):
                seq = r * n_tiles + idx

                @pl.when(seq >= 2)
                def _():
                    d_copy(seq - 2).wait()
                @pl.when((idx == n_tiles - 1) & (r + 1 < rounds))
                def _():
                    n_mid(r + 1)
                base = pl.multiple_of(idx * tile, 16)
                part = head_grad_tile(base, tile, emb, logits, d_stg.at[lax.rem(seq, 2)], lab_row, top, shift, tokens)
                gn_acc[...] = gn_acc[...] + part
                d_copy(seq).start()

            gn_acc[...] = jnp.zeros_like(gn_acc)
            loop(0, n_tiles, tile_step)
            comb[pl.ds(r * HEAD_MBS, HEAD_MBS)] = gn_acc[...].reshape(HEAD_MBS, mtok, dim).astype(BF16)
            each_role((0, 2, 4), lambda node: loop(r * HEAD_MBS, (r + 1) * HEAD_MBS, lambda mb: g_copy(mb, node).start()))
        loss_acc[...] = jnp.zeros_like(loss_acc)
        first_a = HEAD_MBS + 1 + last

        def step(k):
            f_mb = k - s

            paired = (s == last) & (f_mb >= 2 * HEAD_MBS)

            @pl.when((f_mb >= 0) & (f_mb < mbs) & jnp.logical_not(paired))
            def _():
                chunks_of(f_mb, fwd_chunk)

            @pl.when((f_mb < mbs) & paired)
            def _():
                last_fwd_pair(f_mb)

            @pl.when(k == first_a)
            def _():
                loads[2].wait()

                @pl.when(s > 0)
                def _():
                    remote(comb, buf_a, lk_send.at[0], lk_a.at[0], 0).wait_send()

            rel = k - first_a
            r = rel // HEAD_MBS
            even = lax.rem(rel + HEAD_MBS * n_stage, HEAD_MBS) == 0

            @pl.when(k == first_a)
            def _():
                n_early(0)
                n_mid(0)

            @pl.when(even & (rel >= 0))
            def _():
                head_a(r)

            @pl.when(even & (rel >= HEAD_MBS))
            def _():
                g_low(r - 1)

                @pl.when(r == 2)
                def _():
                    loop(0, HEAD_MBS, g_final)

            @pl.when(jnp.logical_not(even) & (rel >= 0))
            def _():
                head_b(r)

            @pl.when(jnp.logical_not(even) & (rel >= HEAD_MBS))
            def _():
                g_mid(r - 1)

        loop(0, first_a + HEAD_MBS * rounds, step)
        g_low(rounds - 1)

    pl.run_scoped(
        forward_and_head,
        pltpu.VMEM((rows, tokens), F32), pltpu.VMEM((dim, tokens), BF16), pltpu.VMEM((tokens, dim), F32),
    )

    g_in, g_buf, gx = x_in, x_out, n_all

    def b_copy(c, dst):
        return remote(at_chunk(g_buf, c), at_chunk(g_in, c), b_send.at[0], b_recv.at[c], dst)

    def gx_copy(c, lane, dst):
        return remote(at_chunk(gx, c), at_chunk(gx, c), gx_send.at[lane], gx_recv.at[c], dst)

    def dpre_copy(c):
        slot = lax.rem(c, 2)
        return pltpu.make_async_copy(act_stg.at[slot], dpre_out.at[c], act_sem.at[slot])

    gx_split = n_chunks // 2
    gx_routes = {0: ((5, n_chunks - 1, n_chunks), (3, 0, n_chunks), (last, 0, n_chunks), (1, 0, n_chunks)), 3: ((2, 0, n_chunks), (5, 0, gx_split)),
                 last: ((6, 0, n_chunks), (5, gx_split, n_chunks - 1)), 5: ((4, 0, n_chunks),)}

    def gx_send_all(c, node):
        for lane, (dst, lo, hi) in enumerate(gx_routes[node]):
            @pl.when((c >= lo) & (c < hi))
            def _(lane=lane, dst=dst):
                gx_copy(c, lane, dst).start()


    def gx_save(c):
        return pltpu.make_async_copy(at_chunk(gx, c), at_chunk(gx_out, c), gx_sem.at[0])

    def bwd_chunk(c):
        slot = lax.rem(c, 2)
        idx = pos(c)

        @pl.when(s < last)
        def _():
            b_copy(c, 0).wait_recv()

        @pl.when(s == last)
        def _():
            g_in[idx] = comb[idx]

        @pl.when(c >= 2)
        def _():
            dpre_copy(c - 2).wait()
        slope_copy(c).wait()
        dx = backward_chunk(g_in[idx], w1, w2, slope_stg.at[slot], act_stg.at[slot]).astype(BF16)

        @pl.when(s > 0)
        def _():
            g_buf[idx] = dx
            b_copy(c, s - 1).start()

        @pl.when(s == 0)
        def _():
            gx[idx] = dx
            gx_send_all(c, 0)
            gx_save(c).start()
        dpre_copy(c).start()

        @pl.when(c + 2 < n_chunks)
        def _():
            slope_copy(c + 2).start()

    full = rows // E_ROWS
    rest = rows - full * E_ROWS

    def backward(n_rows, d_in, e_stg):
        def d_load(i, size=E_ROWS):
            slot = lax.rem(i, 2)
            src = dt_out.at[pl.ds(pl.multiple_of(i * E_ROWS, E_ROWS), size)]
            return pltpu.make_async_copy(src, d_in.at[slot, pl.ds(0, size)], d_sem.at[slot])

        def e_save(i, size=E_ROWS):
            slot = lax.rem(i, 2)
            dst = ge_out.at[pl.ds(pl.multiple_of(i * E_ROWS, E_ROWS), size)]
            return pltpu.make_async_copy(e_stg.at[slot, pl.ds(0, size)], dst, e_sem.at[slot])

        def e_tile(i):
            slot = lax.rem(i, 2)

            @pl.when(i + 1 < full)
            def _():
                d_load(i + 1).start()
            if rest:
                @pl.when(i + 1 == full)
                def _():
                    d_load(full, rest).start()
            d_load(i).wait()

            @pl.when(i == 0)
            def _():
                n_load.wait()

            @pl.when(i >= 2)
            def _():
                e_save(i - 2).wait()
            e_stg[slot] = dot_nn(d_in[slot], n_rows[...].reshape(mbs * mtok, dim))
            e_save(i).start()

        n_load = pltpu.make_async_copy(n_out, n_rows, out_sem.at[1])
        n_load.start()

        def table_start():
            for seq in (rounds * n_tiles - 2, rounds * n_tiles - 1):
                d_copy(seq).wait()
            d_load(0).start()

        @pl.when(s < last)
        def _():
            table_start()
        early = jnp.int32(0)
        for node, tiles in enumerate(EARLY_TILES):
            early = early + jnp.where(s == node, min(tiles, full), 0)
        loop(0, early, e_tile)

        def g_save(mb, count):
            at = pl.ds(mb, count)
            return pltpu.make_async_copy(g_in.at[at], g_out.at[at], out_sem.at[0])

        def gx_forward(c):
            gx_copy(c, 0, 0).wait_recv()
            each_role((3, last, 5), lambda node: gx_send_all(c, node))
            gx_save(c).start()

        def step(k):
            @pl.when(k >= HEAD_MBS)
            def _():
                @pl.when(k < mbs)
                def _():
                    g_final(k)
            b_mb = k - (last - s)

            @pl.when(b_mb == mbs - 1)
            def _():
                g_save(0, mbs - 1).start()

            @pl.when((b_mb >= 0) & (b_mb < mbs))
            def _():
                chunks_of(b_mb, bwd_chunk)

            @pl.when(k == 2)
            def _():
                g_mid(rounds - 1, (5,))

            @pl.when(k == 4)
            def _():
                g_mid(rounds - 1, (6,))

            x_mb = k - n_stage

            @pl.when((s == 3) & (x_mb >= 0) & (x_mb < gx_split // n_half))
            def _():
                chunks_of(x_mb, gx_forward)

        loop(0, mbs + last, step)
        g_save(mbs - 1, 1).start()

        @pl.when(s == last)
        def _():
            table_start()
        kept = jnp.where(s == last, LATE_TILES, 0)
        before = full - early - kept
        first_gx = jnp.where(s == 3, gx_split, 0)

        def late(j):
            c = first_gx + j - before

            @pl.when((j >= before) & (s > 0))
            def _():
                gx_forward(c)
            i = jnp.where(j < before, early + j, full - kept + c - gx_split)

            @pl.when((j < before) | ((c >= gx_split) & (i < full)))
            def _():
                e_tile(i)
            if rest:
                @pl.when(c == gx_split + kept)
                def _():
                    d_load(full, rest).wait()
                    e_save(full - 2).wait()
                    slot = full % 2
                    e_stg[slot, pl.ds(0, rest)] = dot_nn(d_in[slot, pl.ds(0, rest)], n_rows[...].reshape(mbs * mtok, dim))
                    e_save(full, rest).start()

            @pl.when(c == n_chunks - 3)
            def _():
                loss_out[...] = jnp.broadcast_to(jnp.sum(loss_acc[...], axis=1, keepdims=True), loss_out.shape)
                for c in (n_chunks - 2, n_chunks - 1):
                    dpre_copy(c).wait()
                pltpu.make_async_copy(g_in, g_out, out_sem.at[0]).wait()
                sent = stats.at[:, pl.ds(0, last)]
                remote(sent, sent, st_send.at[0], st_recv.at[0], lax.rem(s + 1, n_stage)).wait_send()

                @pl.when(s < last)
                def _():
                    remote(comb, buf_a, g_send.at[0], g_a.at[0], last).wait_send()

                @pl.when(s > 0)
                def _():
                    remote(g_buf, g_in, b_send.at[0], b_recv.at[0], 0).wait_send()

        loop(0, before + n_chunks - first_gx, late)
        if rest:
            e_save(full - 1).wait()
            e_save(full, rest).wait()
        else:
            e_save(full - 2).wait()
            e_save(full - 1).wait()
        pltpu.make_async_copy(gx, gx_out, gx_sem.at[0]).wait()
        for src, routes in gx_routes.items():
            @pl.when(s == src)
            def _(routes=routes):
                for lane, (dst, lo, hi) in enumerate(routes):
                    part = gx if hi - lo == n_chunks else gx.at[pl.ds(0, hi - lo), pl.ds(0, CHUNK)]
                    remote(part, part, gx_send.at[lane], gx_recv.at[0], dst).wait_send()

    pl.run_scoped(
        backward,
        pltpu.VMEM((mbs, mtok, dim), BF16), pltpu.VMEM((2, E_ROWS, mbs * mtok), BF16), pltpu.VMEM((2, E_ROWS, dim), F32),
    )


def pipeline_step(n_stage, labels, part, emb, w1, w2):
    mbs, mtok, dim = part.shape
    rows = emb.shape[0]
    ffn = w1.shape[1]
    chunks = mbs * mtok // CHUNK
    rounds = mbs // HEAD_MBS
    tokens = HEAD_MBS * mtok
    any_spec = pl.BlockSpec(memory_space=pl.ANY)
    vmem_spec = pl.BlockSpec(memory_space=pltpu.VMEM)
    act = pltpu.VMEM((mbs, mtok, dim), BF16)
    dma = pltpu.SemaphoreType.DMA
    act_shape = jax.ShapeDtypeStruct((mbs, mtok, dim), BF16)
    hid_shape = jax.ShapeDtypeStruct((chunks, CHUNK, ffn), BF16)
    return pl.pallas_call(
        functools.partial(step_kernel, n_stage),
        out_shape=(
            jax.ShapeDtypeStruct((chunks, CHUNK, ffn), F32), hid_shape, hid_shape,
            act_shape, act_shape, act_shape, act_shape,
            jax.ShapeDtypeStruct((rows, mbs * mtok), BF16),
            jax.ShapeDtypeStruct((rows, dim), F32),
            jax.ShapeDtypeStruct((8, 128), F32),
        ),
        in_specs=[vmem_spec] + [any_spec] * 4,
        out_specs=(any_spec,) * 9 + (vmem_spec,),
        scratch_shapes=[
            pltpu.VMEM((rows, dim), BF16), pltpu.VMEM((dim, ffn), BF16), pltpu.VMEM((ffn, dim), BF16),
            act, act, act, act, act, act,
            pltpu.VMEM((2, CHUNK, ffn), F32), pltpu.VMEM((2, CHUNK, ffn), BF16),
            pltpu.VMEM((2, vocab_tile(rows), tokens), BF16), pltpu.VMEM((rounds, n_stage, 8, tokens), F32), pltpu.VMEM((1, tokens), F32),
            dma((3,)), dma((1,)), dma((1,)), dma((chunks,)), dma((chunks,)), dma((chunks,)),
            dma((1,)), dma((chunks,)), dma((3,)), dma((chunks,)), dma((1,)), dma((rounds,)),
            dma((1,)), dma((mbs,)), dma((mbs,)), dma((1,)), dma((chunks,)), dma((4,)), dma((chunks,)),
            dma((2,)), dma((2,)), dma((2,)), dma((2,)), dma((2,)), dma((2,)), dma((1,)),
        ],
        compiler_params=pltpu.CompilerParams(collective_id=0, has_side_effects=True, vmem_limit_bytes=VMEM_LIMIT),
        name="pipeline_step",
    )(labels, part, emb, w1, w2)


WINDOW = 256
W_COLS = 1024
E_SLOTS = 4


def tail_kernel(
    rows, tok_ref, loss_ref, x_hbm, g_hbm, gx_hbm, dpre_hbm, hid_hbm, ge_hbm,
    loss_out, g1_out, g2_out, out_hbm,
    x_buf, g_buf, gx_buf, dp_buf, hid_buf, g1_stg, g2_stg, e_buf, packed, packed_id, bounds,
    act_sem, dp_sem, hid_sem, g1_sem, g2_sem, e_in_sem, e_out_sem,
):
    mbs, mtok = tok_ref.shape
    total, dim = g_buf.shape
    ffn = dpre_hbm.shape[1]
    n_blocks = ffn // W_COLS
    e_rows = e_buf.shape[1]
    n_e = rows // e_rows
    per_block = n_e // n_blocks

    def cols(j):
        return pl.ds(pl.multiple_of(j * W_COLS, W_COLS), W_COLS)

    def e_at(i):
        return pl.ds(pl.multiple_of(i * e_rows, 8), e_rows)

    def dp_load(j):
        slot = lax.rem(j, 2)
        return pltpu.make_async_copy(dpre_hbm.at[:, cols(j)], dp_buf.at[slot], dp_sem.at[slot])

    def hid_load(j):
        slot = lax.rem(j, 2)
        return pltpu.make_async_copy(hid_hbm.at[:, cols(j)], hid_buf.at[slot], hid_sem.at[slot])

    def e_load(i):
        slot = lax.rem(i, E_SLOTS)
        return pltpu.make_async_copy(ge_hbm.at[e_at(i)], e_buf.at[slot], e_in_sem.at[slot])

    def e_save(i):
        slot = lax.rem(i, E_SLOTS)
        return pltpu.make_async_copy(e_buf.at[slot], out_hbm.at[e_at(i)], e_out_sem.at[slot])

    def g1_save(j):
        return pltpu.make_async_copy(g1_stg, g1_out.at[0, :, cols(j)], g1_sem.at[0])

    def g2_save(j):
        return pltpu.make_async_copy(g2_stg, g2_out.at[0, cols(j)], g2_sem.at[0])

    x_load = pltpu.make_async_copy(x_hbm, x_buf, act_sem.at[0])
    g_load = pltpu.make_async_copy(g_hbm, g_buf, act_sem.at[1])
    gx_load = pltpu.make_async_copy(gx_hbm, gx_buf, act_sem.at[2])
    gx_load.start()
    loss_out[0] = loss_ref[0, 0] * (1.0 / total)

    s = lax.axis_index("stage")
    loc = tok_ref[...] - s * rows
    upper, lower = triangles(mbs, mtok)
    slot_of = jnp.full((mbs, mtok), -1.0, F32)
    count = jnp.int32(0)
    bounds[0] = count
    for i in range(n_e):
        inside = (loc >= i * e_rows) & (loc < (i + 1) * e_rows)
        rank, number = ranks(inside.astype(F32), upper, lower)
        slot_of = jnp.where(inside, rank + count.astype(F32), slot_of)
        count = count + number
        bounds[i + 1] = count
    slot_of = slot_of.astype(jnp.int32)
    n_packs = jnp.maximum((count + WINDOW - 1) // WINDOW, 1)

    def pack(b):
        slot = lax.broadcasted_iota(jnp.int32, (WINDOW, mtok), 0) + b * WINDOW
        ids = jnp.zeros((WINDOW, 1), F32)
        picks = []
        for mb in range(mbs):
            pick = slot == slot_of[mb:mb + 1, :]
            picks.append(pick.astype(BF16))
            ids = ids + jnp.sum(jnp.where(pick, loc[mb:mb + 1, :].astype(F32), 0.0), axis=1, keepdims=True)
        at = pl.ds(pl.multiple_of(b * WINDOW, WINDOW), WINDOW)
        packed[at, :] = dot_nn(jnp.concatenate(picks, axis=1), gx_buf[...]).astype(BF16)
        filled = lax.broadcasted_iota(jnp.int32, (WINDOW, 1), 0) + b * WINDOW < count
        packed_id[at, :] = jnp.broadcast_to(jnp.where(filled, ids.astype(jnp.int32), -1), (WINDOW, 128))

    def loop(lo, hi, fn):
        def body(i, _):
            fn(i)
            return 0
        lax.fori_loop(lo, hi, body, 0)

    def e_tile(i):
        slot = lax.rem(i, E_SLOTS)
        first = jnp.minimum((bounds[i] // 16) * 16, (n_packs - 1) * WINDOW)
        lane = lax.broadcasted_iota(jnp.int32, (WINDOW, e_rows), 1) + i * e_rows

        def window(k):
            start = pl.multiple_of(jnp.minimum(first + k * WINDOW, (n_packs - 1) * WINDOW), 16)
            at = pl.ds(start, WINDOW)
            fresh = lax.broadcasted_iota(jnp.int32, (WINDOW, 1), 0) + start >= first + k * WINDOW
            ids = jnp.where(fresh, packed_id[at, :][:, 0:1], -1)
            return dot_tn((lane == ids).astype(BF16), packed[at, :])

        e_load(i).wait()
        e_buf[slot] = e_buf[slot] + window(0)

        def more(k):
            e_buf[slot] = e_buf[slot] + window(k)

        loop(1, (bounds[i + 1] - first + WINDOW - 1) // WINDOW, more)
        e_save(i).start()

    def block(j):
        slot = lax.rem(j, 2)

        @pl.when(j == 0)
        def _():
            x_load.wait()

        @pl.when(j > 0)
        def _():
            g1_save(j - 1).wait()
        dp_load(j).wait()

        @pl.when(j == 0)
        def _():
            for cp in (e_load(0), e_load(1), g_load, hid_load(0)):
                cp.start()
        g1_stg[...] = dot_tn(x_buf[...], dp_buf[slot])
        g1_save(j).start()

        @pl.when(j + 1 < n_blocks)
        def _():
            dp_load(j + 1).start()

        def tile(i):
            @pl.when(i + 2 < n_e)
            def _():
                @pl.when(i + 2 >= E_SLOTS)
                def _():
                    e_save(i + 2 - E_SLOTS).wait()
                e_load(i + 2).start()
            e_tile(i)

        loop(j * per_block, (j + 1) * per_block, tile)

        @pl.when(j == 0)
        def _():
            g_load.wait()

        @pl.when(j > 0)
        def _():
            g2_save(j - 1).wait()
        hid_load(j).wait()

        @pl.when(j + 1 < n_blocks)
        def _():
            hid_load(j + 1).start()
        g2_stg[...] = dot_tn(hid_buf[slot], g_buf[...])
        g2_save(j).start()

    x_load.start()
    dp_load(0).start()
    gx_load.wait()
    loop(0, n_packs, pack)
    loop(0, n_blocks, block)
    g1_save(n_blocks - 1).wait()
    g2_save(n_blocks - 1).wait()
    for i in range(max(n_e - E_SLOTS, 0), n_e):
        e_save(i).wait()


def tail(tok, loss, x, g, gx, dpre, hid, ge):
    rows, dim = ge.shape
    total, ffn = dpre.shape
    n_blocks = ffn // W_COLS
    e_rows = rows // (2 * n_blocks)
    n_e = rows // e_rows
    any_spec = pl.BlockSpec(memory_space=pl.ANY)
    vmem_spec = pl.BlockSpec(memory_space=pltpu.VMEM)
    dma = pltpu.SemaphoreType.DMA
    act = pltpu.VMEM((total, dim), BF16)
    return pl.pallas_call(
        functools.partial(tail_kernel, rows),
        out_shape=(
            jax.ShapeDtypeStruct((1,), F32),
            jax.ShapeDtypeStruct((1, dim, ffn), F32),
            jax.ShapeDtypeStruct((1, ffn, dim), F32),
            jax.ShapeDtypeStruct((rows, dim), F32),
        ),
        in_specs=[vmem_spec, vmem_spec] + [any_spec] * 6,
        out_specs=(pl.BlockSpec(memory_space=pltpu.SMEM), any_spec, any_spec, any_spec),
        scratch_shapes=[
            act, act, act, pltpu.VMEM((2, total, W_COLS), BF16), pltpu.VMEM((2, total, W_COLS), BF16),
            pltpu.VMEM((dim, W_COLS), F32), pltpu.VMEM((W_COLS, dim), F32), pltpu.VMEM((E_SLOTS, e_rows, dim), F32),
            pltpu.VMEM((total, dim), BF16), pltpu.VMEM((total, 128), jnp.int32), pltpu.SMEM((n_e + 1,), jnp.int32),
            dma((3,)), dma((2,)), dma((2,)), dma((1,)), dma((1,)), dma((E_SLOTS,)), dma((E_SLOTS,)),
        ],
        compiler_params=pltpu.CompilerParams(vmem_limit_bytes=VMEM_LIMIT),
        name="tail",
    )(tok, loss, x, g, gx, dpre, hid, ge)


def solution(mesh):
    n_stage = mesh.shape["stage"]

    def stage_body(token_ids, label_ids, emb_rows, w_in, w_out):
        tokens = token_ids.shape[0] * token_ids.shape[1]
        part = lookup(token_ids, emb_rows)
        _, hid, dpre, x_in, _, g_all, gx, _, ge, loss = pipeline_step(n_stage, label_ids, part, emb_rows, w_in[0], w_out[0])
        flat = lambda a: a.reshape(tokens, a.shape[-1])
        mean_loss, grad_in, grad_out, grad_emb = tail(token_ids, loss, flat(x_in), flat(g_all), flat(gx), flat(dpre), flat(hid), ge)
        return mean_loss, grad_in, grad_out, grad_emb

    return jax.shard_map(
        stage_body,
        mesh=mesh,
        in_specs=(P("dp", None), P("dp", None), P("stage", None), P("stage", None, None), P("stage", None, None)),
        out_specs=(P("dp"), P(("dp", "stage"), None, None), P(("dp", "stage"), None, None), P(("dp", "stage"), None)),
        check_vma=False,
    )
```

```python
import functools
import math

import jax
import jax.numpy as jnp
from jax import lax
from jax.experimental import pallas as pl
from jax.experimental.pallas import tpu as pltpu
from jax.sharding import PartitionSpec as P

NORM_EPS = 1e-6
MESH = pl.DeviceIdType.MESH
F32 = jnp.float32
BF16 = jnp.bfloat16
GELU_A = math.sqrt(2.0 / math.pi)
GELU_B = 0.044715
LOG2E = math.log2(math.e)
CHUNK = 128
HEAD_MBS = 2
VMEM_LIMIT = 67_000_000


def dot_nn(a, b):
    return lax.dot_general(a, b, (((1,), (0,)), ((), ())), preferred_element_type=F32)


def dot_nt(a, b):
    return lax.dot_general(a, b, (((1,), (1,)), ((), ())), preferred_element_type=F32)


def dot_tn(a, b):
    return lax.dot_general(a, b, (((0,), (0,)), ((), ())), preferred_element_type=F32)


def gelu_and_slope(pre):
    sq = pre * pre
    th = jnp.tanh(pre * (GELU_A + (GELU_A * GELU_B) * sq))
    half_sum = 0.5 + 0.5 * th
    hid = pre * half_sum
    slope = half_sum + (hid - hid * th) * (GELU_A + (3.0 * GELU_A * GELU_B) * sq)
    return hid, slope


def norm_scale(x_f32):
    return lax.rsqrt(jnp.mean(x_f32 * x_f32, axis=-1, keepdims=True) + NORM_EPS)


def remote(src, dst, send_sem, recv_sem, stage):
    return pltpu.make_async_remote_copy(
        src_ref=src, dst_ref=dst, send_sem=send_sem, recv_sem=recv_sem, device_id={"stage": stage}, device_id_type=MESH
    )


def group_barrier(stage, n_stage):
    barrier = pltpu.get_barrier_semaphore()
    for off in range(1, n_stage):
        pl.semaphore_signal(barrier, inc=1, device_id={"stage": lax.rem(stage + off, n_stage)}, device_id_type=MESH)
    pl.semaphore_wait(barrier, n_stage - 1)


def vocab_tile(rows):
    for parts in range(2, rows + 1):
        if rows % parts == 0 and (rows // parts) % 16 == 0 and rows // parts <= 2400:
            return rows // parts
    return rows


def sub_blocks(rows, size):
    return [(start, min(size, rows - start)) for start in range(0, rows, size)]


def forward_chunk(x, w1, w2, slope_slot, hid_slot):
    ffn = w1.shape[1]
    width = ffn // 4
    for part in range(4):
        cols = pl.ds(part * width, width)
        hid, slope = gelu_and_slope(dot_nn(x, w1[:, cols]))
        slope_slot[:, cols] = slope
        hid_slot[:, cols] = hid.astype(BF16)
    return x.astype(F32) + dot_nn(hid_slot[...], w2[...])


def forward_pair(x, w1, w2, slope_slots, hid_slots):
    ffn = w1.shape[1]
    width = ffn // 4
    for part in range(4):
        cols = pl.ds(part * width, width)
        hid, slope = gelu_and_slope(dot_nn(x, w1[:, cols]))
        for slot in range(2):
            slope_slots[slot, :, cols] = slope[slot * CHUNK:(slot + 1) * CHUNK]
            hid_slots[slot, :, cols] = hid[slot * CHUNK:(slot + 1) * CHUNK].astype(BF16)
    return x.astype(F32) + dot_nn(hid_slots[...].reshape(2 * CHUNK, ffn), w2[...])


def backward_chunk(grad, w2_t, w1_t, slope_slot, dpre_slot):
    ffn = slope_slot.shape[1]
    dim = grad.shape[1]
    for part in range(ffn // dim):
        cols = pl.ds(part * dim, dim)
        dpre_slot[:, cols] = (dot_nn(grad, w2_t[:, cols]) * slope_slot[:, cols]).astype(BF16)
    return grad.astype(F32) + dot_nn(dpre_slot[...], w1_t[...])


def swap_transposed(w1, w2):
    dim, ffn = w1.shape
    side = 256

    def strip(part, _):
        at = pl.ds(pl.multiple_of(part * side, side), side)
        for i in range(dim // side):
            rows = pl.ds(i * side, side)
            from_w1 = w1[rows, at].T
            from_w2 = w2[at, rows].T
            w2[at, rows] = from_w1
            w1[rows, at] = from_w2
        return 0

    lax.fori_loop(0, ffn // side, strip, 0)


def head_logits(n_t, emb, logits, lab_row, tokens):
    rows = emb.shape[0]
    tile = vocab_tile(rows)
    c2 = LOG2E * emb.shape[1] ** -0.5

    def tile_step(idx, carry):
        mx, sm, lb = carry
        base = pl.multiple_of(idx * tile, 16)
        for start, size in sub_blocks(tile, 256):
            at = pl.ds(base + start, size)
            block = dot_nn(emb[at, :], n_t[...])
            logits[at, :] = block
            b3 = block.reshape(size // 8, 8, tokens)
            row_ids = lax.broadcasted_iota(jnp.int32, (size, tokens), 0) + (base + start)
            hit = jnp.where(row_ids == lab_row, block, 0.0).reshape(size // 8, 8, tokens)
            mx_new = jnp.maximum(mx, jnp.max(b3, axis=0))
            sm = sm * jnp.exp2((mx - mx_new) * c2) + jnp.sum(jnp.exp2((b3 - mx_new[None]) * c2), axis=0)
            lb = lb + jnp.sum(hit, axis=0)
            mx = mx_new
        return mx, sm, lb

    init = (jnp.full((8, tokens), -3.0e38, F32), jnp.zeros((8, tokens), F32), jnp.zeros((8, tokens), F32))
    mx, sm, lb = lax.fori_loop(0, rows // tile, tile_step, init)
    top = jnp.max(mx, axis=0, keepdims=True)
    tot = jnp.sum(sm * jnp.exp2((mx - top) * c2), axis=0, keepdims=True)
    lab = jnp.sum(lb, axis=0, keepdims=True)
    return top, tot, lab


def head_grad_tile(base, size_all, emb, logits, d_slot, lab_row, shift, tokens):
    scale = emb.shape[1] ** -0.5
    c2 = LOG2E * scale
    total = None
    for start, size in sub_blocks(size_all, 256):
        at = pl.ds(base + start, size)
        row_ids = lax.broadcasted_iota(jnp.int32, (size, tokens), 0) + (base + start)
        prob = jnp.exp2(logits[at, :] * c2 - shift)
        d_log = (prob - jnp.where(row_ids == lab_row, scale, 0.0)).astype(BF16)
        d_slot[pl.ds(start, size), :] = d_log
        part = dot_tn(d_log, emb[at, :])
        total = part if total is None else total + part
    return total


LOOK = 192
LOOK_BASE = 512


def look_at(row):
    return pl.ds(pl.multiple_of(row, 16), LOOK)


def ranks(flag, upper, lower):
    within = dot_nn(flag.astype(BF16), upper)
    total = jnp.sum(flag, axis=1, keepdims=True)
    rows = flag.shape[0]
    before = jnp.sum(jnp.where(lower, jnp.transpose(jnp.broadcast_to(total, (rows, rows))), 0.0), axis=1, keepdims=True)
    return within - flag + before, jnp.sum(flag).astype(jnp.int32)


def triangles(mbs, mtok):
    upper = (lax.broadcasted_iota(jnp.int32, (mtok, mtok), 0)
             <= lax.broadcasted_iota(jnp.int32, (mtok, mtok), 1)).astype(BF16)
    lower = lax.broadcasted_iota(jnp.int32, (mbs, mbs), 1) < lax.broadcasted_iota(jnp.int32, (mbs, mbs), 0)
    return upper, lower


def lookup_kernel(tok_ref, emb_hbm, part_hbm, emb, part, rank_ref, picks, found, emb_sem, part_sem):
    mbs, mtok = tok_ref.shape
    rows, dim = emb.shape
    tile = vocab_tile(rows)
    n_tiles = rows // tile
    loads = [pltpu.make_async_copy(emb_hbm.at[pl.ds(i * tile, tile)], emb.at[pl.ds(i * tile, tile)], emb_sem.at[i])
             for i in range(n_tiles)]
    for ld in loads:
        ld.start()

    picks[:, pl.ds(0, LOOK_BASE + LOOK), :] = jnp.zeros((mbs, LOOK_BASE + LOOK, mtok), BF16)
    found[pl.ds(0, LOOK_BASE + LOOK), :] = jnp.zeros((LOOK_BASE + LOOK, dim), BF16)
    loc = tok_ref[...] - lax.axis_index("stage") * rows
    upper, lower = triangles(mbs, mtok)
    counts = []
    for i in range(n_tiles):
        inside = (loc >= i * tile) & (loc < (i + 1) * tile)
        rank, number = ranks(inside.astype(F32), upper, lower)
        rank_ref[i] = jnp.where(inside, rank, -1.0).astype(jnp.int32)
        counts.append(number)

    def window(i, k, row):
        slot = lax.broadcasted_iota(jnp.int32, (LOOK, mtok), 0) + k * LOOK
        ids = jnp.zeros((LOOK, 1), F32)
        for mb in range(mbs):
            pick = slot == rank_ref[i, mb:mb + 1, :]
            picks[mb, look_at(row), :] = pick.astype(BF16)
            ids = ids + jnp.sum(jnp.where(pick, loc[mb:mb + 1, :].astype(F32), 0.0), axis=1, keepdims=True)
        filled = lax.broadcasted_iota(jnp.int32, (LOOK, 1), 0) + k * LOOK < counts[i]
        return jnp.where(filled, ids.astype(jnp.int32), -1)

    def find(i, row, ids):
        lane = lax.broadcasted_iota(jnp.int32, (LOOK, tile), 1) + i * tile
        rows_found = dot_nn((lane == ids).astype(BF16), emb[pl.ds(i * tile, tile), :])
        found[look_at(row), :] = rows_found.astype(BF16)

    starts = [jnp.int32(0)]
    for number in counts:
        starts.append(starts[-1] + (jnp.minimum(number, LOOK) + 15) // 16 * 16)
    first_ids = [window(i, 0, starts[i]) for i in range(n_tiles)]
    for i in range(n_tiles):
        loads[i].wait()
        find(i, starts[i], first_ids[i])

    extra_end = jnp.int32(1)
    for i in range(n_tiles):
        def extra(k, w, i=i):
            row = LOOK_BASE + w * LOOK
            find(i, row, window(i, k, row))
            return w + 1
        extra_end = lax.fori_loop(1, (counts[i] + LOOK - 1) // LOOK, extra, extra_end)
    crowded = (extra_end > 1) | (starts[n_tiles] > LOOK_BASE)

    def save(mb):
        return pltpu.make_async_copy(part.at[mb], part_hbm.at[mb], part_sem.at[mb])

    for mb in range(mbs):
        part[mb] = dot_tn(picks[mb, 0:LOOK_BASE, :], found[0:LOOK_BASE, :]).astype(BF16)

        @pl.when(jnp.logical_not(crowded))
        def _(mb=mb):
            save(mb).start()

    @pl.when(crowded)
    def _():
        def add_mb(mb, _):
            def add(w, _):
                at = look_at(LOOK_BASE + w * LOOK)
                part[mb] = part[mb] + dot_tn(picks[mb, at, :], found[at, :]).astype(BF16)
                return 0
            lax.fori_loop(0, extra_end, add, 0)
            save(mb).start()
            return 0
        lax.fori_loop(0, mbs, add_mb, 0)

    for mb in range(mbs):
        save(mb).wait()


def lookup(tok, emb):
    mbs, mtok = tok.shape
    rows, dim = emb.shape
    n_tiles = rows // vocab_tile(rows)
    slots = LOOK_BASE + (1 + mbs * mtok // LOOK) * LOOK
    any_spec = pl.BlockSpec(memory_space=pl.ANY)
    dma = pltpu.SemaphoreType.DMA
    return pl.pallas_call(
        lookup_kernel,
        out_shape=jax.ShapeDtypeStruct((mbs, mtok, dim), BF16),
        in_specs=[pl.BlockSpec(memory_space=pltpu.VMEM), any_spec],
        out_specs=any_spec,
        scratch_shapes=[
            pltpu.VMEM((rows, dim), BF16), pltpu.VMEM((mbs, mtok, dim), BF16), pltpu.VMEM((n_tiles, mbs, mtok), jnp.int32),
            pltpu.VMEM((mbs, slots, mtok), BF16), pltpu.VMEM((slots, dim), BF16),
            dma((n_tiles,)), dma((mbs,)),
        ],
        compiler_params=pltpu.CompilerParams(vmem_limit_bytes=VMEM_LIMIT),
        name="lookup",
    )(tok, emb)


E_ROWS = 512
LATE_TILES = 3
EARLY_TILES = (11, 9, 8, 6, 4, 3, 0, 0)
LOOKUP_LEAD = 8
LOOKUP_PARENT = {2: (3, 0), 1: (0, 0), 4: (5, 0), 6: (7, 0), 5: (3, 1), 7: (0, 1), 3: (0, 2)}
GRAD_PARENT = {0: (1, 0), 2: (3, 0), 4: (5, 0), 1: (6, 0), 6: (7, 0), 3: (5, 1), 5: (7, 1)}


def step_kernel(
    n_stage, lab_ref, part_hbm, emb_hbm, w1_hbm, w2_hbm,
    slope_out, hid_out, dpre_out, xin_out, n_out, g_out, gx_out, dt_out, ge_out, loss_out,
    emb, w1, w2, x_in, x_out, n_all, comb, buf_a, buf_b, slope_stg, act_stg, d_stg, stats, loss_acc,
    load_sem, part_sem, lk_send, lk_a, lk_b, lk_c, x_send, x_recv, n_send, n_recv, st_send, st_recv,
    g_send, g_a, g_b, b_send, b_recv, gx_send, gx_recv, slope_sem, act_sem, dt_sem, d_sem, e_sem, out_sem, gx_sem,
):
    s = lax.axis_index("stage")
    last = n_stage - 1
    mbs, mtok, dim = x_in.shape
    n_half = mtok // CHUNK
    n_chunks = mbs * n_half
    rows = emb.shape[0]
    ffn = w1.shape[1]
    tile = vocab_tile(rows)
    tokens = HEAD_MBS * mtok
    rounds = mbs // HEAD_MBS
    scale = dim ** -0.5
    c2 = LOG2E * scale
    row_start = s * rows
    bufs = (buf_a, buf_b, x_in)
    lk_sems = (lk_a, lk_b, lk_c)

    loads = [pltpu.make_async_copy(src, dst, load_sem.at[i])
             for i, (src, dst) in enumerate([(w1_hbm, w1), (w2_hbm, w2), (emb_hbm, emb)])]
    part_load = pltpu.make_async_copy(part_hbm, comb, part_sem.at[0])
    part_load.start()
    group_barrier(s, n_stage)

    def pos(c):
        return (c // n_half, pl.ds(pl.multiple_of(lax.rem(c, n_half) * CHUNK, CHUNK), CHUNK))

    def at_chunk(ref, c):
        return ref.at[c // n_half, pl.ds(pl.multiple_of(lax.rem(c, n_half) * CHUNK, CHUNK), CHUNK)]

    def loop(lo, hi, fn):
        def body(i, _):
            fn(i)
            return 0
        lax.fori_loop(lo, hi, body, 0)

    def chunks_of(mb, fn):
        loop(mb * n_half, (mb + 1) * n_half, fn)

    def each_role(roles, fn):
        for node in roles:
            @pl.when(s == node)
            def _(node=node):
                fn(node)

    def lk_copy(c, child):
        parent, slot = LOOKUP_PARENT[child]
        return remote(at_chunk(comb, c), at_chunk(bufs[slot], c), lk_send.at[0], lk_sems[slot].at[c], parent)

    def lk_total(c, slots):
        total = comb[pos(c)].astype(F32)
        for slot in range(slots):
            remote(at_chunk(comb, c), at_chunk(bufs[slot], c), lk_send.at[0], lk_sems[slot].at[c], 0).wait_recv()
            total = total + bufs[slot][pos(c)].astype(F32)
        return total.astype(BF16)

    def lk_forward(c, node, slots):
        comb[pos(c)] = lk_total(c, slots)
        lk_copy(c, node).start()

    part_load.wait()
    each_role((1, 2, 4, 6), lambda node: loop(0, n_chunks, lambda c: lk_copy(c, node).start()))
    for ld in loads:
        ld.start()
    each_role((5, 7), lambda node: loop(0, n_chunks, lambda c: lk_forward(c, node, 1)))
    each_role((3,), lambda node: loop(0, LOOKUP_LEAD, lambda c: lk_forward(c, node, 2)))
    loads[0].wait()
    loads[1].wait()

    n_routes = {last: (5, 1, 6), 5: (4,), 1: (3, 0), 3: (2,)}

    def x_copy(c, dst_stage):
        return remote(at_chunk(x_out, c), at_chunk(x_in, c), x_send.at[0], x_recv.at[c], dst_stage)

    def n_copy(c, lane, dst_stage):
        return remote(at_chunk(n_all, c), at_chunk(n_all, c), n_send.at[lane], n_recv.at[c], dst_stage)

    def fwd_copies(c):
        slot = lax.rem(c, 2)
        return (pltpu.make_async_copy(slope_stg.at[slot], slope_out.at[c], slope_sem.at[slot]),
                pltpu.make_async_copy(act_stg.at[slot], hid_out.at[c], act_sem.at[slot]))

    def slope_copy(c):
        slot = lax.rem(c, 2)
        return pltpu.make_async_copy(slope_out.at[c], slope_stg.at[slot], slope_sem.at[slot])

    def fwd_chunk(c):
        idx = pos(c)

        @pl.when((s == 3) & (c + LOOKUP_LEAD < n_chunks))
        def _():
            lk_forward(c + LOOKUP_LEAD, 3, 2)

        @pl.when(s == 0)
        def _():
            x_in[idx] = lk_total(c, 3)

        @pl.when(s > 0)
        def _():
            x_copy(c, 0).wait_recv()

        @pl.when(c >= 2)
        def _():
            for cp in fwd_copies(c - 2):
                cp.wait()

        slot = lax.rem(c, 2)
        out = forward_chunk(x_in[idx], w1, w2, slope_stg.at[slot], act_stg.at[slot]).astype(BF16)
        x_out[idx] = out
        for cp in fwd_copies(c):
            cp.start()

        @pl.when(s < last)
        def _():
            x_copy(c, s + 1).start()

        @pl.when(s == last)
        def _():
            out_f = out.astype(F32)
            n_all[idx] = (out_f * norm_scale(out_f)).astype(BF16)
            for lane, dst in enumerate(n_routes[last]):
                n_copy(c, lane, dst).start()

    def last_fwd_pair(mb):
        first = mb * n_half
        for c in (first, first + 1):
            x_copy(c, 0).wait_recv()
            for cp in fwd_copies(c - 2):
                cp.wait()
        out = forward_pair(x_in[mb], w1, w2, slope_stg, act_stg).astype(BF16)
        x_out[mb] = out
        out_f = out.astype(F32)
        n_all[mb] = (out_f * norm_scale(out_f)).astype(BF16)
        for c in (first, first + 1):
            for cp in fwd_copies(c):
                cp.start()
            for lane, dst in enumerate(n_routes[last]):
                n_copy(c, lane, dst).start()

    def n_round(r, fn):
        loop(r * HEAD_MBS * n_half, (r + 1) * HEAD_MBS * n_half, fn)

    def n_early(r):
        def take(c, node):
            n_copy(c, 0, 0 if node == last else last).wait_recv()
            for lane, dst in enumerate(n_routes[node]):
                n_copy(c, lane, dst).start()
        each_role((1, 5), lambda node: n_round(r, lambda c: take(c, node)))

    def n_mid(r):
        def take(c, node):
            n_copy(c, 0, last).wait_recv()
            n_copy(c, 0, n_routes[node][0]).start()
        each_role((3,), lambda node: n_round(r, lambda c: take(c, node)))

    def n_late(r):
        @pl.when((lax.rem(s, 2) == 0))
        def _():
            n_round(r, lambda c: n_copy(c, 0, last).wait_recv())

    def g_copy(mb, child):
        parent, slot = GRAD_PARENT[child]
        return remote(comb.at[mb], bufs[slot].at[mb], g_send.at[0], (g_a, g_b)[slot].at[mb], parent)

    def g_total(mb, slots):
        total = comb[mb].astype(F32)
        for slot in range(slots):
            remote(comb.at[mb], bufs[slot].at[mb], g_send.at[0], (g_a, g_b)[slot].at[mb], 0).wait_recv()
            total = total + bufs[slot][mb].astype(F32)
        return total

    def g_forward(mb, node, slots):
        comb[mb] = g_total(mb, slots).astype(BF16)
        g_copy(mb, node).start()

    def g_low(r):
        each_role((1, 3), lambda node: loop(r * HEAD_MBS, (r + 1) * HEAD_MBS, lambda mb: g_forward(mb, node, 1)))

    def g_mid(r, nodes=(5, 6)):
        each_role(nodes, lambda node: loop(r * HEAD_MBS, (r + 1) * HEAD_MBS, lambda mb: g_forward(mb, node, {5: 2, 6: 1}[node])))

    def g_final(mb):
        @pl.when(s == last)
        def _():
            grad_n = g_total(mb, 2)
            x_f = x_out[mb].astype(F32)
            inv = norm_scale(x_f)
            n_f = x_f * inv
            dx = inv * (grad_n - n_f * jnp.mean(grad_n * n_f, axis=-1, keepdims=True))
            comb[mb] = dx.astype(BF16)

    def lab_row_of(r):
        parts = [lab_ref[pl.ds(r * HEAD_MBS + i, 1), :] for i in range(HEAD_MBS)]
        return jnp.concatenate(parts, axis=1) - row_start

    def st_copy(r, off):
        dst = lax.rem(s + off, n_stage)
        return remote(stats.at[r, s], stats.at[r, s], st_send.at[0], st_recv.at[r], dst)

    saves = [pltpu.make_async_copy(x_in, xin_out, out_sem.at[0]), pltpu.make_async_copy(n_all, n_out, out_sem.at[1])]

    n_tiles = rows // tile

    def d_copy(seq):
        slot = lax.rem(seq, 2)
        r = seq // n_tiles
        idx = lax.rem(seq, n_tiles)
        dst = dt_out.at[pl.ds(pl.multiple_of(idx * tile, 16), tile), pl.ds(pl.multiple_of(r * tokens, tokens), tokens)]
        return pltpu.make_async_copy(d_stg.at[slot], dst, dt_sem.at[slot])

    def forward_and_head(logits, n_t, gn_acc):
        def head_a(r):
            n_late(r)

            @pl.when(r == rounds - 1)
            def _():
                for cp in saves:
                    cp.start()

            n_t[...] = n_all[pl.ds(r * HEAD_MBS, HEAD_MBS)].reshape(tokens, dim).T
            top, tot, lab = head_logits(n_t, emb, logits, lab_row_of(r), tokens)

            @pl.when(r == rounds - 1)
            def _():
                for cp in saves:
                    cp.wait()

                for src, dsts in n_routes.items():
                    @pl.when(s == src)
                    def _(dsts=dsts):
                        for lane, dst in enumerate(dsts):
                            remote(n_all, n_all, n_send.at[lane], n_recv.at[0], dst).wait_send()
            stats[r, s] = jnp.concatenate([top, tot, lab, jnp.zeros((5, tokens), F32)], axis=0)
            for off in range(1, n_stage):
                st_copy(r, off).start()

        def head_b(r):
            @pl.when(r + 1 < rounds)
            def _():
                n_early(r + 1)

            @pl.when((r == rounds - 2) & (s < last))
            def _():
                remote(x_out, x_in, x_send.at[0], x_recv.at[0], 0).wait_send()

            @pl.when(r == rounds - 1)
            def _():
                for c in (n_chunks - 2, n_chunks - 1):
                    for cp in fwd_copies(c):
                        cp.wait()
                slope_copy(0).start()
                slope_copy(1).start()

            @pl.when(r == jnp.where(s == last, rounds - 1, rounds - 2))
            def _():
                swap_transposed(w1, w2)
            others = stats.at[r, pl.ds(0, last)]
            remote(others, others, st_send.at[0], st_recv.at[r], lax.rem(s + 1, n_stage)).wait_recv()
            blocks = [stats[r, i] for i in range(n_stage)]
            top = blocks[0][0:1]
            for blk in blocks[1:]:
                top = jnp.maximum(top, blk[0:1])
            tot = jnp.zeros_like(top)
            lab = jnp.zeros_like(top)
            for blk in blocks:
                tot = tot + blk[1:2] * jnp.exp2((blk[0:1] - top) * c2)
                lab = lab + blk[2:3]
            loss_acc[...] = loss_acc[...] + (jnp.log(tot) + (top - lab) * scale)
            shift = top * c2 + (jnp.log(tot) * LOG2E - math.log2(scale))
            lab_row = lab_row_of(r)

            def tile_step(idx):
                seq = r * n_tiles + idx

                @pl.when(seq >= 2)
                def _():
                    d_copy(seq - 2).wait()
                @pl.when((idx == n_tiles - 1) & (r + 1 < rounds))
                def _():
                    n_mid(r + 1)
                base = pl.multiple_of(idx * tile, 16)
                part = head_grad_tile(base, tile, emb, logits, d_stg.at[lax.rem(seq, 2)], lab_row, shift, tokens)
                gn_acc[...] = gn_acc[...] + part
                d_copy(seq).start()

            gn_acc[...] = jnp.zeros_like(gn_acc)
            loop(0, n_tiles, tile_step)
            comb[pl.ds(r * HEAD_MBS, HEAD_MBS)] = gn_acc[...].reshape(HEAD_MBS, mtok, dim).astype(BF16)
            each_role((0, 2, 4), lambda node: loop(r * HEAD_MBS, (r + 1) * HEAD_MBS, lambda mb: g_copy(mb, node).start()))
        loss_acc[...] = jnp.zeros_like(loss_acc)
        first_a = HEAD_MBS + 1 + last

        def step(k):
            f_mb = k - s

            paired = (s == last) & (f_mb >= 2 * HEAD_MBS)

            @pl.when((f_mb >= 0) & (f_mb < mbs) & jnp.logical_not(paired))
            def _():
                chunks_of(f_mb, fwd_chunk)

            @pl.when((f_mb < mbs) & paired)
            def _():
                last_fwd_pair(f_mb)

            @pl.when(k == first_a)
            def _():
                loads[2].wait()

                @pl.when(s > 0)
                def _():
                    remote(comb, buf_a, lk_send.at[0], lk_a.at[0], 0).wait_send()

            rel = k - first_a
            r = rel // HEAD_MBS
            even = lax.rem(rel + HEAD_MBS * n_stage, HEAD_MBS) == 0

            @pl.when(k == first_a)
            def _():
                n_early(0)
                n_mid(0)

            @pl.when(even & (rel >= 0))
            def _():
                head_a(r)

            @pl.when(even & (rel >= HEAD_MBS))
            def _():
                g_low(r - 1)

                @pl.when(r == 2)
                def _():
                    loop(0, HEAD_MBS, g_final)

            @pl.when(jnp.logical_not(even) & (rel >= 0))
            def _():
                head_b(r)

            @pl.when(jnp.logical_not(even) & (rel >= HEAD_MBS))
            def _():
                g_mid(r - 1)

        loop(0, first_a + HEAD_MBS * rounds, step)
        g_low(rounds - 1)

    pl.run_scoped(
        forward_and_head,
        pltpu.VMEM((rows, tokens), F32), pltpu.VMEM((dim, tokens), BF16), pltpu.VMEM((tokens, dim), F32),
    )

    g_in, g_buf, gx = x_in, x_out, n_all

    def b_copy(c, dst):
        return remote(at_chunk(g_buf, c), at_chunk(g_in, c), b_send.at[0], b_recv.at[c], dst)

    def gx_copy(c, lane, dst):
        return remote(at_chunk(gx, c), at_chunk(gx, c), gx_send.at[lane], gx_recv.at[c], dst)

    def dpre_copy(c):
        slot = lax.rem(c, 2)
        return pltpu.make_async_copy(act_stg.at[slot], dpre_out.at[c], act_sem.at[slot])

    gx_split = n_chunks // 2
    gx_routes = {0: ((5, n_chunks - 1, n_chunks), (3, 0, n_chunks), (last, 0, n_chunks), (1, 0, n_chunks)), 3: ((2, 0, n_chunks), (5, 0, gx_split)),
                 last: ((6, 0, n_chunks), (5, gx_split, n_chunks - 1)), 5: ((4, 0, n_chunks),)}

    def gx_send_all(c, node):
        for lane, (dst, lo, hi) in enumerate(gx_routes[node]):
            @pl.when((c >= lo) & (c < hi))
            def _(lane=lane, dst=dst):
                gx_copy(c, lane, dst).start()


    def gx_save(c):
        return pltpu.make_async_copy(at_chunk(gx, c), at_chunk(gx_out, c), gx_sem.at[0])

    def bwd_chunk(c):
        slot = lax.rem(c, 2)
        idx = pos(c)

        @pl.when(s < last)
        def _():
            b_copy(c, 0).wait_recv()

        @pl.when(s == last)
        def _():
            g_in[idx] = comb[idx]

        @pl.when(c >= 2)
        def _():
            dpre_copy(c - 2).wait()
        slope_copy(c).wait()
        dx = backward_chunk(g_in[idx], w1, w2, slope_stg.at[slot], act_stg.at[slot]).astype(BF16)

        @pl.when(s > 0)
        def _():
            g_buf[idx] = dx
            b_copy(c, s - 1).start()

        @pl.when(s == 0)
        def _():
            gx[idx] = dx
            gx_send_all(c, 0)
            gx_save(c).start()
        dpre_copy(c).start()

        @pl.when(c + 2 < n_chunks)
        def _():
            slope_copy(c + 2).start()

    full = rows // E_ROWS
    rest = rows - full * E_ROWS

    def backward(n_rows, d_in, e_stg):
        def d_load(i, size=E_ROWS):
            slot = lax.rem(i, 2)
            src = dt_out.at[pl.ds(pl.multiple_of(i * E_ROWS, E_ROWS), size)]
            return pltpu.make_async_copy(src, d_in.at[slot, pl.ds(0, size)], d_sem.at[slot])

        def e_save(i, size=E_ROWS):
            slot = lax.rem(i, 2)
            dst = ge_out.at[pl.ds(pl.multiple_of(i * E_ROWS, E_ROWS), size)]
            return pltpu.make_async_copy(e_stg.at[slot, pl.ds(0, size)], dst, e_sem.at[slot])

        def e_tile(i):
            slot = lax.rem(i, 2)

            @pl.when(i + 1 < full)
            def _():
                d_load(i + 1).start()
            if rest:
                @pl.when(i + 1 == full)
                def _():
                    d_load(full, rest).start()
            d_load(i).wait()

            @pl.when(i == 0)
            def _():
                n_load.wait()

            @pl.when(i >= 2)
            def _():
                e_save(i - 2).wait()
            e_stg[slot] = dot_nn(d_in[slot], n_rows[...].reshape(mbs * mtok, dim))
            e_save(i).start()

        n_load = pltpu.make_async_copy(n_out, n_rows, out_sem.at[1])
        n_load.start()

        def table_start():
            for seq in (rounds * n_tiles - 2, rounds * n_tiles - 1):
                d_copy(seq).wait()
            d_load(0).start()

        @pl.when(s < last)
        def _():
            table_start()
        early = jnp.int32(0)
        for node, tiles in enumerate(EARLY_TILES):
            early = early + jnp.where(s == node, min(tiles, full), 0)
        loop(0, early, e_tile)

        def g_save(mb, count):
            at = pl.ds(mb, count)
            return pltpu.make_async_copy(g_in.at[at], g_out.at[at], out_sem.at[0])

        def gx_forward(c):
            gx_copy(c, 0, 0).wait_recv()
            each_role((3, last, 5), lambda node: gx_send_all(c, node))
            gx_save(c).start()

        def step(k):
            @pl.when(k >= HEAD_MBS)
            def _():
                @pl.when(k < mbs)
                def _():
                    g_final(k)
            b_mb = k - (last - s)

            @pl.when(b_mb == mbs - 1)
            def _():
                g_save(0, mbs - 1).start()

            @pl.when((b_mb >= 0) & (b_mb < mbs))
            def _():
                chunks_of(b_mb, bwd_chunk)

            @pl.when(k == 2)
            def _():
                g_mid(rounds - 1, (5,))

            @pl.when(k == 4)
            def _():
                g_mid(rounds - 1, (6,))

            x_mb = k - n_stage

            @pl.when((s == 3) & (x_mb >= 0) & (x_mb < gx_split // n_half))
            def _():
                chunks_of(x_mb, gx_forward)

        loop(0, mbs + last, step)
        g_save(mbs - 1, 1).start()

        @pl.when(s == last)
        def _():
            table_start()
        kept = jnp.where(s == last, LATE_TILES, 0)
        before = full - early - kept
        first_gx = jnp.where(s == 3, gx_split, 0)

        def late(j):
            c = first_gx + j - before

            @pl.when((j >= before) & (s > 0))
            def _():
                gx_forward(c)
            i = jnp.where(j < before, early + j, full - kept + c - gx_split)

            @pl.when((j < before) | ((c >= gx_split) & (i < full)))
            def _():
                e_tile(i)
            if rest:
                @pl.when(c == gx_split + kept)
                def _():
                    d_load(full, rest).wait()
                    e_save(full - 2).wait()
                    slot = full % 2
                    e_stg[slot, pl.ds(0, rest)] = dot_nn(d_in[slot, pl.ds(0, rest)], n_rows[...].reshape(mbs * mtok, dim))
                    e_save(full, rest).start()

            @pl.when(c == n_chunks - 3)
            def _():
                loss_out[...] = jnp.broadcast_to(jnp.sum(loss_acc[...], axis=1, keepdims=True), loss_out.shape)
                for c in (n_chunks - 2, n_chunks - 1):
                    dpre_copy(c).wait()
                pltpu.make_async_copy(g_in, g_out, out_sem.at[0]).wait()
                sent = stats.at[:, pl.ds(0, last)]
                remote(sent, sent, st_send.at[0], st_recv.at[0], lax.rem(s + 1, n_stage)).wait_send()

                @pl.when(s < last)
                def _():
                    remote(comb, buf_a, g_send.at[0], g_a.at[0], last).wait_send()

                @pl.when(s > 0)
                def _():
                    remote(g_buf, g_in, b_send.at[0], b_recv.at[0], 0).wait_send()

        loop(0, before + n_chunks - first_gx, late)
        if rest:
            e_save(full - 1).wait()
            e_save(full, rest).wait()
        else:
            e_save(full - 2).wait()
            e_save(full - 1).wait()
        pltpu.make_async_copy(gx, gx_out, gx_sem.at[0]).wait()
        for src, routes in gx_routes.items():
            @pl.when(s == src)
            def _(routes=routes):
                for lane, (dst, lo, hi) in enumerate(routes):
                    part = gx if hi - lo == n_chunks else gx.at[pl.ds(0, hi - lo), pl.ds(0, CHUNK)]
                    remote(part, part, gx_send.at[lane], gx_recv.at[0], dst).wait_send()

    pl.run_scoped(
        backward,
        pltpu.VMEM((mbs, mtok, dim), BF16), pltpu.VMEM((2, E_ROWS, mbs * mtok), BF16), pltpu.VMEM((2, E_ROWS, dim), F32),
    )


def pipeline_step(n_stage, labels, part, emb, w1, w2):
    mbs, mtok, dim = part.shape
    rows = emb.shape[0]
    ffn = w1.shape[1]
    chunks = mbs * mtok // CHUNK
    rounds = mbs // HEAD_MBS
    tokens = HEAD_MBS * mtok
    any_spec = pl.BlockSpec(memory_space=pl.ANY)
    vmem_spec = pl.BlockSpec(memory_space=pltpu.VMEM)
    act = pltpu.VMEM((mbs, mtok, dim), BF16)
    dma = pltpu.SemaphoreType.DMA
    act_shape = jax.ShapeDtypeStruct((mbs, mtok, dim), BF16)
    hid_shape = jax.ShapeDtypeStruct((chunks, CHUNK, ffn), BF16)
    return pl.pallas_call(
        functools.partial(step_kernel, n_stage),
        out_shape=(
            jax.ShapeDtypeStruct((chunks, CHUNK, ffn), F32), hid_shape, hid_shape,
            act_shape, act_shape, act_shape, act_shape,
            jax.ShapeDtypeStruct((rows, mbs * mtok), BF16),
            jax.ShapeDtypeStruct((rows, dim), F32),
            jax.ShapeDtypeStruct((8, 128), F32),
        ),
        in_specs=[vmem_spec] + [any_spec] * 4,
        out_specs=(any_spec,) * 9 + (vmem_spec,),
        scratch_shapes=[
            pltpu.VMEM((rows, dim), BF16), pltpu.VMEM((dim, ffn), BF16), pltpu.VMEM((ffn, dim), BF16),
            act, act, act, act, act, act,
            pltpu.VMEM((2, CHUNK, ffn), F32), pltpu.VMEM((2, CHUNK, ffn), BF16),
            pltpu.VMEM((2, vocab_tile(rows), tokens), BF16), pltpu.VMEM((rounds, n_stage, 8, tokens), F32), pltpu.VMEM((1, tokens), F32),
            dma((3,)), dma((1,)), dma((1,)), dma((chunks,)), dma((chunks,)), dma((chunks,)),
            dma((1,)), dma((chunks,)), dma((3,)), dma((chunks,)), dma((1,)), dma((rounds,)),
            dma((1,)), dma((mbs,)), dma((mbs,)), dma((1,)), dma((chunks,)), dma((4,)), dma((chunks,)),
            dma((2,)), dma((2,)), dma((2,)), dma((2,)), dma((2,)), dma((2,)), dma((1,)),
        ],
        compiler_params=pltpu.CompilerParams(collective_id=0, has_side_effects=True, vmem_limit_bytes=VMEM_LIMIT),
        name="pipeline_step",
    )(labels, part, emb, w1, w2)


WINDOW = 256
W_COLS = 1024
E_SLOTS = 4


def tail_kernel(
    rows, tok_ref, loss_ref, x_hbm, g_hbm, gx_hbm, dpre_hbm, hid_hbm, ge_hbm,
    loss_out, g1_out, g2_out, out_hbm,
    x_buf, g_buf, gx_buf, dp_buf, hid_buf, g1_stg, g2_stg, e_buf, packed, packed_id, bounds,
    act_sem, dp_sem, hid_sem, g1_sem, g2_sem, e_in_sem, e_out_sem,
):
    mbs, mtok = tok_ref.shape
    total, dim = g_buf.shape
    ffn = dpre_hbm.shape[1]
    n_blocks = ffn // W_COLS
    e_rows = e_buf.shape[1]
    n_e = rows // e_rows
    per_block = n_e // n_blocks

    def cols(j):
        return pl.ds(pl.multiple_of(j * W_COLS, W_COLS), W_COLS)

    def e_at(i):
        return pl.ds(pl.multiple_of(i * e_rows, 8), e_rows)

    def dp_load(j):
        slot = lax.rem(j, 2)
        return pltpu.make_async_copy(dpre_hbm.at[:, cols(j)], dp_buf.at[slot], dp_sem.at[slot])

    def hid_load(j):
        slot = lax.rem(j, 2)
        return pltpu.make_async_copy(hid_hbm.at[:, cols(j)], hid_buf.at[slot], hid_sem.at[slot])

    def e_load(i):
        slot = lax.rem(i, E_SLOTS)
        return pltpu.make_async_copy(ge_hbm.at[e_at(i)], e_buf.at[slot], e_in_sem.at[slot])

    def e_save(i):
        slot = lax.rem(i, E_SLOTS)
        return pltpu.make_async_copy(e_buf.at[slot], out_hbm.at[e_at(i)], e_out_sem.at[slot])

    def g1_save(j):
        return pltpu.make_async_copy(g1_stg, g1_out.at[0, :, cols(j)], g1_sem.at[0])

    def g2_save(j):
        return pltpu.make_async_copy(g2_stg, g2_out.at[0, cols(j)], g2_sem.at[0])

    x_load = pltpu.make_async_copy(x_hbm, x_buf, act_sem.at[0])
    g_load = pltpu.make_async_copy(g_hbm, g_buf, act_sem.at[1])
    gx_load = pltpu.make_async_copy(gx_hbm, gx_buf, act_sem.at[2])
    gx_load.start()
    loss_out[0] = loss_ref[0, 0] * (1.0 / total)

    s = lax.axis_index("stage")
    loc = tok_ref[...] - s * rows
    upper, lower = triangles(mbs, mtok)
    slot_of = jnp.full((mbs, mtok), -1.0, F32)
    count = jnp.int32(0)
    bounds[0] = count
    for i in range(n_e):
        inside = (loc >= i * e_rows) & (loc < (i + 1) * e_rows)
        rank, number = ranks(inside.astype(F32), upper, lower)
        slot_of = jnp.where(inside, rank + count.astype(F32), slot_of)
        count = count + number
        bounds[i + 1] = count
    slot_of = slot_of.astype(jnp.int32)
    n_packs = jnp.maximum((count + WINDOW - 1) // WINDOW, 1)

    def pack(b):
        slot = lax.broadcasted_iota(jnp.int32, (WINDOW, mtok), 0) + b * WINDOW
        ids = jnp.zeros((WINDOW, 1), F32)
        picks = []
        for mb in range(mbs):
            pick = slot == slot_of[mb:mb + 1, :]
            picks.append(pick.astype(BF16))
            ids = ids + jnp.sum(jnp.where(pick, loc[mb:mb + 1, :].astype(F32), 0.0), axis=1, keepdims=True)
        at = pl.ds(pl.multiple_of(b * WINDOW, WINDOW), WINDOW)
        packed[at, :] = dot_nn(jnp.concatenate(picks, axis=1), gx_buf[...]).astype(BF16)
        filled = lax.broadcasted_iota(jnp.int32, (WINDOW, 1), 0) + b * WINDOW < count
        packed_id[at, :] = jnp.broadcast_to(jnp.where(filled, ids.astype(jnp.int32), -1), (WINDOW, 128))

    def loop(lo, hi, fn):
        def body(i, _):
            fn(i)
            return 0
        lax.fori_loop(lo, hi, body, 0)

    def e_tile(i):
        slot = lax.rem(i, E_SLOTS)
        first = jnp.minimum((bounds[i] // 16) * 16, (n_packs - 1) * WINDOW)
        lane = lax.broadcasted_iota(jnp.int32, (WINDOW, e_rows), 1) + i * e_rows

        def window(k):
            start = pl.multiple_of(jnp.minimum(first + k * WINDOW, (n_packs - 1) * WINDOW), 16)
            at = pl.ds(start, WINDOW)
            fresh = lax.broadcasted_iota(jnp.int32, (WINDOW, 1), 0) + start >= first + k * WINDOW
            ids = jnp.where(fresh, packed_id[at, :][:, 0:1], -1)
            return dot_tn((lane == ids).astype(BF16), packed[at, :])

        e_load(i).wait()
        e_buf[slot] = e_buf[slot] + window(0)

        def more(k):
            e_buf[slot] = e_buf[slot] + window(k)

        loop(1, (bounds[i + 1] - first + WINDOW - 1) // WINDOW, more)
        e_save(i).start()

    def block(j):
        slot = lax.rem(j, 2)

        @pl.when(j == 0)
        def _():
            x_load.wait()

        @pl.when(j > 0)
        def _():
            g1_save(j - 1).wait()
        dp_load(j).wait()

        @pl.when(j == 0)
        def _():
            for cp in (e_load(0), e_load(1), g_load, hid_load(0)):
                cp.start()
        g1_stg[...] = dot_tn(x_buf[...], dp_buf[slot])
        g1_save(j).start()

        @pl.when(j + 1 < n_blocks)
        def _():
            dp_load(j + 1).start()

        def tile(i):
            @pl.when(i + 2 < n_e)
            def _():
                @pl.when(i + 2 >= E_SLOTS)
                def _():
                    e_save(i + 2 - E_SLOTS).wait()
                e_load(i + 2).start()
            e_tile(i)

        loop(j * per_block, (j + 1) * per_block, tile)

        @pl.when(j == 0)
        def _():
            g_load.wait()

        @pl.when(j > 0)
        def _():
            g2_save(j - 1).wait()
        hid_load(j).wait()

        @pl.when(j + 1 < n_blocks)
        def _():
            hid_load(j + 1).start()
        g2_stg[...] = dot_tn(hid_buf[slot], g_buf[...])
        g2_save(j).start()

    x_load.start()
    dp_load(0).start()
    gx_load.wait()
    loop(0, n_packs, pack)
    loop(0, n_blocks, block)
    g1_save(n_blocks - 1).wait()
    g2_save(n_blocks - 1).wait()
    for i in range(max(n_e - E_SLOTS, 0), n_e):
        e_save(i).wait()


def tail(tok, loss, x, g, gx, dpre, hid, ge):
    rows, dim = ge.shape
    total, ffn = dpre.shape
    n_blocks = ffn // W_COLS
    e_rows = rows // (2 * n_blocks)
    n_e = rows // e_rows
    any_spec = pl.BlockSpec(memory_space=pl.ANY)
    vmem_spec = pl.BlockSpec(memory_space=pltpu.VMEM)
    dma = pltpu.SemaphoreType.DMA
    act = pltpu.VMEM((total, dim), BF16)
    return pl.pallas_call(
        functools.partial(tail_kernel, rows),
        out_shape=(
            jax.ShapeDtypeStruct((1,), F32),
            jax.ShapeDtypeStruct((1, dim, ffn), F32),
            jax.ShapeDtypeStruct((1, ffn, dim), F32),
            jax.ShapeDtypeStruct((rows, dim), F32),
        ),
        in_specs=[vmem_spec, vmem_spec] + [any_spec] * 6,
        out_specs=(pl.BlockSpec(memory_space=pltpu.SMEM), any_spec, any_spec, any_spec),
        scratch_shapes=[
            act, act, act, pltpu.VMEM((2, total, W_COLS), BF16), pltpu.VMEM((2, total, W_COLS), BF16),
            pltpu.VMEM((dim, W_COLS), F32), pltpu.VMEM((W_COLS, dim), F32), pltpu.VMEM((E_SLOTS, e_rows, dim), F32),
            pltpu.VMEM((total, dim), BF16), pltpu.VMEM((total, 128), jnp.int32), pltpu.SMEM((n_e + 1,), jnp.int32),
            dma((3,)), dma((2,)), dma((2,)), dma((1,)), dma((1,)), dma((E_SLOTS,)), dma((E_SLOTS,)),
        ],
        compiler_params=pltpu.CompilerParams(vmem_limit_bytes=VMEM_LIMIT),
        name="tail",
    )(tok, loss, x, g, gx, dpre, hid, ge)


def solution(mesh):
    n_stage = mesh.shape["stage"]

    def stage_body(token_ids, label_ids, emb_rows, w_in, w_out):
        tokens = token_ids.shape[0] * token_ids.shape[1]
        part = lookup(token_ids, emb_rows)
        _, hid, dpre, x_in, _, g_all, gx, _, ge, loss = pipeline_step(n_stage, label_ids, part, emb_rows, w_in[0], w_out[0])
        flat = lambda a: a.reshape(tokens, a.shape[-1])
        mean_loss, grad_in, grad_out, grad_emb = tail(token_ids, loss, flat(x_in), flat(g_all), flat(gx), flat(dpre), flat(hid), ge)
        return mean_loss, grad_in, grad_out, grad_emb

    return jax.shard_map(
        stage_body,
        mesh=mesh,
        in_specs=(P("dp", None), P("dp", None), P("stage", None), P("stage", None, None), P("stage", None, None)),
        out_specs=(P("dp"), P(("dp", "stage"), None, None), P(("dp", "stage"), None, None), P(("dp", "stage"), None)),
        check_vma=False,
    )
```

```python
import functools
import math

import jax
import jax.numpy as jnp
from jax import lax
from jax.experimental import pallas as pl
from jax.experimental.pallas import tpu as pltpu
from jax.sharding import PartitionSpec as P

NORM_EPS = 1e-6
MESH = pl.DeviceIdType.MESH
F32 = jnp.float32
BF16 = jnp.bfloat16
GELU_A = math.sqrt(2.0 / math.pi)
GELU_B = 0.044715
LOG2E = math.log2(math.e)
CHUNK = 128
HEAD_MBS = 2
VMEM_LIMIT = 67_000_000


def dot_nn(a, b):
    return lax.dot_general(a, b, (((1,), (0,)), ((), ())), preferred_element_type=F32)


def dot_nt(a, b):
    return lax.dot_general(a, b, (((1,), (1,)), ((), ())), preferred_element_type=F32)


def dot_tn(a, b):
    return lax.dot_general(a, b, (((0,), (0,)), ((), ())), preferred_element_type=F32)


def gelu_and_slope(pre):
    sq = pre * pre
    th = jnp.tanh(pre * (GELU_A + (GELU_A * GELU_B) * sq))
    half_sum = 0.5 + 0.5 * th
    hid = pre * half_sum
    slope = half_sum + (hid - hid * th) * (GELU_A + (3.0 * GELU_A * GELU_B) * sq)
    return hid, slope


def norm_scale(x_f32):
    return lax.rsqrt(jnp.mean(x_f32 * x_f32, axis=-1, keepdims=True) + NORM_EPS)


def remote(src, dst, send_sem, recv_sem, stage):
    return pltpu.make_async_remote_copy(
        src_ref=src, dst_ref=dst, send_sem=send_sem, recv_sem=recv_sem, device_id={"stage": stage}, device_id_type=MESH
    )


def group_barrier(stage, n_stage):
    barrier = pltpu.get_barrier_semaphore()
    for off in range(1, n_stage):
        pl.semaphore_signal(barrier, inc=1, device_id={"stage": lax.rem(stage + off, n_stage)}, device_id_type=MESH)
    pl.semaphore_wait(barrier, n_stage - 1)


def vocab_tile(rows):
    for parts in range(2, rows + 1):
        if rows % parts == 0 and (rows // parts) % 16 == 0 and rows // parts <= 2400:
            return rows // parts
    return rows


def sub_blocks(rows, size):
    return [(start, min(size, rows - start)) for start in range(0, rows, size)]


def forward_chunk(x, w1, w2, slope_slot, hid_slot):
    ffn = w1.shape[1]
    width = ffn // 4
    for part in range(4):
        cols = pl.ds(part * width, width)
        hid, slope = gelu_and_slope(dot_nn(x, w1[:, cols]))
        slope_slot[:, cols] = slope
        hid_slot[:, cols] = hid.astype(BF16)
    return x.astype(F32) + dot_nn(hid_slot[...], w2[...])


def forward_pair(x, w1, w2, slope_slots, hid_slots):
    ffn = w1.shape[1]
    width = ffn // 4
    for part in range(4):
        cols = pl.ds(part * width, width)
        hid, slope = gelu_and_slope(dot_nn(x, w1[:, cols]))
        for slot in range(2):
            slope_slots[slot, :, cols] = slope[slot * CHUNK:(slot + 1) * CHUNK]
            hid_slots[slot, :, cols] = hid[slot * CHUNK:(slot + 1) * CHUNK].astype(BF16)
    return x.astype(F32) + dot_nn(hid_slots[...].reshape(2 * CHUNK, ffn), w2[...])


def backward_chunk(grad, w2_t, w1_t, slope_slot, dpre_slot):
    ffn = slope_slot.shape[1]
    dim = grad.shape[1]
    for part in range(ffn // dim):
        cols = pl.ds(part * dim, dim)
        dpre_slot[:, cols] = (dot_nn(grad, w2_t[:, cols]) * slope_slot[:, cols]).astype(BF16)
    return grad.astype(F32) + dot_nn(dpre_slot[...], w1_t[...])


def swap_transposed(w1, w2):
    dim, ffn = w1.shape
    side = 256

    def strip(part, _):
        at = pl.ds(pl.multiple_of(part * side, side), side)
        for i in range(dim // side):
            rows = pl.ds(i * side, side)
            from_w1 = w1[rows, at].T
            from_w2 = w2[at, rows].T
            w2[at, rows] = from_w1
            w1[rows, at] = from_w2
        return 0

    lax.fori_loop(0, ffn // side, strip, 0)


def head_logits(n_t, emb, logits, lab_row, tokens):
    rows = emb.shape[0]
    tile = vocab_tile(rows)
    c2 = LOG2E * emb.shape[1] ** -0.5

    def tile_step(idx, carry):
        mx, sm, lb = carry
        base = pl.multiple_of(idx * tile, 16)
        for start, size in sub_blocks(tile, 256):
            at = pl.ds(base + start, size)
            block = dot_nn(emb[at, :], n_t[...])
            logits[at, :] = block
            b3 = block.reshape(size // 8, 8, tokens)
            row_ids = lax.broadcasted_iota(jnp.int32, (size, tokens), 0) + (base + start)
            hit = jnp.where(row_ids == lab_row, block, 0.0).reshape(size // 8, 8, tokens)
            mx_new = jnp.maximum(mx, jnp.max(b3, axis=0))
            sm = sm * jnp.exp2((mx - mx_new) * c2) + jnp.sum(jnp.exp2((b3 - mx_new[None]) * c2), axis=0)
            lb = lb + jnp.sum(hit, axis=0)
            mx = mx_new
        return mx, sm, lb

    init = (jnp.full((8, tokens), -3.0e38, F32), jnp.zeros((8, tokens), F32), jnp.zeros((8, tokens), F32))
    mx, sm, lb = lax.fori_loop(0, rows // tile, tile_step, init)
    top = jnp.max(mx, axis=0, keepdims=True)
    tot = jnp.sum(sm * jnp.exp2((mx - top) * c2), axis=0, keepdims=True)
    lab = jnp.sum(lb, axis=0, keepdims=True)
    return top, tot, lab


def head_grad_tile(base, size_all, emb, logits, d_slot, lab_row, shift, tokens):
    scale = emb.shape[1] ** -0.5
    c2 = LOG2E * scale
    total = None
    for start, size in sub_blocks(size_all, 256):
        at = pl.ds(base + start, size)
        row_ids = lax.broadcasted_iota(jnp.int32, (size, tokens), 0) + (base + start)
        prob = jnp.exp2(logits[at, :] * c2 - shift)
        d_log = (prob - jnp.where(row_ids == lab_row, scale, 0.0)).astype(BF16)
        d_slot[pl.ds(start, size), :] = d_log
        part = dot_tn(d_log, emb[at, :])
        total = part if total is None else total + part
    return total


LOOK = 192
LOOK_BASE = 512


def look_at(row):
    return pl.ds(pl.multiple_of(row, 16), LOOK)


def ranks(flag, upper, lower):
    within = dot_nn(flag.astype(BF16), upper)
    total = jnp.sum(flag, axis=1, keepdims=True)
    rows = flag.shape[0]
    before = jnp.sum(jnp.where(lower, jnp.transpose(jnp.broadcast_to(total, (rows, rows))), 0.0), axis=1, keepdims=True)
    return within - flag + before, jnp.sum(flag).astype(jnp.int32)


def triangles(mbs, mtok):
    upper = (lax.broadcasted_iota(jnp.int32, (mtok, mtok), 0)
             <= lax.broadcasted_iota(jnp.int32, (mtok, mtok), 1)).astype(BF16)
    lower = lax.broadcasted_iota(jnp.int32, (mbs, mbs), 1) < lax.broadcasted_iota(jnp.int32, (mbs, mbs), 0)
    return upper, lower


def lookup_kernel(tok_ref, emb_hbm, part_hbm, emb, part, rank_ref, picks, found, emb_sem, part_sem):
    mbs, mtok = tok_ref.shape
    rows, dim = emb.shape
    tile = vocab_tile(rows)
    n_tiles = rows // tile
    loads = [pltpu.make_async_copy(emb_hbm.at[pl.ds(i * tile, tile)], emb.at[pl.ds(i * tile, tile)], emb_sem.at[i])
             for i in range(n_tiles)]
    for ld in loads:
        ld.start()

    picks[:, pl.ds(0, LOOK_BASE + LOOK), :] = jnp.zeros((mbs, LOOK_BASE + LOOK, mtok), BF16)
    found[pl.ds(0, LOOK_BASE + LOOK), :] = jnp.zeros((LOOK_BASE + LOOK, dim), BF16)
    loc = tok_ref[...] - lax.axis_index("stage") * rows
    upper, lower = triangles(mbs, mtok)
    counts = []
    for i in range(n_tiles):
        inside = (loc >= i * tile) & (loc < (i + 1) * tile)
        rank, number = ranks(inside.astype(F32), upper, lower)
        rank_ref[i] = jnp.where(inside, rank, -1.0).astype(jnp.int32)
        counts.append(number)

    def window(i, k, row):
        slot = lax.broadcasted_iota(jnp.int32, (LOOK, mtok), 0) + k * LOOK
        ids = jnp.zeros((LOOK, 1), F32)
        for mb in range(mbs):
            pick = slot == rank_ref[i, mb:mb + 1, :]
            picks[mb, look_at(row), :] = pick.astype(BF16)
            ids = ids + jnp.sum(jnp.where(pick, loc[mb:mb + 1, :].astype(F32), 0.0), axis=1, keepdims=True)
        filled = lax.broadcasted_iota(jnp.int32, (LOOK, 1), 0) + k * LOOK < counts[i]
        return jnp.where(filled, ids.astype(jnp.int32), -1)

    def find(i, row, ids):
        lane = lax.broadcasted_iota(jnp.int32, (LOOK, tile), 1) + i * tile
        rows_found = dot_nn((lane == ids).astype(BF16), emb[pl.ds(i * tile, tile), :])
        found[look_at(row), :] = rows_found.astype(BF16)

    starts = [jnp.int32(0)]
    for number in counts:
        starts.append(starts[-1] + (jnp.minimum(number, LOOK) + 15) // 16 * 16)
    first_ids = [window(i, 0, starts[i]) for i in range(n_tiles)]
    for i in range(n_tiles):
        loads[i].wait()
        find(i, starts[i], first_ids[i])

    extra_end = jnp.int32(1)
    for i in range(n_tiles):
        def extra(k, w, i=i):
            row = LOOK_BASE + w * LOOK
            find(i, row, window(i, k, row))
            return w + 1
        extra_end = lax.fori_loop(1, (counts[i] + LOOK - 1) // LOOK, extra, extra_end)
    crowded = (extra_end > 1) | (starts[n_tiles] > LOOK_BASE)

    def save(mb):
        return pltpu.make_async_copy(part.at[mb], part_hbm.at[mb], part_sem.at[mb])

    for mb in range(mbs):
        part[mb] = dot_tn(picks[mb, 0:LOOK_BASE, :], found[0:LOOK_BASE, :]).astype(BF16)

        @pl.when(jnp.logical_not(crowded))
        def _(mb=mb):
            save(mb).start()

    @pl.when(crowded)
    def _():
        def add_mb(mb, _):
            def add(w, _):
                at = look_at(LOOK_BASE + w * LOOK)
                part[mb] = part[mb] + dot_tn(picks[mb, at, :], found[at, :]).astype(BF16)
                return 0
            lax.fori_loop(0, extra_end, add, 0)
            save(mb).start()
            return 0
        lax.fori_loop(0, mbs, add_mb, 0)

    for mb in range(mbs):
        save(mb).wait()


def lookup(tok, emb):
    mbs, mtok = tok.shape
    rows, dim = emb.shape
    n_tiles = rows // vocab_tile(rows)
    slots = LOOK_BASE + (1 + mbs * mtok // LOOK) * LOOK
    any_spec = pl.BlockSpec(memory_space=pl.ANY)
    dma = pltpu.SemaphoreType.DMA
    return pl.pallas_call(
        lookup_kernel,
        out_shape=jax.ShapeDtypeStruct((mbs, mtok, dim), BF16),
        in_specs=[pl.BlockSpec(memory_space=pltpu.VMEM), any_spec],
        out_specs=any_spec,
        scratch_shapes=[
            pltpu.VMEM((rows, dim), BF16), pltpu.VMEM((mbs, mtok, dim), BF16), pltpu.VMEM((n_tiles, mbs, mtok), jnp.int32),
            pltpu.VMEM((mbs, slots, mtok), BF16), pltpu.VMEM((slots, dim), BF16),
            dma((n_tiles,)), dma((mbs,)),
        ],
        compiler_params=pltpu.CompilerParams(vmem_limit_bytes=VMEM_LIMIT),
        name="lookup",
    )(tok, emb)


E_ROWS = 512
LATE_TILES = 3
EARLY_TILES = (11, 9, 8, 6, 4, 3, 0, 0)
LOOKUP_LEAD = 8
LOOKUP_PARENT = {2: (3, 0), 1: (0, 0), 4: (5, 0), 6: (7, 0), 5: (3, 1), 7: (0, 1), 3: (0, 2)}
GRAD_PARENT = {0: (1, 0), 2: (3, 0), 4: (5, 0), 1: (6, 0), 6: (7, 0), 3: (5, 1), 5: (7, 1)}


def step_kernel(
    n_stage, lab_ref, part_hbm, emb_hbm, w1_hbm, w2_hbm,
    slope_out, hid_out, dpre_out, xin_out, n_out, g_out, gx_out, dt_out, ge_out, loss_out,
    emb, w1, w2, x_in, x_out, n_all, comb, buf_a, buf_b, slope_stg, act_stg, d_stg, stats, loss_acc,
    load_sem, part_sem, lk_send, lk_a, lk_b, lk_c, x_send, x_recv, n_send, n_recv, st_send, st_recv,
    g_send, g_a, g_b, b_send, b_recv, gx_send, gx_recv, slope_sem, act_sem, dt_sem, d_sem, e_sem, out_sem, gx_sem,
):
    s = lax.axis_index("stage")
    last = n_stage - 1
    mbs, mtok, dim = x_in.shape
    n_half = mtok // CHUNK
    n_chunks = mbs * n_half
    rows = emb.shape[0]
    ffn = w1.shape[1]
    tile = vocab_tile(rows)
    tokens = HEAD_MBS * mtok
    rounds = mbs // HEAD_MBS
    scale = dim ** -0.5
    c2 = LOG2E * scale
    row_start = s * rows
    bufs = (buf_a, buf_b, x_in)
    lk_sems = (lk_a, lk_b, lk_c)

    loads = [pltpu.make_async_copy(src, dst, load_sem.at[i])
             for i, (src, dst) in enumerate([(w1_hbm, w1), (w2_hbm, w2), (emb_hbm, emb)])]
    part_load = pltpu.make_async_copy(part_hbm, comb, part_sem.at[0])
    part_load.start()
    group_barrier(s, n_stage)

    def pos(c):
        return (c // n_half, pl.ds(pl.multiple_of(lax.rem(c, n_half) * CHUNK, CHUNK), CHUNK))

    def at_chunk(ref, c):
        return ref.at[c // n_half, pl.ds(pl.multiple_of(lax.rem(c, n_half) * CHUNK, CHUNK), CHUNK)]

    def loop(lo, hi, fn):
        def body(i, _):
            fn(i)
            return 0
        lax.fori_loop(lo, hi, body, 0)

    def chunks_of(mb, fn):
        loop(mb * n_half, (mb + 1) * n_half, fn)

    def each_role(roles, fn):
        for node in roles:
            @pl.when(s == node)
            def _(node=node):
                fn(node)

    def lk_copy(c, child):
        parent, slot = LOOKUP_PARENT[child]
        return remote(at_chunk(comb, c), at_chunk(bufs[slot], c), lk_send.at[0], lk_sems[slot].at[c], parent)

    def lk_total(c, slots):
        total = comb[pos(c)].astype(F32)
        for slot in range(slots):
            remote(at_chunk(comb, c), at_chunk(bufs[slot], c), lk_send.at[0], lk_sems[slot].at[c], 0).wait_recv()
            total = total + bufs[slot][pos(c)].astype(F32)
        return total.astype(BF16)

    def lk_forward(c, node, slots):
        comb[pos(c)] = lk_total(c, slots)
        lk_copy(c, node).start()

    part_load.wait()
    each_role((1, 2, 4, 6), lambda node: loop(0, n_chunks, lambda c: lk_copy(c, node).start()))
    for ld in loads:
        ld.start()
    each_role((5, 7), lambda node: loop(0, n_chunks, lambda c: lk_forward(c, node, 1)))
    each_role((3,), lambda node: loop(0, LOOKUP_LEAD, lambda c: lk_forward(c, node, 2)))
    loads[0].wait()
    loads[1].wait()

    n_routes = {last: (5, 1, 6), 5: (4,), 1: (3, 0), 3: (2,)}

    def x_copy(c, dst_stage):
        return remote(at_chunk(x_out, c), at_chunk(x_in, c), x_send.at[0], x_recv.at[c], dst_stage)

    def n_copy(c, lane, dst_stage):
        return remote(at_chunk(n_all, c), at_chunk(n_all, c), n_send.at[lane], n_recv.at[c], dst_stage)

    def fwd_copies(c):
        slot = lax.rem(c, 2)
        return (pltpu.make_async_copy(slope_stg.at[slot], slope_out.at[c], slope_sem.at[slot]),
                pltpu.make_async_copy(act_stg.at[slot], hid_out.at[c], act_sem.at[slot]))

    def slope_copy(c):
        slot = lax.rem(c, 2)
        return pltpu.make_async_copy(slope_out.at[c], slope_stg.at[slot], slope_sem.at[slot])

    def fwd_chunk(c):
        idx = pos(c)

        @pl.when((s == 3) & (c + LOOKUP_LEAD < n_chunks))
        def _():
            lk_forward(c + LOOKUP_LEAD, 3, 2)

        @pl.when(s == 0)
        def _():
            x_in[idx] = lk_total(c, 3)

        @pl.when(s > 0)
        def _():
            x_copy(c, 0).wait_recv()

        @pl.when(c >= 2)
        def _():
            for cp in fwd_copies(c - 2):
                cp.wait()

        slot = lax.rem(c, 2)
        out = forward_chunk(x_in[idx], w1, w2, slope_stg.at[slot], act_stg.at[slot]).astype(BF16)
        x_out[idx] = out
        for cp in fwd_copies(c):
            cp.start()

        @pl.when(s < last)
        def _():
            x_copy(c, s + 1).start()

        @pl.when(s == last)
        def _():
            out_f = out.astype(F32)
            n_all[idx] = (out_f * norm_scale(out_f)).astype(BF16)
            for lane, dst in enumerate(n_routes[last]):
                n_copy(c, lane, dst).start()

    def last_fwd_pair(mb):
        first = mb * n_half
        for c in (first, first + 1):
            x_copy(c, 0).wait_recv()
            for cp in fwd_copies(c - 2):
                cp.wait()
        out = forward_pair(x_in[mb], w1, w2, slope_stg, act_stg).astype(BF16)
        x_out[mb] = out
        out_f = out.astype(F32)
        n_all[mb] = (out_f * norm_scale(out_f)).astype(BF16)
        for c in (first, first + 1):
            for cp in fwd_copies(c):
                cp.start()
            for lane, dst in enumerate(n_routes[last]):
                n_copy(c, lane, dst).start()

    def n_round(r, fn):
        loop(r * HEAD_MBS * n_half, (r + 1) * HEAD_MBS * n_half, fn)

    def n_early(r):
        def take(c, node):
            n_copy(c, 0, 0 if node == last else last).wait_recv()
            for lane, dst in enumerate(n_routes[node]):
                n_copy(c, lane, dst).start()
        each_role((1, 5), lambda node: n_round(r, lambda c: take(c, node)))

    def n_mid(r):
        def take(c, node):
            n_copy(c, 0, last).wait_recv()
            n_copy(c, 0, n_routes[node][0]).start()
        each_role((3,), lambda node: n_round(r, lambda c: take(c, node)))

    def n_late(r):
        @pl.when((lax.rem(s, 2) == 0))
        def _():
            n_round(r, lambda c: n_copy(c, 0, last).wait_recv())

    def g_copy(mb, child):
        parent, slot = GRAD_PARENT[child]
        return remote(comb.at[mb], bufs[slot].at[mb], g_send.at[0], (g_a, g_b)[slot].at[mb], parent)

    def g_total(mb, slots):
        total = comb[mb].astype(F32)
        for slot in range(slots):
            remote(comb.at[mb], bufs[slot].at[mb], g_send.at[0], (g_a, g_b)[slot].at[mb], 0).wait_recv()
            total = total + bufs[slot][mb].astype(F32)
        return total

    def g_forward(mb, node, slots):
        comb[mb] = g_total(mb, slots).astype(BF16)
        g_copy(mb, node).start()

    def g_low(r):
        each_role((1, 3), lambda node: loop(r * HEAD_MBS, (r + 1) * HEAD_MBS, lambda mb: g_forward(mb, node, 1)))

    def g_mid(r, nodes=(5, 6)):
        each_role(nodes, lambda node: loop(r * HEAD_MBS, (r + 1) * HEAD_MBS, lambda mb: g_forward(mb, node, {5: 2, 6: 1}[node])))

    def g_final(mb):
        @pl.when(s == last)
        def _():
            grad_n = g_total(mb, 2)
            x_f = x_out[mb].astype(F32)
            inv = norm_scale(x_f)
            n_f = x_f * inv
            dx = inv * (grad_n - n_f * jnp.mean(grad_n * n_f, axis=-1, keepdims=True))
            comb[mb] = dx.astype(BF16)

    def lab_row_of(r):
        parts = [lab_ref[pl.ds(r * HEAD_MBS + i, 1), :] for i in range(HEAD_MBS)]
        return jnp.concatenate(parts, axis=1) - row_start

    def st_copy(r, off):
        dst = lax.rem(s + off, n_stage)
        return remote(stats.at[r, s], stats.at[r, s], st_send.at[0], st_recv.at[r], dst)

    saves = [pltpu.make_async_copy(x_in, xin_out, out_sem.at[0]), pltpu.make_async_copy(n_all, n_out, out_sem.at[1])]

    n_tiles = rows // tile

    def d_copy(seq):
        slot = lax.rem(seq, 2)
        r = seq // n_tiles
        idx = lax.rem(seq, n_tiles)
        dst = dt_out.at[pl.ds(pl.multiple_of(idx * tile, 16), tile), pl.ds(pl.multiple_of(r * tokens, tokens), tokens)]
        return pltpu.make_async_copy(d_stg.at[slot], dst, dt_sem.at[slot])

    def forward_and_head(logits, n_t, gn_acc):
        def head_a(r):
            n_late(r)

            @pl.when(r == rounds - 1)
            def _():
                for cp in saves:
                    cp.start()

            n_t[...] = n_all[pl.ds(r * HEAD_MBS, HEAD_MBS)].reshape(tokens, dim).T
            top, tot, lab = head_logits(n_t, emb, logits, lab_row_of(r), tokens)

            @pl.when(r == rounds - 1)
            def _():
                for cp in saves:
                    cp.wait()

                for src, dsts in n_routes.items():
                    @pl.when(s == src)
                    def _(dsts=dsts):
                        for lane, dst in enumerate(dsts):
                            remote(n_all, n_all, n_send.at[lane], n_recv.at[0], dst).wait_send()
            stats[r, s] = jnp.concatenate([top, tot, lab, jnp.zeros((5, tokens), F32)], axis=0)
            for off in range(1, n_stage):
                st_copy(r, off).start()

        def head_b(r):
            @pl.when(r + 1 < rounds)
            def _():
                n_early(r + 1)

            @pl.when((r == rounds - 2) & (s < last))
            def _():
                remote(x_out, x_in, x_send.at[0], x_recv.at[0], 0).wait_send()

            @pl.when(r == rounds - 1)
            def _():
                for c in (n_chunks - 2, n_chunks - 1):
                    for cp in fwd_copies(c):
                        cp.wait()
                slope_copy(0).start()
                slope_copy(1).start()

            @pl.when(r == jnp.where(s == last, rounds - 1, rounds - 2))
            def _():
                swap_transposed(w1, w2)
            others = stats.at[r, pl.ds(0, last)]
            remote(others, others, st_send.at[0], st_recv.at[r], lax.rem(s + 1, n_stage)).wait_recv()
            blocks = [stats[r, i] for i in range(n_stage)]
            top = blocks[0][0:1]
            for blk in blocks[1:]:
                top = jnp.maximum(top, blk[0:1])
            tot = jnp.zeros_like(top)
            lab = jnp.zeros_like(top)
            for blk in blocks:
                tot = tot + blk[1:2] * jnp.exp2((blk[0:1] - top) * c2)
                lab = lab + blk[2:3]
            loss_acc[...] = loss_acc[...] + (jnp.log(tot) + (top - lab) * scale)
            shift = top * c2 + (jnp.log(tot) * LOG2E - math.log2(scale))
            lab_row = lab_row_of(r)

            def tile_step(idx):
                seq = r * n_tiles + idx

                @pl.when(seq >= 2)
                def _():
                    d_copy(seq - 2).wait()
                @pl.when((idx == n_tiles - 1) & (r + 1 < rounds))
                def _():
                    n_mid(r + 1)
                base = pl.multiple_of(idx * tile, 16)
                part = head_grad_tile(base, tile, emb, logits, d_stg.at[lax.rem(seq, 2)], lab_row, shift, tokens)
                gn_acc[...] = gn_acc[...] + part
                d_copy(seq).start()

            gn_acc[...] = jnp.zeros_like(gn_acc)
            loop(0, n_tiles, tile_step)
            comb[pl.ds(r * HEAD_MBS, HEAD_MBS)] = gn_acc[...].reshape(HEAD_MBS, mtok, dim).astype(BF16)
            each_role((0, 2, 4), lambda node: loop(r * HEAD_MBS, (r + 1) * HEAD_MBS, lambda mb: g_copy(mb, node).start()))
        loss_acc[...] = jnp.zeros_like(loss_acc)
        first_a = HEAD_MBS + 1 + last

        def step(k):
            f_mb = k - s

            paired = (s == last) & (f_mb >= 2 * HEAD_MBS)

            @pl.when((f_mb >= 0) & (f_mb < mbs) & jnp.logical_not(paired))
            def _():
                chunks_of(f_mb, fwd_chunk)

            @pl.when((f_mb < mbs) & paired)
            def _():
                last_fwd_pair(f_mb)

            @pl.when(k == first_a)
            def _():
                loads[2].wait()

                @pl.when(s > 0)
                def _():
                    remote(comb, buf_a, lk_send.at[0], lk_a.at[0], 0).wait_send()

            rel = k - first_a
            r = rel // HEAD_MBS
            even = lax.rem(rel + HEAD_MBS * n_stage, HEAD_MBS) == 0

            @pl.when(k == first_a)
            def _():
                n_early(0)
                n_mid(0)

            @pl.when(even & (rel >= 0))
            def _():
                head_a(r)

            @pl.when(even & (rel >= HEAD_MBS))
            def _():
                g_low(r - 1)

                @pl.when(r == 2)
                def _():
                    loop(0, HEAD_MBS, g_final)

            @pl.when(jnp.logical_not(even) & (rel >= 0))
            def _():
                head_b(r)

            @pl.when(jnp.logical_not(even) & (rel >= HEAD_MBS))
            def _():
                g_mid(r - 1)

        loop(0, first_a + HEAD_MBS * rounds, step)
        g_low(rounds - 1)

    pl.run_scoped(
        forward_and_head,
        pltpu.VMEM((rows, tokens), F32), pltpu.VMEM((dim, tokens), BF16), pltpu.VMEM((tokens, dim), F32),
    )

    g_in, g_buf, gx = x_in, x_out, n_all

    def b_copy(c, dst):
        return remote(at_chunk(g_buf, c), at_chunk(g_in, c), b_send.at[0], b_recv.at[c], dst)

    def gx_copy(c, lane, dst):
        return remote(at_chunk(gx, c), at_chunk(gx, c), gx_send.at[lane], gx_recv.at[c], dst)

    def dpre_copy(c):
        slot = lax.rem(c, 2)
        return pltpu.make_async_copy(act_stg.at[slot], dpre_out.at[c], act_sem.at[slot])

    gx_split = n_chunks // 2
    gx_routes = {0: ((5, n_chunks - 1, n_chunks), (3, 0, n_chunks), (last, 0, n_chunks), (1, 0, n_chunks)), 3: ((2, 0, n_chunks), (5, 0, gx_split)),
                 last: ((6, 0, n_chunks), (5, gx_split, n_chunks - 1)), 5: ((4, 0, n_chunks),)}

    def gx_send_all(c, node):
        for lane, (dst, lo, hi) in enumerate(gx_routes[node]):
            @pl.when((c >= lo) & (c < hi))
            def _(lane=lane, dst=dst):
                gx_copy(c, lane, dst).start()


    def gx_save(c):
        return pltpu.make_async_copy(at_chunk(gx, c), at_chunk(gx_out, c), gx_sem.at[0])

    def bwd_chunk(c):
        slot = lax.rem(c, 2)
        idx = pos(c)

        @pl.when(s < last)
        def _():
            b_copy(c, 0).wait_recv()

        @pl.when(s == last)
        def _():
            g_in[idx] = comb[idx]

        @pl.when(c >= 2)
        def _():
            dpre_copy(c - 2).wait()
        slope_copy(c).wait()
        dx = backward_chunk(g_in[idx], w1, w2, slope_stg.at[slot], act_stg.at[slot]).astype(BF16)

        @pl.when(s > 0)
        def _():
            g_buf[idx] = dx
            b_copy(c, s - 1).start()

        @pl.when(s == 0)
        def _():
            gx[idx] = dx
            gx_send_all(c, 0)
            gx_save(c).start()
        dpre_copy(c).start()

        @pl.when(c + 2 < n_chunks)
        def _():
            slope_copy(c + 2).start()

    full = rows // E_ROWS
    rest = rows - full * E_ROWS

    def backward(n_rows, d_in, e_stg):
        def d_load(i, size=E_ROWS):
            slot = lax.rem(i, 2)
            src = dt_out.at[pl.ds(pl.multiple_of(i * E_ROWS, E_ROWS), size)]
            return pltpu.make_async_copy(src, d_in.at[slot, pl.ds(0, size)], d_sem.at[slot])

        def e_save(i, size=E_ROWS):
            slot = lax.rem(i, 2)
            dst = ge_out.at[pl.ds(pl.multiple_of(i * E_ROWS, E_ROWS), size)]
            return pltpu.make_async_copy(e_stg.at[slot, pl.ds(0, size)], dst, e_sem.at[slot])

        def e_tile(i):
            slot = lax.rem(i, 2)

            @pl.when(i + 1 < full)
            def _():
                d_load(i + 1).start()
            if rest:
                @pl.when(i + 1 == full)
                def _():
                    d_load(full, rest).start()
            d_load(i).wait()

            @pl.when(i == 0)
            def _():
                n_load.wait()

            @pl.when(i >= 2)
            def _():
                e_save(i - 2).wait()
            e_stg[slot] = dot_nn(d_in[slot], n_rows[...].reshape(mbs * mtok, dim))
            e_save(i).start()

        n_load = pltpu.make_async_copy(n_out, n_rows, out_sem.at[1])
        n_load.start()

        def table_start():
            for seq in (rounds * n_tiles - 2, rounds * n_tiles - 1):
                d_copy(seq).wait()
            d_load(0).start()

        @pl.when(s < last)
        def _():
            table_start()
        early = jnp.int32(0)
        for node, tiles in enumerate(EARLY_TILES):
            early = early + jnp.where(s == node, min(tiles, full), 0)
        loop(0, early, e_tile)

        def g_save(mb, count):
            at = pl.ds(mb, count)
            return pltpu.make_async_copy(g_in.at[at], g_out.at[at], out_sem.at[0])

        def gx_forward(c):
            gx_copy(c, 0, 0).wait_recv()
            each_role((3, last, 5), lambda node: gx_send_all(c, node))
            gx_save(c).start()

        def step(k):
            @pl.when(k >= HEAD_MBS)
            def _():
                @pl.when(k < mbs)
                def _():
                    g_final(k)
            b_mb = k - (last - s)

            @pl.when(b_mb == mbs - 1)
            def _():
                g_save(0, mbs - 1).start()

            @pl.when((b_mb >= 0) & (b_mb < mbs))
            def _():
                chunks_of(b_mb, bwd_chunk)

            @pl.when(k == 2)
            def _():
                g_mid(rounds - 1, (5,))

            @pl.when(k == 4)
            def _():
                g_mid(rounds - 1, (6,))

            x_mb = k - n_stage

            @pl.when((s == 3) & (x_mb >= 0) & (x_mb < gx_split // n_half))
            def _():
                chunks_of(x_mb, gx_forward)

        loop(0, mbs + last, step)
        g_save(mbs - 1, 1).start()

        @pl.when(s == last)
        def _():
            table_start()
        kept = jnp.where(s == last, LATE_TILES, 0)
        before = full - early - kept
        first_gx = jnp.where(s == 3, gx_split, 0)

        def late(j):
            c = first_gx + j - before

            @pl.when((j >= before) & (s > 0))
            def _():
                gx_forward(c)
            i = jnp.where(j < before, early + j, full - kept + c - gx_split)

            @pl.when((j < before) | ((c >= gx_split) & (i < full)))
            def _():
                e_tile(i)
            if rest:
                @pl.when(c == gx_split + kept)
                def _():
                    d_load(full, rest).wait()
                    e_save(full - 2).wait()
                    slot = full % 2
                    e_stg[slot, pl.ds(0, rest)] = dot_nn(d_in[slot, pl.ds(0, rest)], n_rows[...].reshape(mbs * mtok, dim))
                    e_save(full, rest).start()

            @pl.when(c == n_chunks - 3)
            def _():
                loss_out[...] = jnp.broadcast_to(jnp.sum(loss_acc[...], axis=1, keepdims=True), loss_out.shape)
                for c in (n_chunks - 2, n_chunks - 1):
                    dpre_copy(c).wait()
                pltpu.make_async_copy(g_in, g_out, out_sem.at[0]).wait()
                sent = stats.at[:, pl.ds(0, last)]
                remote(sent, sent, st_send.at[0], st_recv.at[0], lax.rem(s + 1, n_stage)).wait_send()

                @pl.when(s < last)
                def _():
                    remote(comb, buf_a, g_send.at[0], g_a.at[0], last).wait_send()

                @pl.when(s > 0)
                def _():
                    remote(g_buf, g_in, b_send.at[0], b_recv.at[0], 0).wait_send()

        loop(0, before + n_chunks - first_gx, late)
        if rest:
            e_save(full - 1).wait()
            e_save(full, rest).wait()
        else:
            e_save(full - 2).wait()
            e_save(full - 1).wait()
        pltpu.make_async_copy(gx, gx_out, gx_sem.at[0]).wait()
        for src, routes in gx_routes.items():
            @pl.when(s == src)
            def _(routes=routes):
                for lane, (dst, lo, hi) in enumerate(routes):
                    part = gx if hi - lo == n_chunks else gx.at[pl.ds(0, hi - lo), pl.ds(0, CHUNK)]
                    remote(part, part, gx_send.at[lane], gx_recv.at[0], dst).wait_send()

    pl.run_scoped(
        backward,
        pltpu.VMEM((mbs, mtok, dim), BF16), pltpu.VMEM((2, E_ROWS, mbs * mtok), BF16), pltpu.VMEM((2, E_ROWS, dim), F32),
    )


def pipeline_step(n_stage, labels, part, emb, w1, w2):
    mbs, mtok, dim = part.shape
    rows = emb.shape[0]
    ffn = w1.shape[1]
    chunks = mbs * mtok // CHUNK
    rounds = mbs // HEAD_MBS
    tokens = HEAD_MBS * mtok
    any_spec = pl.BlockSpec(memory_space=pl.ANY)
    vmem_spec = pl.BlockSpec(memory_space=pltpu.VMEM)
    act = pltpu.VMEM((mbs, mtok, dim), BF16)
    dma = pltpu.SemaphoreType.DMA
    act_shape = jax.ShapeDtypeStruct((mbs, mtok, dim), BF16)
    hid_shape = jax.ShapeDtypeStruct((chunks, CHUNK, ffn), BF16)
    return pl.pallas_call(
        functools.partial(step_kernel, n_stage),
        out_shape=(
            jax.ShapeDtypeStruct((chunks, CHUNK, ffn), F32), hid_shape, hid_shape,
            act_shape, act_shape, act_shape, act_shape,
            jax.ShapeDtypeStruct((rows, mbs * mtok), BF16),
            jax.ShapeDtypeStruct((rows, dim), F32),
            jax.ShapeDtypeStruct((8, 128), F32),
        ),
        in_specs=[vmem_spec] + [any_spec] * 4,
        out_specs=(any_spec,) * 9 + (vmem_spec,),
        scratch_shapes=[
            pltpu.VMEM((rows, dim), BF16), pltpu.VMEM((dim, ffn), BF16), pltpu.VMEM((ffn, dim), BF16),
            act, act, act, act, act, act,
            pltpu.VMEM((2, CHUNK, ffn), F32), pltpu.VMEM((2, CHUNK, ffn), BF16),
            pltpu.VMEM((2, vocab_tile(rows), tokens), BF16), pltpu.VMEM((rounds, n_stage, 8, tokens), F32), pltpu.VMEM((1, tokens), F32),
            dma((3,)), dma((1,)), dma((1,)), dma((chunks,)), dma((chunks,)), dma((chunks,)),
            dma((1,)), dma((chunks,)), dma((3,)), dma((chunks,)), dma((1,)), dma((rounds,)),
            dma((1,)), dma((mbs,)), dma((mbs,)), dma((1,)), dma((chunks,)), dma((4,)), dma((chunks,)),
            dma((2,)), dma((2,)), dma((2,)), dma((2,)), dma((2,)), dma((2,)), dma((1,)),
        ],
        compiler_params=pltpu.CompilerParams(collective_id=0, has_side_effects=True, vmem_limit_bytes=VMEM_LIMIT),
        name="pipeline_step",
    )(labels, part, emb, w1, w2)


WINDOW = 256
W_COLS = 1024
E_SLOTS = 4


def tail_kernel(
    rows, tok_ref, loss_ref, x_hbm, g_hbm, gx_hbm, dpre_hbm, hid_hbm, ge_hbm,
    loss_out, g1_out, g2_out, out_hbm,
    x_buf, g_buf, gx_buf, dp_buf, hid_buf, g1_stg, g2_stg, e_buf, packed, packed_id, bounds,
    act_sem, dp_sem, hid_sem, g1_sem, g2_sem, e_in_sem, e_out_sem,
):
    mbs, mtok = tok_ref.shape
    total, dim = g_buf.shape
    ffn = dpre_hbm.shape[1]
    n_blocks = ffn // W_COLS
    e_rows = e_buf.shape[1]
    n_e = rows // e_rows
    per_block = n_e // n_blocks

    def cols(j):
        return pl.ds(pl.multiple_of(j * W_COLS, W_COLS), W_COLS)

    def e_at(i):
        return pl.ds(pl.multiple_of(i * e_rows, 8), e_rows)

    def dp_load(j):
        slot = lax.rem(j, 2)
        return pltpu.make_async_copy(dpre_hbm.at[:, cols(j)], dp_buf.at[slot], dp_sem.at[slot])

    def hid_load(j):
        slot = lax.rem(j, 2)
        return pltpu.make_async_copy(hid_hbm.at[:, cols(j)], hid_buf.at[slot], hid_sem.at[slot])

    def e_load(i):
        slot = lax.rem(i, E_SLOTS)
        return pltpu.make_async_copy(ge_hbm.at[e_at(i)], e_buf.at[slot], e_in_sem.at[slot])

    def e_save(i):
        slot = lax.rem(i, E_SLOTS)
        return pltpu.make_async_copy(e_buf.at[slot], out_hbm.at[e_at(i)], e_out_sem.at[slot])

    def g1_save(j):
        return pltpu.make_async_copy(g1_stg, g1_out.at[0, :, cols(j)], g1_sem.at[0])

    def g2_save(j):
        return pltpu.make_async_copy(g2_stg, g2_out.at[0, cols(j)], g2_sem.at[0])

    x_load = pltpu.make_async_copy(x_hbm, x_buf, act_sem.at[0])
    g_load = pltpu.make_async_copy(g_hbm, g_buf, act_sem.at[1])
    gx_load = pltpu.make_async_copy(gx_hbm, gx_buf, act_sem.at[2])
    gx_load.start()
    loss_out[0] = loss_ref[0, 0] * (1.0 / total)

    s = lax.axis_index("stage")
    loc = tok_ref[...] - s * rows
    upper, lower = triangles(mbs, mtok)
    slot_of = jnp.full((mbs, mtok), -1.0, F32)
    count = jnp.int32(0)
    bounds[0] = count
    for i in range(n_e):
        inside = (loc >= i * e_rows) & (loc < (i + 1) * e_rows)
        rank, number = ranks(inside.astype(F32), upper, lower)
        slot_of = jnp.where(inside, rank + count.astype(F32), slot_of)
        count = count + number
        bounds[i + 1] = count
    slot_of = slot_of.astype(jnp.int32)
    n_packs = jnp.maximum((count + WINDOW - 1) // WINDOW, 1)

    def pack(b):
        slot = lax.broadcasted_iota(jnp.int32, (WINDOW, mtok), 0) + b * WINDOW
        ids = jnp.zeros((WINDOW, 1), F32)
        picks = []
        for mb in range(mbs):
            pick = slot == slot_of[mb:mb + 1, :]
            picks.append(pick.astype(BF16))
            ids = ids + jnp.sum(jnp.where(pick, loc[mb:mb + 1, :].astype(F32), 0.0), axis=1, keepdims=True)
        at = pl.ds(pl.multiple_of(b * WINDOW, WINDOW), WINDOW)
        packed[at, :] = dot_nn(jnp.concatenate(picks, axis=1), gx_buf[...]).astype(BF16)
        filled = lax.broadcasted_iota(jnp.int32, (WINDOW, 1), 0) + b * WINDOW < count
        packed_id[at, :] = jnp.broadcast_to(jnp.where(filled, ids.astype(jnp.int32), -1), (WINDOW, 128))

    def loop(lo, hi, fn):
        def body(i, _):
            fn(i)
            return 0
        lax.fori_loop(lo, hi, body, 0)

    def e_tile(i):
        slot = lax.rem(i, E_SLOTS)
        first = jnp.minimum((bounds[i] // 16) * 16, (n_packs - 1) * WINDOW)
        lane = lax.broadcasted_iota(jnp.int32, (WINDOW, e_rows), 1) + i * e_rows

        def window(k):
            start = pl.multiple_of(jnp.minimum(first + k * WINDOW, (n_packs - 1) * WINDOW), 16)
            at = pl.ds(start, WINDOW)
            fresh = lax.broadcasted_iota(jnp.int32, (WINDOW, 1), 0) + start >= first + k * WINDOW
            ids = jnp.where(fresh, packed_id[at, :][:, 0:1], -1)
            return dot_tn((lane == ids).astype(BF16), packed[at, :])

        e_load(i).wait()
        e_buf[slot] = e_buf[slot] + window(0)

        def more(k):
            e_buf[slot] = e_buf[slot] + window(k)

        loop(1, (bounds[i + 1] - first + WINDOW - 1) // WINDOW, more)
        e_save(i).start()

    def block(j):
        slot = lax.rem(j, 2)

        @pl.when(j == 0)
        def _():
            x_load.wait()

        @pl.when(j > 0)
        def _():
            g1_save(j - 1).wait()
        dp_load(j).wait()

        @pl.when(j == 0)
        def _():
            for cp in (e_load(0), e_load(1), g_load, hid_load(0)):
                cp.start()
        g1_stg[...] = dot_tn(x_buf[...], dp_buf[slot])
        g1_save(j).start()

        @pl.when(j + 1 < n_blocks)
        def _():
            dp_load(j + 1).start()

        loop(j * per_block, (j + 1) * per_block, e_tile)

        @pl.when(j == 0)
        def _():
            g_load.wait()

        @pl.when(j > 0)
        def _():
            g2_save(j - 1).wait()
        hid_load(j).wait()

        @pl.when(j + 1 < n_blocks)
        def _():
            hid_load(j + 1).start()

        def ahead(i):
            @pl.when(i >= E_SLOTS)
            def _():
                e_save(i - E_SLOTS).wait()
            e_load(i).start()

        @pl.when(j + 1 < n_blocks)
        def _():
            loop((j + 1) * per_block, (j + 2) * per_block, ahead)
        g2_stg[...] = dot_tn(hid_buf[slot], g_buf[...])
        g2_save(j).start()

    x_load.start()
    dp_load(0).start()
    gx_load.wait()
    loop(0, n_packs, pack)
    loop(0, n_blocks, block)
    g1_save(n_blocks - 1).wait()
    g2_save(n_blocks - 1).wait()
    for i in range(max(n_e - E_SLOTS, 0), n_e):
        e_save(i).wait()


def tail(tok, loss, x, g, gx, dpre, hid, ge):
    rows, dim = ge.shape
    total, ffn = dpre.shape
    n_blocks = ffn // W_COLS
    e_rows = rows // (2 * n_blocks)
    n_e = rows // e_rows
    any_spec = pl.BlockSpec(memory_space=pl.ANY)
    vmem_spec = pl.BlockSpec(memory_space=pltpu.VMEM)
    dma = pltpu.SemaphoreType.DMA
    act = pltpu.VMEM((total, dim), BF16)
    return pl.pallas_call(
        functools.partial(tail_kernel, rows),
        out_shape=(
            jax.ShapeDtypeStruct((1,), F32),
            jax.ShapeDtypeStruct((1, dim, ffn), F32),
            jax.ShapeDtypeStruct((1, ffn, dim), F32),
            jax.ShapeDtypeStruct((rows, dim), F32),
        ),
        in_specs=[vmem_spec, vmem_spec] + [any_spec] * 6,
        out_specs=(pl.BlockSpec(memory_space=pltpu.SMEM), any_spec, any_spec, any_spec),
        scratch_shapes=[
            act, act, act, pltpu.VMEM((2, total, W_COLS), BF16), pltpu.VMEM((2, total, W_COLS), BF16),
            pltpu.VMEM((dim, W_COLS), F32), pltpu.VMEM((W_COLS, dim), F32), pltpu.VMEM((E_SLOTS, e_rows, dim), F32),
            pltpu.VMEM((total, dim), BF16), pltpu.VMEM((total, 128), jnp.int32), pltpu.SMEM((n_e + 1,), jnp.int32),
            dma((3,)), dma((2,)), dma((2,)), dma((1,)), dma((1,)), dma((E_SLOTS,)), dma((E_SLOTS,)),
        ],
        compiler_params=pltpu.CompilerParams(vmem_limit_bytes=VMEM_LIMIT),
        name="tail",
    )(tok, loss, x, g, gx, dpre, hid, ge)


def solution(mesh):
    n_stage = mesh.shape["stage"]

    def stage_body(token_ids, label_ids, emb_rows, w_in, w_out):
        tokens = token_ids.shape[0] * token_ids.shape[1]
        part = lookup(token_ids, emb_rows)
        _, hid, dpre, x_in, _, g_all, gx, _, ge, loss = pipeline_step(n_stage, label_ids, part, emb_rows, w_in[0], w_out[0])
        flat = lambda a: a.reshape(tokens, a.shape[-1])
        mean_loss, grad_in, grad_out, grad_emb = tail(token_ids, loss, flat(x_in), flat(g_all), flat(gx), flat(dpre), flat(hid), ge)
        return mean_loss, grad_in, grad_out, grad_emb

    return jax.shard_map(
        stage_body,
        mesh=mesh,
        in_specs=(P("dp", None), P("dp", None), P("stage", None), P("stage", None, None), P("stage", None, None)),
        out_specs=(P("dp"), P(("dp", "stage"), None, None), P(("dp", "stage"), None, None), P(("dp", "stage"), None)),
        check_vma=False,
    )
```
